128 devices in a mesh: seq: 16 (over y_hi, z, core), tp: 8 (over x, y_lo).
Axes of the slice: x: 4, y: 4 (y_hi: 2, y_lo: 2; y = y_hi * 2 + y_lo), z: 4, core: 2. Of those that a mesh axis runs over, the one named last changes fastest.
Arguments:
- streams: bfloat16 [8192, 4, 4096], P('seq', None, 'tp'), may hold values from -6 to 6
- doc_ids: int32 [8192], P('seq'), may hold values from 0 to 3, never falling along the last dimension, each value on 1 to 4096 neighbouring positions
- mix_weight: float32 [4, 4096, 24], P(None, 'tp'), may hold values from -0.046875 to 0.046875
- mix_bias: float32 [24], replicated, may hold values from -1 to 1
- attn_gain: float32 [4096], replicated, may hold values from 0.1 to 1.9
- w_qkv: bfloat16 [4096, 3, 4096], P(None, None, 'tp'), may hold values from -1 to 1
- w_out: bfloat16 [4096, 4096], P('tp'), may hold values from -0.5 to 0.5
Outputs:
- new_streams: bfloat16 [8192, 4, 4096], P('seq', None, 'tp')
The draws below stay inside these ranges and needn't reach their ends.
Inputs may be any that keep to these rules, and one draw needn't show every extreme that they name: doc_ids never fall along the sequence; each of the 4 documents has 1 to 4096 positions, and the longest has exactly 4096.
All inputs are finite; a program needn't handle non-finite values.
Results may differ from the reference program's by a relative error of at most 0.014.
The reference program's roundings to bfloat16 on the way count: a program that leaves them out, or rounds other values in their place, can miss the bound.
Values may be sent and summed in bfloat16 or wider, within the bound.
A program may use at most 256 MiB of HBM per device.

```python
import math
import jax
import jax.numpy as jnp
import numpy as np
from jax import lax

D = 4096
HEADS = 32
HEAD_DIM = 128
STREAMS = 4
BALANCE_ROUNDS = 20
DOCS = 4
TOKENS = 8192
COEFS = 24


def draw_w_qkv(key, part):
    key_base = jax.random.fold_in(key, 11)
    scale_in = jnp.float32(D) ** (-0.5)
    base = jax.random.normal(key_base, (D, 3, D), jnp.float32) * scale_in
    base = jnp.clip(base, -4.0 * scale_in, 4.0 * scale_in)
    return base.astype(jnp.bfloat16)


def block_scale(stream_key, extent, cuts, least, high):
    gain, own = 1.0, jax.random.fold_in(stream_key, 6)
    for position, shards_of in cuts:
        steps = jnp.exp(jax.random.uniform(jax.random.fold_in(own, position), (shards_of,), jnp.float32, least / len(cuts), high / len(cuts)))
        gain = gain * jnp.repeat(steps, extent[position] // shards_of).reshape([-1 if axis == position else 1 for axis in range(len(extent))])
    return gain


def length_profile(number_of, total, most, skew):
    loads = [(1 << 20) // math.isqrt(grade ** skew) + 1 for grade in range(2, number_of + 1)]
    spare, counts = total - most - (number_of - 1), [1] * (number_of - 1)
    while spare > 0:
        free = [i for i in range(number_of - 1) if counts[i] < most]
        whole, left = sum([loads[i] for i in free]), spare
        for i in free:
            more = min(most - counts[i], max(1, left * loads[i] // whole), spare)
            counts[i] = counts[i] + more
            spare = spare - more
    return np.array([most] + counts)


def uneven_parts(stream_key, number_of, total, limit, slope):
    if number_of == 2:
        one = jax.random.randint(stream_key, (), max(1, total - limit), min(limit, total - 1) + 1)
        return jnp.stack([one, total - one])
    sizes = jnp.asarray(length_profile(number_of, total, limit, slope), jnp.int32)
    twos = (number_of - 1) // 2
    source_of, taker = sizes[1:1 + 2 * twos:2], sizes[2:2 + 2 * twos:2]
    margin = jnp.minimum(source_of - 1, limit - taker)
    passed = jax.random.randint(jax.random.fold_in(stream_key, 1), (twos,), 0, 1 << 20) % (margin + 1)
    sizes = sizes.at[1:1 + 2 * twos:2].set(source_of - passed).at[2:2 + 2 * twos:2].set(taker + passed)
    return sizes[jax.random.permutation(jax.random.fold_in(stream_key, 2), number_of)]


def scatter_about(key, shape, width, limit, pieces=(), held_as=jnp.bfloat16):
    loudness = block_scale(key, shape, pieces, -0.22, 0.18) if pieces else 1.0
    result = jax.random.normal(key, shape, jnp.float32) * width * loudness
    return jnp.minimum(jnp.maximum(result, -limit), limit).astype(held_as)


def setup_inputs(seed: int = 0) -> dict:
    key_list = jax.random.split(jax.random.key(seed), 8)
    return {
        "streams": scatter_about(key_list[0], (TOKENS, STREAMS, D), 1.0, 6.0, ((0, 16), (2, 8))),
        "doc_ids": jnp.searchsorted(jnp.cumsum(uneven_parts(key_list[1], DOCS, TOKENS, TOKENS // 2, 0)), jnp.arange(TOKENS), side="right").astype(jnp.int32),
        "mix_weight": scatter_about(key_list[2], (STREAMS, D, COEFS), (STREAMS * D) ** -0.5, 0.046875, ((1, 8),), jnp.float32),
        "mix_bias": jnp.clip(jax.random.uniform(key_list[3], (COEFS,), jnp.float32, -1.0, 1.0), -1.0, 1.0),
        "attn_gain": jnp.clip(1.0 + 0.18 * jax.random.normal(key_list[4], (D,), jnp.float32), 0.1, 1.9),
        "w_qkv": draw_w_qkv(jax.random.fold_in(key_list[7], 71), 0),
        "w_out": scatter_about(key_list[6], (D, D), HEAD_DIM ** -0.5, 0.5, ((0, 8),)),
    }


masked_score = -1e+30
norm_eps = 1e-06

def doubly_stochastic(mixing_matrix):

    def balance_round(round_index, running_matrix):
        running_matrix = running_matrix / lax.optimization_barrier(jnp.sum(running_matrix, axis=2, keepdims=True))
        return running_matrix / lax.optimization_barrier(jnp.sum(running_matrix, axis=1, keepdims=True))
    return lax.fori_loop(0, BALANCE_ROUNDS, balance_round, mixing_matrix)

def coefficients(squares, partial_logits, mix_bias):
    root_mean = jnp.sqrt(squares / (STREAMS * D) + norm_eps)
    coef_logits = partial_logits / root_mean[:, None] + mix_bias
    input_weights = jax.nn.sigmoid(coef_logits[:, :STREAMS])
    output_weights = 2.0 * jax.nn.sigmoid(coef_logits[:, STREAMS:2 * STREAMS])
    unnormalized_mixing = jnp.exp(coef_logits[:, 2 * STREAMS:]).reshape(-1, STREAMS, STREAMS)
    return (input_weights, output_weights, doubly_stochastic(unnormalized_mixing))

def head_attention(queries, keys, values, doc_ids):
    positions = jnp.arange(TOKENS, dtype=jnp.int32)
    block_rows = math.gcd(512, TOKENS)

    def one_block(first_row):
        query_block = lax.dynamic_slice_in_dim(queries, first_row, block_rows, 0)
        query_pos = first_row + jnp.arange(block_rows, dtype=jnp.int32)
        query_doc = lax.dynamic_slice_in_dim(doc_ids, first_row, block_rows, 0)
        scores = jnp.dot(query_block, keys.T, preferred_element_type=jnp.float32) * HEAD_DIM ** (-0.5)
        allowed = (positions[None, :] <= query_pos[:, None]) & (doc_ids[None, :] == query_doc[:, None])
        scores = jnp.where(allowed, scores, masked_score)
        row_max = lax.optimization_barrier(jnp.max(scores, axis=1, keepdims=True))
        exp_weights = jnp.where(allowed, jnp.exp(scores - row_max), 0.0)
        numerator = jnp.dot(exp_weights.astype(jnp.bfloat16), values, preferred_element_type=jnp.float32)
        return (numerator / lax.optimization_barrier(jnp.sum(exp_weights, axis=1, keepdims=True))).astype(jnp.bfloat16)
    block_starts = jnp.arange(TOKENS // block_rows, dtype=jnp.int32) * block_rows
    return lax.map(one_block, block_starts).reshape(TOKENS, HEAD_DIM)

def reference(streams, doc_ids, mix_weight, mix_bias, attn_gain, w_qkv, w_out):
    wide_streams = streams.astype(jnp.float32)
    squares = lax.optimization_barrier(jnp.sum(wide_streams * wide_streams, axis=(1, 2)))
    partial_logits = jnp.einsum('tsd,sdc->tc', wide_streams, mix_weight, precision=lax.Precision.HIGHEST)
    input_weights, output_weights, mixing = coefficients(squares, partial_logits, mix_bias)
    mixed_input = jnp.einsum('ts,tsd->td', input_weights, wide_streams, precision=lax.Precision.HIGHEST).astype(jnp.bfloat16)
    input_wide = mixed_input.astype(jnp.float32)
    norm_scale = lax.rsqrt(lax.optimization_barrier(jnp.mean(input_wide * input_wide, axis=1)) + norm_eps)
    gained = (input_wide * attn_gain).astype(jnp.bfloat16)
    projected = jnp.dot(gained, w_qkv.reshape(D, 3 * D), preferred_element_type=jnp.float32)
    projected = (projected * norm_scale[:, None]).astype(jnp.bfloat16).reshape(TOKENS, 3, HEADS, HEAD_DIM)
    per_head = jnp.moveaxis(projected, 2, 0)
    context = lax.map(lambda head_slab: head_attention(head_slab[:, 0], head_slab[:, 1], head_slab[:, 2], doc_ids), per_head)
    context = jnp.moveaxis(context, 0, 1).reshape(TOKENS, D)
    branch_out = jnp.dot(context, w_out, preferred_element_type=jnp.float32)
    carried = jnp.einsum('tij,tjd->tid', mixing, wide_streams, precision=lax.Precision.HIGHEST)
    return (carried + output_weights[:, :, None] * branch_out[:, None, :]).astype(jnp.bfloat16)
```

```python
import jax
import jax.numpy as jnp
from jax import lax
from jax.experimental import pallas as pl
from jax.experimental.pallas import tpu as pltpu
from jax.sharding import PartitionSpec as P

D = 4096
HD = 128
S = 4
ROUNDS = 20
EPS = 1e-6
T = 512
W = 512
NC = 4
R = T // NC
F32 = jnp.float32
BF = jnp.bfloat16
MESH = pl.DeviceIdType.MESH
NT = (((1,), (1,)), ((), ()))
NEG = -1e30
VMEM = pltpu.VMEM
DMA = pltpu.SemaphoreType.DMA


def where_am_i():
    seq = lax.axis_index("seq")
    tp = lax.axis_index("tp")
    return seq, tp


def remote(src, dst, ssem, rsem, seq, tp):
    return pltpu.make_async_remote_copy(
        src_ref=src, dst_ref=dst, send_sem=ssem, recv_sem=rsem,
        device_id={"seq": seq, "tp": tp}, device_id_type=MESH,
    )


def greet(peers):
    barrier = pltpu.get_barrier_semaphore()
    for seq, tp in peers:
        pl.semaphore_signal(barrier, inc=1, device_id={"seq": seq, "tp": tp}, device_id_type=MESH)
    return lambda: pl.semaphore_wait(barrier, len(peers))


def columns(rows8):
    k = rows8.shape[0]
    if k < 128:
        rows8 = jnp.concatenate([rows8, jnp.zeros((128 - k, rows8.shape[1]), F32)], axis=0)
    return rows8.T


def balanced(e0, e1):
    sub = lax.broadcasted_iota(jnp.int32, e0.shape, 0)
    even, low = sub % 2 == 0, sub % 4 < 2

    def row_total(e):
        u = e + jnp.where(even, pltpu.roll(e, 7, 0), pltpu.roll(e, 1, 0))
        return u + jnp.where(low, pltpu.roll(u, 6, 0), pltpu.roll(u, 2, 0))

    def one_round(_, pair):
        e0, e1 = pair
        e0 = e0 / row_total(e0)
        e1 = e1 / row_total(e1)
        t = e0 + e1
        t = t + pltpu.roll(t, 4, 0)
        return e0 / t, e1 / t

    return lax.fori_loop(0, ROUNDS, one_round, (e0, e1))


def first_kernel(
    xs, docs, wmix, bias, gain, w_hbm,
    att, mix_cols, counts,
    wbuf, g, sb, relay, gained, unow, urecv, nall, nrecv, crecv, csend, pre_cols,
    w_sem, u_ss, u_rs, n_ss, n_rs, c_ss, c_rs, g_ss, g_rs, a_ss, a_rs,
    sib_ss, sib_rs, x_ss, x_rs, f_ss, f_rs, sib2_ss, sib2_rs,
):
    seq, tp = where_am_i()
    yhi, z, core = seq // 8, (seq // 2) % 4, seq % 2
    x, y = tp // 2, tp % 2
    tp_peers = [(seq, (tp + r) % 8) for r in range(1, 8)]
    seq_peers = [((seq + r) % 16, tp) for r in range(1, 16)]
    other_y = x * 2 + 1 - y
    diagonal = ((seq + 8) % 16, other_y)
    entered = greet(tp_peers + seq_peers + [diagonal])

    def wcopy(i):
        return pltpu.make_async_copy(w_hbm.at[i], wbuf.at[i], w_sem.at[i])

    for i in range(3):
        wcopy(i).start()

    acc = jnp.zeros((T, 128), F32)
    logits = jnp.zeros((32, T), F32)
    for s in range(S):
        xv = xs[s]
        w = jnp.concatenate([wmix[s], jnp.zeros((8, W), F32)], axis=0)
        hi = w.astype(BF).astype(F32)
        mid = (w - hi).astype(BF).astype(F32)
        low = (w - hi) - mid
        parts = jnp.concatenate([hi, mid, low], axis=0).astype(BF)
        got = lax.dot_general(parts, xv, NT, preferred_element_type=F32)
        logits = logits + (got[0:32] + (got[32:64] + got[64:96]))
        x32 = xv.astype(F32)
        sq = x32 * x32
        acc = acc + ((sq[:, 0:128] + sq[:, 128:256]) + (sq[:, 256:384] + sq[:, 384:512]))
    squares = jnp.sum(acc.T, axis=0, keepdims=True)
    sub = lax.broadcasted_iota(jnp.int32, (8, T), 0)
    unow[...] = jnp.where(sub < 4, logits[0:8], jnp.where(sub == 4, jnp.broadcast_to(squares, (8, T)), 0.0))
    nall[...] = logits[0:24]
    dv = docs[...]
    csub = lax.broadcasted_iota(jnp.int32, (8, 128), 0)
    cv = jnp.zeros((8, 128), jnp.int32)
    for k in range(1, 4):
        n = jnp.sum(jnp.where(dv < k, 1, 0), axis=1, keepdims=True)
        n = jnp.sum(n, axis=0, keepdims=True)
        cv = jnp.where(csub == k, jnp.broadcast_to(n, (8, 128)), cv)
    csend[...] = cv

    entered()
    for r, (sq_, tp_) in enumerate(tp_peers):
        remote(unow, urecv.at[r], u_ss.at[r], u_rs.at[r], sq_, tp_).start()
    for r, (sq_, tp_) in enumerate(seq_peers):
        remote(csend, crecv.at[r], c_ss.at[r], c_rs.at[r], sq_, tp_).start()

    total = unow[...]
    for r, (sq_, tp_) in enumerate(tp_peers):
        remote(unow, urecv.at[r], u_ss.at[r], u_rs.at[r], sq_, tp_).wait_recv()
        total = total + urecv[r]
    inv_rms = lax.rsqrt(total[4:5] / (S * D) + EPS)
    pre = 1.0 / (1.0 + jnp.exp(-(total * inv_rms + bias[0:8])))
    pre_cols[...] = columns(pre)

    right = ((x + 1) % 4) * 2 + y
    left = ((x + 3) % 4) * 2 + y
    b_p = other_y
    b_l0, b_l1 = left, ((x + 3) % 4) * 2 + 1 - y
    b_r0, b_r1 = right, ((x + 1) % 4) * 2 + 1 - y
    b_f0, b_f1 = ((x + 2) % 4) * 2 + y, ((x + 2) % 4) * 2 + 1 - y

    def move(c, k, blk, role, to):
        return remote(g.at[c, blk], g.at[c, blk], g_ss.at[c, k], g_rs.at[c, role], seq, to)

    def arrived(c, role, blk):
        move(c, 0, blk, role, right).wait_recv()

    def make_chunk(c):
        rows = slice(c * R, (c + 1) * R)
        v = pre_cols[rows, 0:1] * xs[0, rows, :].astype(F32)
        for s in range(1, S):
            v = v + pre_cols[rows, s : s + 1] * xs[s, rows, :].astype(F32)
        g[c, tp] = v.astype(BF)

    def send_chunk(c):
        move(c, 0, tp, 1, right).start()
        move(c, 1, tp, 3, left).start()
        move(c, 2, tp, 0, other_y).start()

    make_chunk(0)
    for c in range(NC):
        if c + 1 < NC:
            make_chunk(c + 1)
        send_chunk(c)
    for c in range(NC):
        arrived(c, 0, b_p)
        move(c, 3, b_p, 2, right).start()
        move(c, 4, b_p, 4, left).start()
        arrived(c, 1, b_l0)
        move(c, 5, b_l0, 5, right).start()
        arrived(c, 4, b_r1)
        move(c, 6, b_r1, 6, left).start()
    for r, (sq_, tp_) in enumerate(tp_peers):
        remote(nall, nrecv.at[r], n_ss.at[r], n_rs.at[r], sq_, tp_).start()
    for i in range(3):
        wcopy(i).wait()

    def block_of(half, d):
        return half * 8 + ((z + 4 - d) % 4) * 2 + core

    def spread(c, d):
        to_z = (z + d) % 4
        return remote(
            sb.at[to_z, c], att.at[seq, c], a_ss.at[c, d - 1], a_rs.at[c, d - 1],
            yhi * 8 + to_z * 2 + core, tp,
        )

    def twin(c, d):
        ref = att.at[block_of(yhi, d), c, pl.ds(0, 2)]
        return remote(ref, ref, sib_ss.at[c, d], sib_rs.at[c, d], seq + 1 - 2 * core, tp)

    def twin_in(c, d):
        ref = att.at[yhi * 8 + ((z + 4 - d) % 4) * 2 + 1 - core, c, pl.ds(0, 2)]
        return remote(ref, ref, sib_ss.at[c, d], sib_rs.at[c, d], seq + 1 - 2 * core, tp)

    def cross(c, d):
        ref = att.at[block_of(0, d), c, pl.ds(0, 2)]
        return remote(ref, relay.at[d, c], x_ss.at[c, d], x_rs.at[c, d], diagonal[0], diagonal[1])

    def final(c, d):
        return remote(
            relay.at[d, c], att.at[block_of(0, d), c, pl.ds(0, 2)],
            f_ss.at[c, d], f_rs.at[c, d], seq, other_y,
        )

    def twin2(c, d):
        ref = att.at[block_of(0, d), c, pl.ds(0, 2)]
        return remote(ref, ref, sib2_ss.at[c, d], sib2_rs.at[c, d], seq + 1 - 2 * core, tp)

    def twin2_in(c, d):
        ref = att.at[((z + 4 - d) % 4) * 2 + 1 - core, c, pl.ds(0, 2)]
        return remote(ref, ref, sib2_ss.at[c, d], sib2_rs.at[c, d], seq + 1 - 2 * core, tp)

    def step(c, carry):
        @pl.when(c < NC)
        def _():
            arrived(c, 2, b_l1)
            arrived(c, 3, b_r0)
            arrived(c, 5, b_f0)
            arrived(c, 6, b_f1)
            ss = jnp.zeros((R, 128), F32)
            for b in range(8):
                g32 = g[c, b].astype(F32)
                q = g32 * g32
                ss = ss + ((q[:, 0:128] + q[:, 128:256]) + (q[:, 256:384] + q[:, 384:512]))
                gained[:, b * W : (b + 1) * W] = (g32 * gain[:, b * W : (b + 1) * W]).astype(BF)
            norm = lax.rsqrt(jnp.sum(ss, axis=1, keepdims=True) / D + EPS)
            lhs = gained[...]
            for slot, third in ((0, 1), (1, 2), (2, 0)):
                acc = jnp.dot(lhs, wbuf[third], preferred_element_type=F32)
                out = (acc * norm).astype(BF)
                for h in range(4):
                    sb[h, c, slot] = out[:, h * HD : (h + 1) * HD]
            att[seq, c] = sb[z, c]
            for d in (2, 1, 3):
                spread(c, d).start()

        @pl.when((c >= 1) & (c <= NC))
        def _():
            for d in range(4):
                if d:
                    spread_in(c - 1, d)
                twin(c - 1, d).start()

                @pl.when(yhi == 0)
                def _():
                    cross(c - 1, d).start()

        @pl.when((c >= 2) & (c <= NC + 1) & (yhi == 1))
        def _():
            for d in range(4):
                cross(c - 2, d).wait_recv()
                final(c - 2, d).start()

        @pl.when((c >= 3) & (yhi == 1))
        def _():
            for d in range(4):
                final(c - 3, d).wait_recv()
                twin2(c - 3, d).start()

        return carry

    def spread_in(c, d):
        ref = att.at[block_of(yhi, d), c]
        remote(sb.at[z, c], ref, a_ss.at[c, d - 1], a_rs.at[c, d - 1], seq, other_y).wait_recv()

    lax.fori_loop(0, NC + 3, step, 0)

    ztot = nall[...]
    for r, (sq_, tp_) in enumerate(tp_peers):
        remote(nall, nrecv.at[r], n_ss.at[r], n_rs.at[r], sq_, tp_).wait_recv()
        ztot = ztot + nrecv[r]
    ztot = ztot * inv_rms + bias[...]
    post = 2.0 / (1.0 + jnp.exp(-ztot[0:8]))
    e0, e1 = balanced(jnp.exp(ztot[8:16]), jnp.exp(ztot[16:24]))
    mix_cols[...] = columns(jnp.concatenate([post, e0, e1], axis=0))
    cv = csend[...]
    for r, (sq_, tp_) in enumerate(seq_peers):
        remote(csend, crecv.at[r], c_ss.at[r], c_rs.at[r], sq_, tp_).wait_recv()
        cv = cv + crecv[r]
    counts[...] = cv

    for r, (sq_, tp_) in enumerate(tp_peers):
        remote(unow, urecv.at[r], u_ss.at[r], u_rs.at[r], sq_, tp_).wait_send()
        remote(nall, nrecv.at[r], n_ss.at[r], n_rs.at[r], sq_, tp_).wait_send()
    for r, (sq_, tp_) in enumerate(seq_peers):
        remote(csend, crecv.at[r], c_ss.at[r], c_rs.at[r], sq_, tp_).wait_send()

    def drain(c, carry):
        for k in range(7):
            move(c, k, tp, 0, right).wait_send()
        for d in range(1, 4):
            spread(c, d).wait_send()
        for d in range(4):
            twin(c, d).wait_send()
            twin_in(c, d).wait_recv()

        @pl.when(yhi == 0)
        def _():
            for d in range(4):
                cross(c, d).wait_send()

        @pl.when(yhi == 1)
        def _():
            for d in range(4):
                final(c, d).wait_send()
                twin2(c, d).wait_send()
                twin2_in(c, d).wait_recv()

        return carry

    lax.fori_loop(0, NC, drain, 0)


def attention_kernel(att, cnt, ctx, m_ref, l_ref, acc_ref):
    seq, _ = where_am_i()
    yhi, core = seq // 8, seq % 2
    starts = [cnt[k, 0] for k in range(1, 4)]
    scale = HD ** (-0.5) * 1.4426950408889634

    def start_of(p):
        v = p * 0
        for c in starts:
            v = jnp.where(c <= p, jnp.maximum(v, c), v)
        return v

    def one_query_block(qi, carry):
        qb = yhi * 8 + qi * 2 + core
        q = att[qb, :, 2].reshape(T, HD)
        first = start_of(qb * T)
        last = start_of(qb * T + T - 1)
        lo = first // T
        mid = jnp.minimum((last + T - 1) // T, qb)
        qpos = qb * T + lax.broadcasted_iota(jnp.int32, (T, 1), 0)
        qstart = start_of(qpos)
        m_ref[...] = jnp.full((T, 128), NEG, F32)
        l_ref[...] = jnp.zeros((T, 128), F32)
        acc_ref[...] = jnp.zeros((T, HD), F32)

        def block(kb, masked):
            k = att[kb, :, 0].reshape(T, HD)
            v = att[kb, :, 1].reshape(T, HD)
            s = lax.dot_general(q, k, NT, preferred_element_type=F32)
            if masked:
                kpos = kb * T + lax.broadcasted_iota(jnp.int32, (1, T), 1)
                ok = (kpos <= qpos) & (kpos >= qstart)
                s = jnp.where(ok, s, NEG)
            top = jnp.maximum(
                jnp.maximum(s[:, 0:128], s[:, 128:256]), jnp.maximum(s[:, 256:384], s[:, 384:512])
            )
            m_old = m_ref[:, 0:1]
            m_new = jnp.maximum(m_old, jnp.max(top, axis=1, keepdims=True))
            p = jnp.exp2((s - m_new) * scale)
            if masked:
                p = jnp.where(ok, p, 0.0)
            alpha = jnp.exp2((m_old - m_new) * scale)
            part = (p[:, 0:128] + p[:, 128:256]) + (p[:, 256:384] + p[:, 384:512])
            l_ref[...] = l_ref[...] * alpha + part
            acc_ref[...] = acc_ref[...] * alpha + jnp.dot(p.astype(BF), v, preferred_element_type=F32)
            m_ref[...] = jnp.broadcast_to(m_new, (T, 128))

        def with_mask(kb, c):
            block(kb, True)
            return c

        def without(kb, c):
            block(kb, False)
            return c

        lax.fori_loop(lo, mid, with_mask, 0)
        lax.fori_loop(mid, qb, without, 0)
        lax.fori_loop(qb, qb + 1, with_mask, 0)
        out = acc_ref[...] / jnp.sum(l_ref[...], axis=1, keepdims=True)
        ctx[qi] = out.astype(BF).reshape(NC, R, HD)
        return carry

    lax.fori_loop(0, 4, one_query_block, 0)


def last_kernel(
    ctx, mix_cols, xs, w_hbm,
    out,
    wbuf, cbuf, snd, own, rcv,
    w_sem, z_ss, z_rs, s_ss, s_rs,
):
    seq, tp = where_am_i()
    yhi, z, core = seq // 8, (seq // 2) % 4, seq % 2
    x, y = tp // 2, tp % 2
    right = ((x + 1) % 4) * 2 + y
    left = ((x + 3) % 4) * 2 + y
    other_y = x * 2 + 1 - y
    z_peers = [yhi * 8 + ((z + d) % 4) * 2 + core for d in range(1, 4)]
    entered = greet([(p, tp) for p in z_peers] + [(seq, right), (seq, left), (seq, other_y)])
    wcopy = pltpu.make_async_copy(w_hbm, wbuf, w_sem)
    wcopy.start()
    entered()

    def back(c, d):
        to_z = (z + d) % 4
        return remote(
            ctx.at[to_z, c], cbuf.at[z, c], z_ss.at[c, d - 1], z_rs.at[c, d - 1], z_peers[d - 1], tp
        )

    def back_in(c, d):
        from_z = (z + 4 - d) % 4
        remote(
            ctx.at[z, c], cbuf.at[from_z, c], z_ss.at[c, d - 1], z_rs.at[c, d - 1], z_peers[d - 1], tp
        ).wait_recv()

    for c in range(NC):
        for d in (2, 1, 3):
            back(c, d).start()
    cbuf[z] = ctx[z]
    wcopy.wait()

    def pass_on(c, k, to):
        return remote(snd.at[c, k], rcv.at[c, k], s_ss.at[c, k], s_rs.at[c, k], seq, to)

    b0, b1 = ((x + 1) % 4) * 2, ((x + 3) % 4) * 2
    bf = ((x + 2) % 4) * 2

    def project(c, carry):
        for d in range(1, 4):
            back_in(c, d)
        lhs = jnp.concatenate([cbuf[h, c] for h in range(4)], axis=1)

        def term(b):
            cols = pl.ds(pl.multiple_of(b * W, W), W)
            return jnp.dot(lhs, wbuf[:, cols], preferred_element_type=F32)

        snd[c, 0] = term(bf).astype(BF)
        snd[c, 1] = term(bf + 1).astype(BF)
        pass_on(c, 0, right).start()
        pass_on(c, 1, left).start()
        snd[c, 3] = term(b0 + 1).astype(BF)
        snd[c, 4] = term(b1).astype(BF)
        pass_on(c, 3, right).start()
        pass_on(c, 4, left).start()
        own[c, 0] = term(b0)
        own[c, 1] = term(b1 + 1)
        own[c, 2] = term(x * 2)
        own[c, 3] = term(x * 2 + 1)
        return carry

    lax.fori_loop(0, NC, project, 0)

    def second(c, carry):
        pass_on(c, 0, right).wait_recv()
        snd[c, 2] = (own[c, 0] + rcv[c, 0].astype(F32)).astype(BF)
        pass_on(c, 2, right).start()
        pass_on(c, 1, left).wait_recv()
        snd[c, 5] = (own[c, 1] + rcv[c, 1].astype(F32)).astype(BF)
        pass_on(c, 5, left).start()
        return carry

    lax.fori_loop(0, NC, second, 0)

    def third(c, carry):
        @pl.when(c < NC)
        def _():
            for k in (3, 4, 2, 5):
                pass_on(c, k, right).wait_recv()
            o = 1 - y
            snd[c, 6] = (
                own[c, 2 + o] + rcv[c, 2 + o].astype(F32) + rcv[c, 4 + o].astype(F32)
            ).astype(BF)
            pass_on(c, 6, other_y).start()

        @pl.when(c >= 1)
        def _():
            e = c - 1
            pass_on(e, 6, other_y).wait_recv()
            rows = pl.ds(pl.multiple_of(e * R, R), R)
            branch = (own[e, 2 + y] + rcv[e, 2 + y].astype(F32)) + (
                rcv[e, 4 + y].astype(F32) + rcv[e, 6].astype(F32)
            )
            wide = [xs[j, rows, :].astype(F32) for j in range(S)]
            for i in range(S):
                v = mix_cols[rows, 4 + i : 5 + i] * branch
                for j in range(S):
                    k = 8 + 4 * i + j
                    v = v + mix_cols[rows, k : k + 1] * wide[j]
                out[i, rows, :] = v.astype(BF)

        return carry

    lax.fori_loop(0, NC + 1, third, 0)

    def drain(c, carry):
        for d in range(1, 4):
            back(c, d).wait_send()
        for k in range(7):
            pass_on(c, k, right).wait_send()
        return carry

    lax.fori_loop(0, NC, drain, 0)


def local(streams, doc_ids, mix_weight, mix_bias, attn_gain, w_qkv, w_out):
    xs = jnp.transpose(streams, (1, 0, 2))
    wmix = jnp.transpose(mix_weight, (0, 2, 1))
    wq = jnp.transpose(w_qkv, (1, 0, 2))
    vm = pl.BlockSpec(memory_space=VMEM)
    hbm = pl.BlockSpec(memory_space=pl.ANY)
    sds = jax.ShapeDtypeStruct
    att, mix_cols, counts = pl.pallas_call(
        first_kernel,
        name="gather_project",
        out_shape=(
            sds((16, NC, 3, R, HD), BF),
            sds((T, 128), F32),
            sds((8, 128), jnp.int32),
        ),
        in_specs=[vm, vm, vm, vm, vm, hbm],
        out_specs=(vm, vm, vm),
        scratch_shapes=[
            VMEM((3, D, W), BF),
            VMEM((NC, 8, R, W), BF),
            VMEM((4, NC, 3, R, HD), BF),
            VMEM((4, NC, 2, R, HD), BF),
            VMEM((R, D), BF),
            VMEM((8, T), F32),
            VMEM((7, 8, T), F32),
            VMEM((24, T), F32),
            VMEM((7, 24, T), F32),
            VMEM((15, 8, 128), jnp.int32),
            VMEM((8, 128), jnp.int32),
            VMEM((T, 128), F32),
            DMA((3,)),
            DMA((7,)), DMA((7,)),
            DMA((7,)), DMA((7,)),
            DMA((15,)), DMA((15,)),
            DMA((NC, 7)), DMA((NC, 7)),
            DMA((NC, 3)), DMA((NC, 3)),
            DMA((NC, 4)), DMA((NC, 4)),
            DMA((NC, 4)), DMA((NC, 4)),
            DMA((NC, 4)), DMA((NC, 4)),
            DMA((NC, 4)), DMA((NC, 4)),
        ],
        compiler_params=pltpu.CompilerParams(
            collective_id=0, has_side_effects=True, vmem_limit_bytes=56 * 1024 * 1024
        ),
    )(
        xs, doc_ids.reshape(4, 128), wmix, mix_bias.reshape(24, 1),
        attn_gain.reshape(1, D), wq,
    )
    ctx = pl.pallas_call(
        attention_kernel,
        name="attention",
        out_shape=sds((4, NC, R, HD), BF),
        in_specs=[vm, pl.BlockSpec(memory_space=pltpu.SMEM)],
        out_specs=vm,
        scratch_shapes=[VMEM((T, 128), F32), VMEM((T, 128), F32), VMEM((T, HD), F32)],
        compiler_params=pltpu.CompilerParams(vmem_limit_bytes=32 * 1024 * 1024),
    )(att, counts)
    out = pl.pallas_call(
        last_kernel,
        name="project_out",
        out_shape=sds((S, T, W), BF),
        in_specs=[vm, vm, vm, hbm],
        out_specs=vm,
        scratch_shapes=[
            VMEM((W, D), BF),
            VMEM((4, NC, R, HD), BF),
            VMEM((NC, 7, R, W), BF),
            VMEM((NC, 4, R, W), F32),
            VMEM((NC, 7, R, W), BF),
            DMA(()),
            DMA((NC, 3)), DMA((NC, 3)),
            DMA((NC, 7)), DMA((NC, 7)),
        ],
        compiler_params=pltpu.CompilerParams(
            collective_id=1, has_side_effects=True, vmem_limit_bytes=48 * 1024 * 1024
        ),
    )(ctx, mix_cols, xs, w_out)
    return jnp.transpose(out, (1, 0, 2))


def solution(mesh):
    in_specs = (
        P("seq", None, "tp"),
        P("seq"),
        P(None, "tp", None),
        P(),
        P(),
        P(None, None, "tp"),
        P("tp", None),
    )
    return jax.shard_map(
        local, mesh=mesh, in_specs=in_specs, out_specs=P("seq", None, "tp"), check_vma=False
    )
```

```python
import jax
import jax.numpy as jnp
from jax import lax
from jax.experimental import pallas as pl
from jax.experimental.pallas import tpu as pltpu
from jax.sharding import PartitionSpec as P

D = 4096
HD = 128
S = 4
ROUNDS = 20
EPS = 1e-6
T = 512
W = 512
NC = 8
AHEAD = 3
R = T // NC
F32 = jnp.float32
BF = jnp.bfloat16
MESH = pl.DeviceIdType.MESH
NT = (((1,), (1,)), ((), ()))
NEG = -1e30
VMEM = pltpu.VMEM
DMA = pltpu.SemaphoreType.DMA


def where_am_i():
    seq = lax.axis_index("seq")
    tp = lax.axis_index("tp")
    return seq, tp


def remote(src, dst, ssem, rsem, seq, tp):
    return pltpu.make_async_remote_copy(
        src_ref=src, dst_ref=dst, send_sem=ssem, recv_sem=rsem,
        device_id={"seq": seq, "tp": tp}, device_id_type=MESH,
    )


def greet(peers):
    barrier = pltpu.get_barrier_semaphore()
    for seq, tp in peers:
        pl.semaphore_signal(barrier, inc=1, device_id={"seq": seq, "tp": tp}, device_id_type=MESH)
    return lambda: pl.semaphore_wait(barrier, len(peers))


def columns(rows8):
    k = rows8.shape[0]
    if k < 128:
        rows8 = jnp.concatenate([rows8, jnp.zeros((128 - k, rows8.shape[1]), F32)], axis=0)
    return rows8.T


def balanced(e0, e1):
    sub = lax.broadcasted_iota(jnp.int32, e0.shape, 0)
    even, low = sub % 2 == 0, sub % 4 < 2

    def row_total(e):
        u = e + jnp.where(even, pltpu.roll(e, 7, 0), pltpu.roll(e, 1, 0))
        return u + jnp.where(low, pltpu.roll(u, 6, 0), pltpu.roll(u, 2, 0))

    def one_round(_, pair):
        e0, e1 = pair
        e0 = e0 / row_total(e0)
        e1 = e1 / row_total(e1)
        t = e0 + e1
        t = t + pltpu.roll(t, 4, 0)
        return e0 / t, e1 / t

    return lax.fori_loop(0, ROUNDS, one_round, (e0, e1))


def first_kernel(
    x_hbm, docs_hbm, wmix_hbm, bias_hbm, gain_hbm, w_hbm,
    att, mix_cols, counts,
    xraw, xs, docs, wmix, bias, gain,
    wbuf, g, sb, gained, unow, urecv, nall, nrecv, csend, crecv, pre_cols,
    x_sem, i_sem, w_sem, u_ss, u_rs, n_ss, n_rs, c_ss, c_rs, g_ss, g_rs, a_ss, a_rs, o_sem,
    sib_ss, sib_rs, x_ss, x_rs, sib2_ss, sib2_rs,
):
    seq, tp = where_am_i()
    yhi, z, core = seq // 8, (seq // 2) % 4, seq % 2
    x, y = tp // 2, tp % 2
    sibling, mirror = seq + 1 - 2 * core, (seq + 8) % 16
    tp_peers = [(seq, (tp + r) % 8) for r in range(1, 8)]
    z_peers = [yhi * 8 + ((z + d) % 4) * 2 + core for d in range(1, 4)]
    entered = greet(tp_peers + [(p, tp) for p in z_peers] + [(sibling, tp), (mirror, tp)])

    small = [
        pltpu.make_async_copy(a, b, i_sem.at[i])
        for i, (a, b) in enumerate(
            ((wmix_hbm, wmix), (docs_hbm, docs), (bias_hbm, bias), (gain_hbm, gain))
        )
    ]
    parts_of_x = [
        pltpu.make_async_copy(x_hbm.at[pl.ds(q * 128, 128)], xraw.at[pl.ds(q * 128, 128)], x_sem.at[q])
        for q in range(4)
    ]
    small[0].start()
    for q in range(4):
        parts_of_x[q].start()
    for k in range(1, 4):
        small[k].start()

    def wcopy(i):
        return pltpu.make_async_copy(w_hbm.at[i], wbuf.at[i], w_sem.at[i])

    for i in range(3):
        wcopy(i).start()

    small[0].wait()
    parts = []
    for s in range(S):
        w = jnp.concatenate([wmix[s], jnp.zeros((8, W), F32)], axis=0)
        hi = w.astype(BF).astype(F32)
        mid = (w - hi).astype(BF).astype(F32)
        low = (w - hi) - mid
        parts.append(jnp.concatenate([hi, mid, low], axis=0).astype(BF))
    sub = lax.broadcasted_iota(jnp.int32, (8, 128), 0)
    for q in range(4):
        rows = slice(q * 128, (q + 1) * 128)
        parts_of_x[q].wait()
        xs[:, rows, :] = jnp.swapaxes(xraw[rows], 0, 1)
        acc = jnp.zeros((128, 128), F32)
        logits = jnp.zeros((32, 128), F32)
        for s in range(S):
            xv = xs[s, rows, :]
            got = lax.dot_general(parts[s], xv, NT, preferred_element_type=F32)
            logits = logits + (got[0:32] + (got[32:64] + got[64:96]))
            x32 = xv.astype(F32)
            sq = x32 * x32
            acc = acc + ((sq[:, 0:128] + sq[:, 128:256]) + (sq[:, 256:384] + sq[:, 384:512]))
        squares = jnp.sum(acc.T, axis=0, keepdims=True)
        unow[:, rows] = jnp.where(
            sub < 4, logits[0:8], jnp.where(sub == 4, jnp.broadcast_to(squares, (8, 128)), 0.0)
        )
        nall[:, rows] = logits[0:24]

    entered()
    for r, (sq_, tp_) in enumerate(tp_peers):
        remote(unow, urecv.at[r], u_ss.at[r], u_rs.at[r], sq_, tp_).start()

    for k in range(1, 4):
        small[k].wait()
    dv = docs[...]
    cv = jnp.zeros((8, 128), jnp.int32)
    for k in range(1, 4):
        n = jnp.sum(jnp.where(dv < k, 1, 0), axis=1, keepdims=True)
        n = jnp.sum(n, axis=0, keepdims=True)
        cv = jnp.where(sub == k, jnp.broadcast_to(n, (8, 128)), cv)
    csend[0] = cv
    diag = lax.broadcasted_iota(jnp.int32, (24, 24), 0) == lax.broadcasted_iota(jnp.int32, (24, 24), 1)
    bias_col = jnp.sum(jnp.where(diag, jnp.broadcast_to(bias[...], (24, 24)), 0.0), axis=1, keepdims=True)

    def count_to(level, k, to):
        return remote(csend.at[level], crecv.at[k], c_ss.at[k], c_rs.at[k], to, tp)

    total = unow[...]
    for r, (sq_, tp_) in enumerate(tp_peers):
        remote(unow, urecv.at[r], u_ss.at[r], u_rs.at[r], sq_, tp_).wait_recv()
        total = total + urecv[r]
    inv_rms = lax.rsqrt(total[4:5] / (S * D) + EPS)
    pre = 1.0 / (1.0 + jnp.exp(-(total * inv_rms + bias_col[0:8])))
    pre_cols[...] = columns(pre)

    right = ((x + 1) % 4) * 2 + y
    left = ((x + 3) % 4) * 2 + y
    other_y = x * 2 + 1 - y
    b_p = other_y
    b_l0, b_l1 = left, ((x + 3) % 4) * 2 + 1 - y
    b_r0, b_r1 = right, ((x + 1) % 4) * 2 + 1 - y
    b_f0, b_f1 = ((x + 2) % 4) * 2 + y, ((x + 2) % 4) * 2 + 1 - y

    def move(c, k, blk, role, to):
        return remote(g.at[c, blk], g.at[c, blk], g_ss.at[c, k], g_rs.at[c, role], seq, to)

    def arrived(c, role, blk):
        move(c, 0, blk, role, right).wait_recv()

    def make_chunk(c):
        rows = slice(c * R, (c + 1) * R)
        v = pre_cols[rows, 0:1] * xs[0, rows, :].astype(F32)
        for s in range(1, S):
            v = v + pre_cols[rows, s : s + 1] * xs[s, rows, :].astype(F32)
        g[c, tp] = v.astype(BF)

    def send_chunk(c):
        move(c, 2, tp, 0, other_y).start()
        move(c, 0, tp, 1, right).start()
        move(c, 1, tp, 3, left).start()

    make_chunk(0)
    for c in range(NC):
        if c + 1 < NC:
            make_chunk(c + 1)
        if c < AHEAD:
            send_chunk(c)
    for d in range(3):
        count_to(0, d, z_peers[d]).start()
    for i in range(3):
        wcopy(i).wait()

    def block_of(half, d):
        return half * 8 + ((z + 4 - d) % 4) * 2 + core

    def spread(c, d):
        return remote(
            sb.at[(z + d) % 4, c], att.at[seq, c], a_ss.at[c, d - 1], a_rs.at[c, d - 1], z_peers[d - 1], tp,
        )

    def spread_in(c, d):
        remote(
            sb.at[z, c], att.at[block_of(yhi, d), c], a_ss.at[c, d - 1], a_rs.at[c, d - 1], z_peers[d - 1], tp
        ).wait_recv()

    def kept(c):
        return pltpu.make_async_copy(sb.at[z, c], att.at[seq, c], o_sem.at[c])

    def kv(c, d):
        return sb.at[z, c, pl.ds(0, 2)] if d == 0 else att.at[block_of(yhi, d), c, pl.ds(0, 2)]

    def twin(c, d):
        dst = att.at[block_of(yhi, d), c, pl.ds(0, 2)]
        return remote(kv(c, d), dst, sib_ss.at[c, d], sib_rs.at[c, d], sibling, tp)

    def twin_in(c, d):
        dst = att.at[yhi * 8 + ((z + 4 - d) % 4) * 2 + 1 - core, c, pl.ds(0, 2)]
        return remote(kv(c, d), dst, sib_ss.at[c, d], sib_rs.at[c, d], sibling, tp)

    def cross(c, d):
        dst = att.at[block_of(0, d), c, pl.ds(0, 2)]
        return remote(kv(c, d), dst, x_ss.at[c, d], x_rs.at[c, d], mirror, tp)

    def twin2(c, d):
        ref = att.at[block_of(0, d), c, pl.ds(0, 2)]
        return remote(ref, ref, sib2_ss.at[c, d], sib2_rs.at[c, d], sibling, tp)

    def twin2_in(c, d):
        dst = att.at[((z + 4 - d) % 4) * 2 + 1 - core, c, pl.ds(0, 2)]
        return remote(dst, dst, sib2_ss.at[c, d], sib2_rs.at[c, d], sibling, tp)

    def step(i, carry):
        @pl.when(i + AHEAD < NC)
        def _():
            send_chunk(i + AHEAD)

        @pl.when(i < NC)
        def _():
            arrived(i, 0, b_p)
            move(i, 3, b_p, 2, right).start()
            move(i, 4, b_p, 4, left).start()
            arrived(i, 1, b_l0)
            move(i, 5, b_l0, 5, right).start()

        @pl.when((i >= 1) & (i <= NC))
        def _():
            arrived(i - 1, 4, b_r1)
            move(i - 1, 6, b_r1, 6, left).start()

        @pl.when((i >= 2) & (i <= NC + 1))
        def _():
            c = i - 2
            arrived(c, 2, b_l1)
            arrived(c, 3, b_r0)
            arrived(c, 5, b_f0)
            arrived(c, 6, b_f1)
            ss = jnp.zeros((R, 128), F32)
            for b in range(8):
                g32 = g[c, b].astype(F32)
                q = g32 * g32
                ss = ss + ((q[:, 0:128] + q[:, 128:256]) + (q[:, 256:384] + q[:, 384:512]))
                gained[:, b * W : (b + 1) * W] = (g32 * gain[:, b * W : (b + 1) * W]).astype(BF)
            norm = lax.rsqrt(jnp.sum(ss, axis=1, keepdims=True) / D + EPS)
            lhs = gained[...]
            for slot, third in ((0, 1), (1, 2), (2, 0)):
                acc = jnp.dot(lhs, wbuf[third], preferred_element_type=F32)
                out = (acc * norm).astype(BF)
                for h in range(4):
                    sb[h, c, slot] = out[:, h * HD : (h + 1) * HD]
            for d in (2, 1, 3):
                spread(c, d).start()
            kept(c).start()

        @pl.when((i >= 3) & (i <= NC + 2))
        def _():
            c = i - 3
            for d in range(4):
                if d:
                    spread_in(c, d)

                @pl.when(yhi == 0)
                def _():
                    cross(c, d).start()

                twin(c, d).start()

        @pl.when((i >= 5) & (yhi == 1))
        def _():
            for d in range(4):
                cross(i - 5, d).wait_recv()
                twin2(i - 5, d).start()

        @pl.when(i == NC)
        def _():
            for r, (sq_, tp_) in enumerate(tp_peers):
                remote(nall, nrecv.at[r], n_ss.at[r], n_rs.at[r], sq_, tp_).start()

        @pl.when(i == 3)
        def _():
            v = csend[0]
            for d in range(3):
                count_to(0, d, z_peers[d]).wait_recv()
                v = v + crecv[d]
            csend[1] = v

        @pl.when(i == 4)
        def _():
            count_to(1, 3, sibling).start()

        @pl.when(i == 5)
        def _():
            count_to(1, 3, sibling).wait_recv()
            csend[2] = csend[1] + crecv[3]

        @pl.when(i == 6)
        def _():
            count_to(2, 4, mirror).start()

        return carry

    lax.fori_loop(0, NC + 3, step, 0)

    count_to(2, 4, mirror).wait_recv()
    counts[...] = csend[2] + crecv[4]
    ztot = nall[...]
    for r, (sq_, tp_) in enumerate(tp_peers):
        remote(nall, nrecv.at[r], n_ss.at[r], n_rs.at[r], sq_, tp_).wait_recv()
        ztot = ztot + nrecv[r]
    ztot = ztot * inv_rms + bias_col
    post = 2.0 / (1.0 + jnp.exp(-ztot[0:8]))
    e0, e1 = balanced(jnp.exp(ztot[8:16]), jnp.exp(ztot[16:24]))
    mix_cols[...] = columns(jnp.concatenate([post, e0, e1], axis=0))

    @pl.when(yhi == 1)
    def _():
        def tail(c, carry):
            for d in range(4):
                cross(c, d).wait_recv()
                twin2(c, d).start()
            return carry

        lax.fori_loop(NC - 2, NC, tail, 0)

    for r, (sq_, tp_) in enumerate(tp_peers):
        remote(unow, urecv.at[r], u_ss.at[r], u_rs.at[r], sq_, tp_).wait_send()
        remote(nall, nrecv.at[r], n_ss.at[r], n_rs.at[r], sq_, tp_).wait_send()
    for d in range(3):
        count_to(0, d, z_peers[d]).wait_send()
    count_to(1, 3, sibling).wait_send()
    count_to(2, 4, mirror).wait_send()

    def drain(c, carry):
        for k in range(7):
            move(c, k, tp, 0, right).wait_send()
        kept(c).wait()
        for d in range(1, 4):
            spread(c, d).wait_send()
        for d in range(4):
            twin(c, d).wait_send()
            twin_in(c, d).wait_recv()

        @pl.when(yhi == 0)
        def _():
            for d in range(4):
                cross(c, d).wait_send()

        @pl.when(yhi == 1)
        def _():
            for d in range(4):
                twin2(c, d).wait_send()
                twin2_in(c, d).wait_recv()

        return carry

    lax.fori_loop(0, NC, drain, 0)


def attention_kernel(att_hbm, cnt_hbm, ctx, att, cnt, m_ref, l_ref, acc_ref, c_sem, kv_sem, q_sem):
    seq = lax.axis_index("seq")
    yhi, core = seq // 8, seq % 2
    counts_in = pltpu.make_async_copy(cnt_hbm, cnt, c_sem)
    counts_in.start()

    def q_in(qi):
        qb = yhi * 8 + qi * 2 + core
        return pltpu.make_async_copy(att_hbm.at[qb, :, 2], att.at[qb, :, 2], q_sem.at[qi])

    def kv_in(kb):
        return pltpu.make_async_copy(
            att_hbm.at[kb, :, pl.ds(0, 2)], att.at[kb, :, pl.ds(0, 2)], kv_sem.at[kb]
        )

    q_in(0).start()
    counts_in.wait()
    starts = [cnt[k, 0] for k in range(1, 4)]
    scale = HD ** (-0.5) * 1.4426950408889634

    def start_of(p):
        v = p * 0
        for c in starts:
            v = jnp.where(c <= p, jnp.maximum(v, c), v)
        return v

    first_needed = start_of((yhi * 8 + core) * T) // T

    def fetch(kb, c):
        kv_in(kb).start()
        return c

    def land(kb, c):
        kv_in(kb).wait()
        return c

    lax.fori_loop(first_needed, yhi * 8 + core + 1, fetch, 0)
    for qi in range(1, 4):
        q_in(qi).start()
    lax.fori_loop(yhi * 8 + core + 1, yhi * 8 + core + 7, fetch, 0)

    def one_query_block(qi, carry):
        qb = yhi * 8 + qi * 2 + core
        lax.fori_loop(jnp.where(qi == 0, first_needed, qb - 1), qb + 1, land, 0)
        q_in(qi).wait()
        q = att[qb, :, 2].reshape(T, HD)
        first = start_of(qb * T)
        last = start_of(qb * T + T - 1)
        lo = first // T
        mid = jnp.minimum((last + T - 1) // T, qb)
        qpos = qb * T + lax.broadcasted_iota(jnp.int32, (T, 1), 0)
        qstart = start_of(qpos)
        m_ref[...] = jnp.full((T, 128), NEG, F32)
        l_ref[...] = jnp.zeros((T, 128), F32)
        acc_ref[...] = jnp.zeros((T, HD), F32)

        def block(kb, masked):
            k = att[kb, :, 0].reshape(T, HD)
            v = att[kb, :, 1].reshape(T, HD)
            s = lax.dot_general(q, k, NT, preferred_element_type=F32)
            if masked:
                kpos = kb * T + lax.broadcasted_iota(jnp.int32, (1, T), 1)
                ok = (kpos <= qpos) & (kpos >= qstart)
                s = jnp.where(ok, s, NEG)
            top = jnp.maximum(
                jnp.maximum(s[:, 0:128], s[:, 128:256]), jnp.maximum(s[:, 256:384], s[:, 384:512])
            )
            m_old = m_ref[:, 0:1]
            m_new = jnp.maximum(m_old, jnp.max(top, axis=1, keepdims=True))
            p = jnp.exp2((s - m_new) * scale)
            if masked:
                p = jnp.where(ok, p, 0.0)
            alpha = jnp.exp2((m_old - m_new) * scale)
            part = (p[:, 0:128] + p[:, 128:256]) + (p[:, 256:384] + p[:, 384:512])
            l_ref[...] = l_ref[...] * alpha + part
            acc_ref[...] = acc_ref[...] * alpha + jnp.dot(p.astype(BF), v, preferred_element_type=F32)
            m_ref[...] = jnp.broadcast_to(m_new, (T, 128))

        def with_mask(kb, c):
            block(kb, True)
            return c

        def without(kb, c):
            block(kb, False)
            return c

        lax.fori_loop(lo, mid, with_mask, 0)
        lax.fori_loop(mid, qb, without, 0)
        lax.fori_loop(qb, qb + 1, with_mask, 0)
        out = acc_ref[...] / jnp.sum(l_ref[...], axis=1, keepdims=True)
        ctx[qi] = out.astype(BF).reshape(NC, R, HD)
        return carry

    lax.fori_loop(0, 4, one_query_block, 0)


def last_kernel(
    ctx, mix_cols, x_hbm, w_hbm,
    out,
    xraw, wbuf, cbuf, snd, own, rcv,
    x_sem, w_sem, z_ss, z_rs, s_ss, s_rs,
):
    seq, tp = where_am_i()
    yhi, z, core = seq // 8, (seq // 2) % 4, seq % 2
    x, y = tp // 2, tp % 2
    right = ((x + 1) % 4) * 2 + y
    left = ((x + 3) % 4) * 2 + y
    other_y = x * 2 + 1 - y
    z_peers = [yhi * 8 + ((z + d) % 4) * 2 + core for d in range(1, 4)]
    entered = greet([(p, tp) for p in z_peers] + [(seq, right), (seq, left), (seq, other_y)])
    wcopy = pltpu.make_async_copy(w_hbm, wbuf, w_sem)
    wcopy.start()
    xcopy = pltpu.make_async_copy(x_hbm, xraw, x_sem)
    xcopy.start()
    entered()

    def back(c, d):
        to_z = (z + d) % 4
        return remote(
            ctx.at[to_z, c], cbuf.at[z, c], z_ss.at[c, d - 1], z_rs.at[c, d - 1], z_peers[d - 1], tp
        )

    def back_in(c, d):
        from_z = (z + 4 - d) % 4
        remote(
            ctx.at[z, c], cbuf.at[from_z, c], z_ss.at[c, d - 1], z_rs.at[c, d - 1], z_peers[d - 1], tp
        ).wait_recv()

    for c in range(NC):
        for d in (2, 1, 3):
            back(c, d).start()
    cbuf[z] = ctx[z]
    wcopy.wait()

    def pass_on(c, k, to):
        return remote(snd.at[c, k], rcv.at[c, k], s_ss.at[c, k], s_rs.at[c, k], seq, to)

    b0, b1 = ((x + 1) % 4) * 2, ((x + 3) % 4) * 2
    bf = ((x + 2) % 4) * 2

    def project(c, carry):
        for d in range(1, 4):
            back_in(c, d)
        lhs = jnp.concatenate([cbuf[h, c] for h in range(4)], axis=1)

        def term(b):
            cols = pl.ds(pl.multiple_of(b * W, W), W)
            return jnp.dot(lhs, wbuf[:, cols], preferred_element_type=F32)

        snd[c, 0] = term(bf).astype(BF)
        snd[c, 1] = term(bf + 1).astype(BF)
        pass_on(c, 0, right).start()
        pass_on(c, 1, left).start()
        snd[c, 3] = term(b0 + 1).astype(BF)
        snd[c, 4] = term(b1).astype(BF)
        pass_on(c, 3, right).start()
        pass_on(c, 4, left).start()
        own[c, 0] = term(b0)
        own[c, 1] = term(b1 + 1)
        own[c, 2] = term(x * 2)
        own[c, 3] = term(x * 2 + 1)
        return carry

    lax.fori_loop(0, NC, project, 0)

    def second(c, carry):
        pass_on(c, 0, right).wait_recv()
        snd[c, 2] = (own[c, 0] + rcv[c, 0].astype(F32)).astype(BF)
        pass_on(c, 2, right).start()
        pass_on(c, 1, left).wait_recv()
        snd[c, 5] = (own[c, 1] + rcv[c, 1].astype(F32)).astype(BF)
        pass_on(c, 5, left).start()
        return carry

    lax.fori_loop(0, NC, second, 0)
    xcopy.wait()

    def third(c, carry):
        @pl.when(c < NC)
        def _():
            for k in (3, 4, 2, 5):
                pass_on(c, k, right).wait_recv()
            o = 1 - y
            snd[c, 6] = (
                own[c, 2 + o] + rcv[c, 2 + o].astype(F32) + rcv[c, 4 + o].astype(F32)
            ).astype(BF)
            pass_on(c, 6, other_y).start()

        @pl.when(c >= 1)
        def _():
            e = c - 1
            pass_on(e, 6, other_y).wait_recv()
            rows = pl.ds(pl.multiple_of(e * R, R), R)
            branch = (own[e, 2 + y] + rcv[e, 2 + y].astype(F32)) + (
                rcv[e, 4 + y].astype(F32) + rcv[e, 6].astype(F32)
            )
            xv = jnp.swapaxes(xraw[rows], 0, 1)
            wide = [xv[j].astype(F32) for j in range(S)]
            new = []
            for i in range(S):
                v = mix_cols[rows, 4 + i : 5 + i] * branch
                for j in range(S):
                    k = 8 + 4 * i + j
                    v = v + mix_cols[rows, k : k + 1] * wide[j]
                new.append(v.astype(BF))
            out[rows] = jnp.swapaxes(jnp.stack(new, axis=0), 0, 1)

        return carry

    lax.fori_loop(0, NC + 1, third, 0)

    def drain(c, carry):
        for d in range(1, 4):
            back(c, d).wait_send()
        for k in range(7):
            pass_on(c, k, right).wait_send()
        return carry

    lax.fori_loop(0, NC, drain, 0)


def local(streams, doc_ids, mix_weight, mix_bias, attn_gain, w_qkv, w_out):
    wmix = jnp.transpose(mix_weight, (0, 2, 1))
    wq = jnp.transpose(w_qkv, (1, 0, 2))
    vm = pl.BlockSpec(memory_space=VMEM)
    hbm = pl.BlockSpec(memory_space=pl.ANY)
    sds = jax.ShapeDtypeStruct
    att, mix_cols, counts = pl.pallas_call(
        first_kernel,
        name="gather_project",
        out_shape=(
            sds((16, NC, 3, R, HD), BF),
            sds((T, 128), F32),
            sds((8, 128), jnp.int32),
        ),
        in_specs=[hbm] * 6,
        out_specs=(hbm, vm, vm),
        scratch_shapes=[
            VMEM((T, S, W), BF),
            VMEM((S, T, W), BF),
            VMEM((4, 128), jnp.int32),
            VMEM((S, 24, W), F32),
            VMEM((1, 24), F32),
            VMEM((1, D), F32),
            VMEM((3, D, W), BF),
            VMEM((NC, 8, R, W), BF),
            VMEM((4, NC, 3, R, HD), BF),
            VMEM((R, D), BF),
            VMEM((8, T), F32),
            VMEM((7, 8, T), F32),
            VMEM((24, T), F32),
            VMEM((7, 24, T), F32),
            VMEM((3, 8, 128), jnp.int32),
            VMEM((5, 8, 128), jnp.int32),
            VMEM((T, 128), F32),
            DMA((4,)),
            DMA((4,)),
            DMA((3,)),
            DMA((7,)), DMA((7,)),
            DMA((7,)), DMA((7,)),
            DMA((5,)), DMA((5,)),
            DMA((NC, 7)), DMA((NC, 7)),
            DMA((NC, 3)), DMA((NC, 3)),
            DMA((NC,)),
            DMA((NC, 4)), DMA((NC, 4)),
            DMA((NC, 4)), DMA((NC, 4)),
            DMA((NC, 4)), DMA((NC, 4)),
        ],
        compiler_params=pltpu.CompilerParams(
            collective_id=0, has_side_effects=True, vmem_limit_bytes=60 * 1024 * 1024
        ),
    )(
        streams, doc_ids.reshape(4, 128), wmix, mix_bias.reshape(1, 24), attn_gain.reshape(1, D), wq,
    )
    ctx = pl.pallas_call(
        attention_kernel,
        name="attention",
        out_shape=sds((4, NC, R, HD), BF),
        in_specs=[hbm, hbm],
        out_specs=vm,
        scratch_shapes=[
            VMEM((16, NC, 3, R, HD), BF),
            pltpu.SMEM((8, 128), jnp.int32),
            VMEM((T, 128), F32), VMEM((T, 128), F32), VMEM((T, HD), F32),
            DMA(()), DMA((16,)), DMA((4,)),
        ],
        compiler_params=pltpu.CompilerParams(vmem_limit_bytes=60 * 1024 * 1024),
    )(att, counts)
    return pl.pallas_call(
        last_kernel,
        name="project_out",
        out_shape=sds((T, S, W), BF),
        in_specs=[vm, vm, hbm, hbm],
        out_specs=vm,
        scratch_shapes=[
            VMEM((T, S, W), BF),
            VMEM((W, D), BF),
            VMEM((4, NC, R, HD), BF),
            VMEM((NC, 7, R, W), BF),
            VMEM((NC, 4, R, W), F32),
            VMEM((NC, 7, R, W), BF),
            DMA(()),
            DMA(()),
            DMA((NC, 3)), DMA((NC, 3)),
            DMA((NC, 7)), DMA((NC, 7)),
        ],
        compiler_params=pltpu.CompilerParams(
            collective_id=1, has_side_effects=True, vmem_limit_bytes=60 * 1024 * 1024
        ),
    )(ctx, mix_cols, streams, w_out)


def solution(mesh):
    in_specs = (
        P("seq", None, "tp"),
        P("seq"),
        P(None, "tp", None),
        P(),
        P(),
        P(None, None, "tp"),
        P("tp", None),
    )
    return jax.shard_map(
        local, mesh=mesh, in_specs=in_specs, out_specs=P("seq", None, "tp"), check_vma=False
    )
```

```python
import jax
import jax.numpy as jnp
from jax import lax
from jax.experimental import pallas as pl
from jax.experimental.pallas import tpu as pltpu
from jax.sharding import PartitionSpec as P

D = 4096
HD = 128
S = 4
ROUNDS = 20
EPS = 1e-6
T = 512
W = 512
NC = 8
NO = 4
RO = T // NO
HALF = 256
AHEAD = 3
R = T // NC
F32 = jnp.float32
BF = jnp.bfloat16
MESH = pl.DeviceIdType.MESH
NT = (((1,), (1,)), ((), ()))
NEG = -1e30
VMEM = pltpu.VMEM
DMA = pltpu.SemaphoreType.DMA


def where_am_i():
    seq = lax.axis_index("seq")
    tp = lax.axis_index("tp")
    return seq, tp


def remote(src, dst, ssem, rsem, seq, tp):
    return pltpu.make_async_remote_copy(
        src_ref=src, dst_ref=dst, send_sem=ssem, recv_sem=rsem,
        device_id={"seq": seq, "tp": tp}, device_id_type=MESH,
    )


def greet(peers):
    barrier = pltpu.get_barrier_semaphore()
    for seq, tp in peers:
        pl.semaphore_signal(barrier, inc=1, device_id={"seq": seq, "tp": tp}, device_id_type=MESH)
    return lambda: pl.semaphore_wait(barrier, len(peers))


def columns(rows8):
    k = rows8.shape[0]
    if k < 128:
        rows8 = jnp.concatenate([rows8, jnp.zeros((128 - k, rows8.shape[1]), F32)], axis=0)
    return rows8.T


def balanced(e0, e1):
    sub = lax.broadcasted_iota(jnp.int32, e0.shape, 0)
    even, low = sub % 2 == 0, sub % 4 < 2

    def row_total(e):
        u = e + jnp.where(even, pltpu.roll(e, 7, 0), pltpu.roll(e, 1, 0))
        return u + jnp.where(low, pltpu.roll(u, 6, 0), pltpu.roll(u, 2, 0))

    def one_round(_, pair):
        e0, e1 = pair
        e0 = e0 / row_total(e0)
        e1 = e1 / row_total(e1)
        t = e0 + e1
        t = t + pltpu.roll(t, 4, 0)
        return e0 / t, e1 / t

    return lax.fori_loop(0, ROUNDS, one_round, (e0, e1))


def first_kernel(
    x_hbm, docs_hbm, wmix_hbm, bias_hbm, gain_hbm, w_hbm,
    att, mix_cols, counts,
    xraw, xs, docs, wmix, bias, gain,
    wbuf, g, sb, gained, unow, urecv, nall, nrecv, csend, crecv, pre_cols,
    x_sem, i_sem, w_sem, u_ss, u_rs, n_ss, n_rs, c_ss, c_rs, g_ss, g_rs, a_ss, a_rs, o_sem,
    sib_ss, sib_rs, x_ss, x_rs, sib2_ss, sib2_rs,
):
    seq, tp = where_am_i()
    yhi, z, core = seq // 8, (seq // 2) % 4, seq % 2
    x, y = tp // 2, tp % 2
    sibling, mirror = seq + 1 - 2 * core, (seq + 8) % 16
    tp_peers = [(seq, (tp + r) % 8) for r in range(1, 8)]
    z_peers = [yhi * 8 + ((z + d) % 4) * 2 + core for d in range(1, 4)]
    entered = greet(tp_peers + [(p, tp) for p in z_peers] + [(sibling, tp), (mirror, tp)])

    small = [
        pltpu.make_async_copy(a, b, i_sem.at[i])
        for i, (a, b) in enumerate(
            ((wmix_hbm, wmix), (docs_hbm, docs), (bias_hbm, bias), (gain_hbm, gain))
        )
    ]
    parts_of_x = [
        pltpu.make_async_copy(x_hbm.at[pl.ds(q * 128, 128)], xraw.at[pl.ds(q * 128, 128)], x_sem.at[q])
        for q in range(4)
    ]
    small[0].start()
    for q in range(4):
        parts_of_x[q].start()
    for k in range(1, 4):
        small[k].start()

    def wcopy(i):
        return pltpu.make_async_copy(w_hbm.at[i], wbuf.at[i], w_sem.at[i])

    small[0].wait()
    parts = []
    for s in range(S):
        w = jnp.concatenate([wmix[s], jnp.zeros((8, W), F32)], axis=0)
        hi = w.astype(BF).astype(F32)
        mid = (w - hi).astype(BF).astype(F32)
        low = (w - hi) - mid
        parts.append(jnp.concatenate([hi, mid, low], axis=0).astype(BF))
    sub = lax.broadcasted_iota(jnp.int32, (8, 128), 0)
    for q in range(4):
        rows = slice(q * 128, (q + 1) * 128)
        parts_of_x[q].wait()
        if q == 3:
            for i in range(3):
                wcopy(i).start()
        xs[:, rows, :] = jnp.swapaxes(xraw[rows], 0, 1)
        acc = jnp.zeros((128, 128), F32)
        logits = jnp.zeros((32, 128), F32)
        for s in range(S):
            xv = xs[s, rows, :]
            got = lax.dot_general(parts[s], xv, NT, preferred_element_type=F32)
            logits = logits + (got[0:32] + (got[32:64] + got[64:96]))
            x32 = xv.astype(F32)
            sq = x32 * x32
            acc = acc + ((sq[:, 0:128] + sq[:, 128:256]) + (sq[:, 256:384] + sq[:, 384:512]))
        squares = jnp.sum(acc.T, axis=0, keepdims=True)
        unow[:, rows] = jnp.where(
            sub < 4, logits[0:8], jnp.where(sub == 4, jnp.broadcast_to(squares, (8, 128)), 0.0)
        )
        nall[:, rows] = logits[0:24]

    entered()
    for r, (sq_, tp_) in enumerate(tp_peers):
        remote(unow, urecv.at[r], u_ss.at[r], u_rs.at[r], sq_, tp_).start()

    for k in range(1, 4):
        small[k].wait()
    dv = docs[...]
    cv = jnp.zeros((8, 128), jnp.int32)
    for k in range(1, 4):
        n = jnp.sum(jnp.where(dv < k, 1, 0), axis=1, keepdims=True)
        n = jnp.sum(n, axis=0, keepdims=True)
        cv = jnp.where(sub == k, jnp.broadcast_to(n, (8, 128)), cv)
    csend[0] = cv
    diag = lax.broadcasted_iota(jnp.int32, (24, 24), 0) == lax.broadcasted_iota(jnp.int32, (24, 24), 1)
    bias_col = jnp.sum(jnp.where(diag, jnp.broadcast_to(bias[...], (24, 24)), 0.0), axis=1, keepdims=True)

    def count_to(level, k, to):
        return remote(csend.at[level], crecv.at[k], c_ss.at[k], c_rs.at[k], to, tp)

    total = unow[...]
    for r, (sq_, tp_) in enumerate(tp_peers):
        remote(unow, urecv.at[r], u_ss.at[r], u_rs.at[r], sq_, tp_).wait_recv()
        total = total + urecv[r]
    inv_rms = lax.rsqrt(total[4:5] / (S * D) + EPS)
    pre = 1.0 / (1.0 + jnp.exp(-(total * inv_rms + bias_col[0:8])))
    pre_cols[...] = columns(pre)

    right = ((x + 1) % 4) * 2 + y
    left = ((x + 3) % 4) * 2 + y
    other_y = x * 2 + 1 - y
    b_p = other_y
    b_l0, b_l1 = left, ((x + 3) % 4) * 2 + 1 - y
    b_r0, b_r1 = right, ((x + 1) % 4) * 2 + 1 - y
    b_f0, b_f1 = ((x + 2) % 4) * 2 + y, ((x + 2) % 4) * 2 + 1 - y

    def move(c, k, blk, role, to):
        return remote(g.at[c, blk], g.at[c, blk], g_ss.at[c, k], g_rs.at[c, role], seq, to)

    def arrived(c, role, blk):
        move(c, 0, blk, role, right).wait_recv()

    def make_chunk(c):
        rows = slice(c * R, (c + 1) * R)
        v = pre_cols[rows, 0:1] * xs[0, rows, :].astype(F32)
        for s in range(1, S):
            v = v + pre_cols[rows, s : s + 1] * xs[s, rows, :].astype(F32)
        g[c, tp] = v.astype(BF)

    def send_chunk(c):
        move(c, 2, tp, 0, other_y).start()
        move(c, 0, tp, 1, right).start()
        move(c, 1, tp, 3, left).start()

    make_chunk(0)
    for c in range(NC):
        if c + 1 < NC:
            make_chunk(c + 1)
        if c < AHEAD:
            send_chunk(c)
    for d in range(3):
        count_to(0, d, z_peers[d]).start()
    for i in range(3):
        wcopy(i).wait()

    def block_of(half, d):
        return half * 8 + ((z + 4 - d) % 4) * 2 + core

    def spread(c, d):
        return remote(
            sb.at[(z + d) % 4, c], att.at[seq, c], a_ss.at[c, d - 1], a_rs.at[c, d - 1], z_peers[d - 1], tp,
        )

    def spread_in(c, d):
        remote(
            sb.at[z, c], att.at[block_of(yhi, d), c], a_ss.at[c, d - 1], a_rs.at[c, d - 1], z_peers[d - 1], tp
        ).wait_recv()

    def kept(c):
        return pltpu.make_async_copy(sb.at[z, c], att.at[seq, c], o_sem.at[c])

    def kv(c, d):
        return sb.at[z, c, pl.ds(0, 2)] if d == 0 else att.at[block_of(yhi, d), c, pl.ds(0, 2)]

    def twin(c, d):
        dst = att.at[block_of(yhi, d), c, pl.ds(0, 2)]
        return remote(kv(c, d), dst, sib_ss.at[c, d], sib_rs.at[c, d], sibling, tp)

    def twin_in(c, d):
        dst = att.at[yhi * 8 + ((z + 4 - d) % 4) * 2 + 1 - core, c, pl.ds(0, 2)]
        return remote(kv(c, d), dst, sib_ss.at[c, d], sib_rs.at[c, d], sibling, tp)

    def cross(c, d):
        dst = att.at[block_of(0, d), c, pl.ds(0, 2)]
        return remote(kv(c, d), dst, x_ss.at[c, d], x_rs.at[c, d], mirror, tp)

    def twin2(c, d):
        ref = att.at[block_of(0, d), c, pl.ds(0, 2)]
        return remote(ref, ref, sib2_ss.at[c, d], sib2_rs.at[c, d], sibling, tp)

    def twin2_in(c, d):
        dst = att.at[((z + 4 - d) % 4) * 2 + 1 - core, c, pl.ds(0, 2)]
        return remote(dst, dst, sib2_ss.at[c, d], sib2_rs.at[c, d], sibling, tp)

    def hand_on(i):
        arrived(i, 0, b_p)
        move(i, 3, b_p, 2, right).start()
        move(i, 4, b_p, 4, left).start()

    hand_on(0)

    def step(i, carry):
        @pl.when(i + AHEAD < NC)
        def _():
            send_chunk(i + AHEAD)

        @pl.when(i + 1 < NC)
        def _():
            hand_on(i + 1)

        @pl.when(i < NC)
        def _():
            arrived(i, 1, b_l0)
            move(i, 5, b_l0, 5, right).start()
            arrived(i, 4, b_r1)
            move(i, 6, b_r1, 6, left).start()

        @pl.when((i >= 3) & (i <= NC + 2))
        def _():
            c = i - 3
            for d in range(4):
                if d:
                    spread_in(c, d)

                @pl.when(yhi == 0)
                def _():
                    cross(c, d).start()

                twin(c, d).start()

        @pl.when((i >= 5) & (yhi == 1))
        def _():
            for d in range(4):
                cross(i - 5, d).wait_recv()
                twin2(i - 5, d).start()

        @pl.when((i >= 1) & (i <= NC))
        def _():
            c = i - 1
            arrived(c, 2, b_l1)
            arrived(c, 3, b_r0)
            arrived(c, 5, b_f0)
            arrived(c, 6, b_f1)
            ss = jnp.zeros((R, 128), F32)
            for b in range(8):
                g32 = g[c, b].astype(F32)
                q = g32 * g32
                ss = ss + ((q[:, 0:128] + q[:, 128:256]) + (q[:, 256:384] + q[:, 384:512]))
                gained[:, b * W : (b + 1) * W] = (g32 * gain[:, b * W : (b + 1) * W]).astype(BF)
            norm = lax.rsqrt(jnp.sum(ss, axis=1, keepdims=True) / D + EPS)
            lhs = gained[...]
            for slot, third in ((0, 1), (1, 2), (2, 0)):
                acc = jnp.dot(lhs, wbuf[third], preferred_element_type=F32)
                out = (acc * norm).astype(BF)
                for h in range(4):
                    sb[h, c, slot] = out[:, h * HD : (h + 1) * HD]
            for d in (2, 1, 3):
                spread(c, d).start()
            kept(c).start()

        @pl.when(i == NC)
        def _():
            for r, (sq_, tp_) in enumerate(tp_peers):
                remote(nall, nrecv.at[r], n_ss.at[r], n_rs.at[r], sq_, tp_).start()

        @pl.when(i == 3)
        def _():
            v = csend[0]
            for d in range(3):
                count_to(0, d, z_peers[d]).wait_recv()
                v = v + crecv[d]
            csend[1] = v

        @pl.when(i == 4)
        def _():
            count_to(1, 3, sibling).start()

        @pl.when(i == 5)
        def _():
            count_to(1, 3, sibling).wait_recv()
            csend[2] = csend[1] + crecv[3]

        @pl.when(i == 6)
        def _():
            count_to(2, 4, mirror).start()

        return carry

    lax.fori_loop(0, NC + 3, step, 0)

    count_to(2, 4, mirror).wait_recv()
    counts[...] = csend[2] + crecv[4]
    ztot = nall[...]
    for r, (sq_, tp_) in enumerate(tp_peers):
        remote(nall, nrecv.at[r], n_ss.at[r], n_rs.at[r], sq_, tp_).wait_recv()
        ztot = ztot + nrecv[r]
    ztot = ztot * inv_rms + bias_col
    post = 2.0 / (1.0 + jnp.exp(-ztot[0:8]))
    e0, e1 = balanced(jnp.exp(ztot[8:16]), jnp.exp(ztot[16:24]))
    mix_cols[...] = columns(jnp.concatenate([post, e0, e1], axis=0))

    @pl.when(yhi == 1)
    def _():
        def tail(c, carry):
            for d in range(4):
                cross(c, d).wait_recv()
                twin2(c, d).start()
            return carry

        lax.fori_loop(NC - 2, NC, tail, 0)

    for r, (sq_, tp_) in enumerate(tp_peers):
        remote(unow, urecv.at[r], u_ss.at[r], u_rs.at[r], sq_, tp_).wait_send()
        remote(nall, nrecv.at[r], n_ss.at[r], n_rs.at[r], sq_, tp_).wait_send()
    for d in range(3):
        count_to(0, d, z_peers[d]).wait_send()
    count_to(1, 3, sibling).wait_send()
    count_to(2, 4, mirror).wait_send()

    def drain(c, carry):
        for k in range(7):
            move(c, k, tp, 0, right).wait_send()
        kept(c).wait()
        for d in range(1, 4):
            spread(c, d).wait_send()
        for d in range(4):
            twin(c, d).wait_send()
            twin_in(c, d).wait_recv()

        @pl.when(yhi == 0)
        def _():
            for d in range(4):
                cross(c, d).wait_send()

        @pl.when(yhi == 1)
        def _():
            for d in range(4):
                twin2(c, d).wait_send()
                twin2_in(c, d).wait_recv()

        return carry

    lax.fori_loop(0, NC, drain, 0)


def attention_kernel(att_hbm, cnt_hbm, ctx, att, cnt, vx, m_ref, acc_ref, c_sem, k_sem, v_sem, q_sem):
    seq = lax.axis_index("seq")
    yhi, core = seq // 8, seq % 2
    counts_in = pltpu.make_async_copy(cnt_hbm, cnt, c_sem)
    counts_in.start()

    def q_in(qi):
        qb = yhi * 8 + qi * 2 + core
        return pltpu.make_async_copy(att_hbm.at[qb, :, 2], att.at[qb, :, 2], q_sem.at[qi])

    def k_in(kb):
        return pltpu.make_async_copy(att_hbm.at[kb, :, 0], att.at[kb, :, 0], k_sem.at[kb])

    def v_in(kb):
        return pltpu.make_async_copy(att_hbm.at[kb, :, 1], vx.at[kb, :, :, pl.ds(0, HD)], v_sem.at[kb])

    q_in(0).start()
    counts_in.wait()
    starts = [cnt[k, 0] for k in range(1, 4)]
    scale = HD ** (-0.5) * 1.4426950408889634

    def start_of(p):
        v = p * 0
        for c in starts:
            v = jnp.where(c <= p, jnp.maximum(v, c), v)
        return v

    first_needed = start_of((yhi * 8 + core) * T) // T

    def fetch(kb, c):
        k_in(kb).start()
        v_in(kb).start()
        return c

    def land(kb, c):
        k_in(kb).wait()
        v_in(kb).wait()
        return c

    lax.fori_loop(first_needed, yhi * 8 + core + 1, fetch, 0)
    for qi in range(1, 4):
        q_in(qi).start()
    lax.fori_loop(yhi * 8 + core + 1, yhi * 8 + core + 7, fetch, 0)

    def ones(kb, c):
        vx[kb, :, :, HD:] = jnp.ones((NC, R, HD), BF)
        return c

    lax.fori_loop(first_needed, yhi * 8 + core + 7, ones, 0)

    def one_query_block(qi, carry):
        qb = yhi * 8 + qi * 2 + core
        lax.fori_loop(jnp.where(qi == 0, first_needed, qb - 1), qb + 1, land, 0)
        q_in(qi).wait()
        q = att[qb, :, 2].reshape(T, HD)
        first = start_of(qb * T)
        last = start_of(qb * T + T - 1)
        lo = first // T
        mid = jnp.minimum((last + T - 1) // T, qb)
        qpos = qb * T + lax.broadcasted_iota(jnp.int32, (T, 1), 0)
        qstart = start_of(qpos)
        def block(kb, mode, n=1):
            k = att[pl.ds(kb, n), :, 0].reshape(n * T, HD)
            v = vx[pl.ds(kb, n)].reshape(n * T, 2 * HD)

            def scores(t):
                rows = slice(t * HALF, (t + 1) * HALF)
                s = lax.dot_general(q[rows], k, NT, preferred_element_type=F32)
                if mode != "all":
                    kpos = kb * T + lax.broadcasted_iota(jnp.int32, (1, T), 1)
                    ok = kpos >= qstart[rows]
                    if mode == "diagonal":
                        ok = ok & (kpos <= qpos[rows])
                    s = jnp.where(ok, s, NEG)
                return s

            later = scores(0)
            for t in range(T // HALF):
                rows = slice(t * HALF, (t + 1) * HALF)
                s = later
                if (t + 1) * HALF < T:
                    later = scores(t + 1)
                top = s[:, 0:128]
                for e in range(1, n * 4):
                    top = jnp.maximum(top, s[:, e * 128 : (e + 1) * 128])
                m_new = jnp.max(top, axis=1, keepdims=True)
                if mode != "diagonal":
                    m_old = m_ref[rows, 0:1]
                    m_new = jnp.maximum(m_old, m_new)
                    alpha = jnp.exp2((m_old - m_new) * scale)
                p = jnp.exp2((s - m_new) * scale).astype(BF)
                more = jnp.dot(p, v, preferred_element_type=F32)
                acc_ref[rows] = more if mode == "diagonal" else acc_ref[rows] * alpha + more
                m_ref[rows] = jnp.broadcast_to(m_new, (HALF, 128))

        def some(kb, c):
            block(kb, "start")
            return c

        def two(k, c):
            block(mid + 2 * k, "all", 2)
            return c

        def one(kb, c):
            block(kb, "all")
            return c

        block(qb, "diagonal")
        lax.fori_loop(lo, mid, some, 0)
        pairs = (qb - mid) // 2
        lax.fori_loop(0, pairs, two, 0)
        lax.fori_loop(mid + 2 * pairs, qb, one, 0)
        out = acc_ref[:, 0:HD] / acc_ref[:, HD : HD + 1]
        ctx[qi] = out.astype(BF).reshape(NO, RO, HD)
        return carry

    lax.fori_loop(0, 4, one_query_block, 0)


def last_kernel(
    ctx_hbm, w_hbm,
    branch,
    ctx, wbuf, cbuf, snd, snh, own, rcv, rch,
    c_sem, w_sem, z_ss, z_rs, s_ss, s_rs, h_ss, h_rs,
):
    seq, tp = where_am_i()
    yhi, z, core = seq // 8, (seq // 2) % 4, seq % 2
    x, y = tp // 2, tp % 2
    right = ((x + 1) % 4) * 2 + y
    left = ((x + 3) % 4) * 2 + y
    other_y = x * 2 + 1 - y
    z_peers = [yhi * 8 + ((z + d) % 4) * 2 + core for d in range(1, 4)]
    entered = greet([(p, tp) for p in z_peers] + [(seq, right), (seq, left), (seq, other_y)])
    ccopy = pltpu.make_async_copy(ctx_hbm, ctx, c_sem)
    ccopy.start()
    wcopy = pltpu.make_async_copy(w_hbm, wbuf, w_sem)
    wcopy.start()
    ccopy.wait()
    entered()

    def back(c, d):
        return remote(
            ctx.at[(z + d) % 4, c], cbuf.at[z, c], z_ss.at[c, d - 1], z_rs.at[c, d - 1], z_peers[d - 1], tp
        )

    def back_in(c, d):
        remote(
            ctx.at[z, c], cbuf.at[(z + 4 - d) % 4, c], z_ss.at[c, d - 1], z_rs.at[c, d - 1], z_peers[d - 1], tp
        ).wait_recv()

    for c in range(NO):
        for d in (2, 1, 3):
            back(c, d).start()
    cbuf[z] = ctx[z]
    wcopy.wait()

    def pass_on(c, k, to):
        return remote(snd.at[c, k], rcv.at[c, k], s_ss.at[c, k], s_rs.at[c, k], seq, to)

    def half(c, k, to):
        return remote(snh.at[c, k], rch.at[c, k], h_ss.at[c, k], h_rs.at[c, k], seq, to)

    to_right, to_left, far = ((x + 1) % 4) * 2, ((x + 3) % 4) * 2, ((x + 2) % 4) * 2

    def project(c, carry):
        for d in range(1, 4):
            back_in(c, d)
        lhs = jnp.concatenate([cbuf[h, c] for h in range(4)], axis=1)

        def term(b):
            cols = pl.ds(pl.multiple_of(b * W, W), W)
            return jnp.dot(lhs, wbuf[:, cols], preferred_element_type=F32)

        snd[c, 0] = term(far + 1 - y).astype(BF)
        snd[c, 1] = term(to_right + 1 - y).astype(BF)
        pass_on(c, 0, other_y).start()
        snd[c, 2] = term(to_left + 1 - y).astype(BF)
        pass_on(c, 1, right).start()
        own[c, 0] = term(far + y)
        pass_on(c, 2, left).start()
        own[c, 1] = term(to_right + y)
        own[c, 2] = term(to_left + y)
        own[c, 3] = term(other_y)
        own[c, 4] = term(tp)
        return carry

    lax.fori_loop(0, NO, project, 0)

    def second(c, carry):
        pass_on(c, 0, other_y).wait_recv()
        far_sum = (own[c, 0] + rcv[c, 0].astype(F32)).astype(BF)
        snh[c, 0] = far_sum[0 : RO // 2]
        snh[c, 1] = far_sum[RO // 2 :]
        half(c, 0, right).start()
        half(c, 1, left).start()
        return carry

    lax.fori_loop(0, NO, second, 0)

    def third(c, carry):
        pass_on(c, 1, right).wait_recv()
        pass_on(c, 2, left).wait_recv()
        snd[c, 5] = (own[c, 3] + (rcv[c, 1].astype(F32) + rcv[c, 2].astype(F32))).astype(BF)
        pass_on(c, 5, other_y).start()
        half(c, 0, right).wait_recv()
        snd[c, 3, 0 : RO // 2] = (own[c, 1, 0 : RO // 2] + rch[c, 0].astype(F32)).astype(BF)
        snd[c, 3, RO // 2 :] = own[c, 1, RO // 2 :].astype(BF)
        pass_on(c, 3, right).start()
        half(c, 1, left).wait_recv()
        snd[c, 4, 0 : RO // 2] = own[c, 2, 0 : RO // 2].astype(BF)
        snd[c, 4, RO // 2 :] = (own[c, 2, RO // 2 :] + rch[c, 1].astype(F32)).astype(BF)
        pass_on(c, 4, left).start()
        return carry

    lax.fori_loop(0, NO, third, 0)

    def fourth(c, carry):
        pass_on(c, 5, other_y).wait_recv()
        pass_on(c, 3, right).wait_recv()
        pass_on(c, 4, left).wait_recv()
        rows = pl.ds(pl.multiple_of(c * RO, RO), RO)
        branch[rows, :] = (own[c, 4] + rcv[c, 5].astype(F32)) + (
            rcv[c, 3].astype(F32) + rcv[c, 4].astype(F32)
        )
        return carry

    lax.fori_loop(0, NO, fourth, 0)

    def drain(c, carry):
        for d in range(1, 4):
            back(c, d).wait_send()
        for k in range(6):
            pass_on(c, k, right).wait_send()
        half(c, 0, right).wait_send()
        half(c, 1, left).wait_send()
        return carry

    lax.fori_loop(0, NO, drain, 0)


def combine_kernel(xraw, cols, branch, out):
    xv = jnp.swapaxes(xraw[...], 0, 1)
    wide = [xv[j].astype(F32) for j in range(S)]
    b = branch[...]
    new = []
    for i in range(S):
        v = cols[:, 4 + i : 5 + i] * b
        for j in range(S):
            k = 8 + 4 * i + j
            v = v + cols[:, k : k + 1] * wide[j]
        new.append(v.astype(BF))
    out[...] = jnp.swapaxes(jnp.stack(new, axis=0), 0, 1)


def local(streams, doc_ids, mix_weight, mix_bias, attn_gain, w_qkv, w_out):
    wmix = jnp.transpose(mix_weight, (0, 2, 1))
    wq = jnp.transpose(w_qkv, (1, 0, 2))
    vm = pl.BlockSpec(memory_space=VMEM)
    hbm = pl.BlockSpec(memory_space=pl.ANY)
    sds = jax.ShapeDtypeStruct
    att, mix_cols, counts = pl.pallas_call(
        first_kernel,
        name="gather_project",
        out_shape=(
            sds((16, NC, 3, R, HD), BF),
            sds((T, 128), F32),
            sds((8, 128), jnp.int32),
        ),
        in_specs=[hbm] * 6,
        out_specs=(hbm, vm, vm),
        scratch_shapes=[
            VMEM((T, S, W), BF),
            VMEM((S, T, W), BF),
            VMEM((4, 128), jnp.int32),
            VMEM((S, 24, W), F32),
            VMEM((1, 24), F32),
            VMEM((1, D), F32),
            VMEM((3, D, W), BF),
            VMEM((NC, 8, R, W), BF),
            VMEM((4, NC, 3, R, HD), BF),
            VMEM((R, D), BF),
            VMEM((8, T), F32),
            VMEM((7, 8, T), F32),
            VMEM((24, T), F32),
            VMEM((7, 24, T), F32),
            VMEM((3, 8, 128), jnp.int32),
            VMEM((5, 8, 128), jnp.int32),
            VMEM((T, 128), F32),
            DMA((4,)),
            DMA((4,)),
            DMA((3,)),
            DMA((7,)), DMA((7,)),
            DMA((7,)), DMA((7,)),
            DMA((5,)), DMA((5,)),
            DMA((NC, 7)), DMA((NC, 7)),
            DMA((NC, 3)), DMA((NC, 3)),
            DMA((NC,)),
            DMA((NC, 4)), DMA((NC, 4)),
            DMA((NC, 4)), DMA((NC, 4)),
            DMA((NC, 4)), DMA((NC, 4)),
        ],
        compiler_params=pltpu.CompilerParams(
            collective_id=0, has_side_effects=True, vmem_limit_bytes=60 * 1024 * 1024
        ),
    )(
        streams, doc_ids.reshape(4, 128), wmix, mix_bias.reshape(1, 24), attn_gain.reshape(1, D), wq,
    )
    ctx = pl.pallas_call(
        attention_kernel,
        name="attention",
        out_shape=sds((4, NO, RO, HD), BF),
        in_specs=[hbm, hbm],
        out_specs=vm,
        scratch_shapes=[
            VMEM((16, NC, 3, R, HD), BF),
            pltpu.SMEM((8, 128), jnp.int32),
            VMEM((16, NC, R, 2 * HD), BF),
            VMEM((T, 128), F32), VMEM((T, 2 * HD), F32),
            DMA(()), DMA((16,)), DMA((16,)), DMA((4,)),
        ],
        compiler_params=pltpu.CompilerParams(vmem_limit_bytes=60 * 1024 * 1024),
    )(att, counts)
    branch = pl.pallas_call(
        last_kernel,
        name="project_out",
        out_shape=sds((T, W), F32),
        in_specs=[hbm, hbm],
        out_specs=vm,
        scratch_shapes=[
            VMEM((4, NO, RO, HD), BF),
            VMEM((W, D), BF),
            VMEM((4, NO, RO, HD), BF),
            VMEM((NO, 6, RO, W), BF),
            VMEM((NO, 2, RO // 2, W), BF),
            VMEM((NO, 5, RO, W), F32),
            VMEM((NO, 6, RO, W), BF),
            VMEM((NO, 2, RO // 2, W), BF),
            DMA(()),
            DMA(()),
            DMA((NO, 3)), DMA((NO, 3)),
            DMA((NO, 6)), DMA((NO, 6)),
            DMA((NO, 2)), DMA((NO, 2)),
        ],
        compiler_params=pltpu.CompilerParams(
            collective_id=1, has_side_effects=True, vmem_limit_bytes=60 * 1024 * 1024
        ),
    )(ctx, w_out)
    return pl.pallas_call(
        combine_kernel,
        name="combine",
        grid=(4,),
        out_shape=sds((T, S, W), BF),
        in_specs=[
            pl.BlockSpec((T // 4, S, W), lambda i: (i, 0, 0)),
            pl.BlockSpec((T // 4, 128), lambda i: (i, 0)),
            pl.BlockSpec((T // 4, W), lambda i: (i, 0)),
        ],
        out_specs=pl.BlockSpec((T // 4, S, W), lambda i: (i, 0, 0)),
        compiler_params=pltpu.CompilerParams(vmem_limit_bytes=60 * 1024 * 1024),
    )(streams, mix_cols, branch)


def solution(mesh):
    in_specs = (
        P("seq", None, "tp"),
        P("seq"),
        P(None, "tp", None),
        P(),
        P(),
        P(None, None, "tp"),
        P("tp", None),
    )
    return jax.shard_map(
        local, mesh=mesh, in_specs=in_specs, out_specs=P("seq", None, "tp"), check_vma=False
    )
```

```python
import jax
import jax.numpy as jnp
from jax import lax
from jax.experimental import pallas as pl
from jax.experimental.pallas import tpu as pltpu
from jax.sharding import PartitionSpec as P

D = 4096
HD = 128
S = 4
ROUNDS = 20
EPS = 1e-6
T = 512
W = 512
NC = 8
NO = 4
RO = T // NO
BLOCKS = 160
TILES = 9216
HALF = 256
AHEAD = 3
R = T // NC
F32 = jnp.float32
BF = jnp.bfloat16
MESH = pl.DeviceIdType.MESH
NT = (((1,), (1,)), ((), ()))
NEG = -1e30
VMEM = pltpu.VMEM
DMA = pltpu.SemaphoreType.DMA


def where_am_i():
    seq = lax.axis_index("seq")
    tp = lax.axis_index("tp")
    return seq, tp


def remote(src, dst, ssem, rsem, seq, tp):
    return pltpu.make_async_remote_copy(
        src_ref=src, dst_ref=dst, send_sem=ssem, recv_sem=rsem,
        device_id={"seq": seq, "tp": tp}, device_id_type=MESH,
    )


def greet(peers):
    barrier = pltpu.get_barrier_semaphore()
    for seq, tp in peers:
        pl.semaphore_signal(barrier, inc=1, device_id={"seq": seq, "tp": tp}, device_id_type=MESH)
    return lambda: pl.semaphore_wait(barrier, len(peers))


def columns(rows8):
    k = rows8.shape[0]
    if k < 128:
        rows8 = jnp.concatenate([rows8, jnp.zeros((128 - k, rows8.shape[1]), F32)], axis=0)
    return rows8.T


def balanced(e0, e1):
    sub = lax.broadcasted_iota(jnp.int32, e0.shape, 0)
    even, low = sub % 2 == 0, sub % 4 < 2

    def row_total(e):
        u = e + jnp.where(even, pltpu.roll(e, 7, 0), pltpu.roll(e, 1, 0))
        return u + jnp.where(low, pltpu.roll(u, 6, 0), pltpu.roll(u, 2, 0))

    def one_round(_, pair):
        e0, e1 = pair
        e0 = e0 / row_total(e0)
        e1 = e1 / row_total(e1)
        t = e0 + e1
        t = t + pltpu.roll(t, 4, 0)
        return e0 / t, e1 / t

    return lax.fori_loop(0, ROUNDS, one_round, (e0, e1))


def first_kernel(
    x_hbm, docs_hbm, wmix_hbm, bias_hbm, gain_hbm, w_hbm,
    att, mix_cols, counts,
    xraw, xs, docs, wmix, bias, gain,
    wbuf, g, sb, gained, norms, unow, urecv, nall, nrecv, csend, crecv, pre_cols,
    x_sem, i_sem, w_sem, u_ss, u_rs, n_ss, n_rs, c_ss, c_rs, g_ss, g_rs, a_ss, a_rs, q_ss, q_rs, o_sem, t_sem,
    sib_ss, sib_rs, x_ss, x_rs, sib2_ss, sib2_rs,
):
    seq, tp = where_am_i()
    yhi, z, core = seq // 8, (seq // 2) % 4, seq % 2
    x, y = tp // 2, tp % 2
    sibling, mirror = seq + 1 - 2 * core, (seq + 8) % 16
    tp_peers = [(seq, (tp + r) % 8) for r in range(1, 8)]
    z_peers = [yhi * 8 + ((z + d) % 4) * 2 + core for d in range(1, 4)]
    entered = greet(tp_peers + [(p, tp) for p in z_peers] + [(sibling, tp), (mirror, tp)])

    small = [
        pltpu.make_async_copy(a, b, i_sem.at[i])
        for i, (a, b) in enumerate(
            ((wmix_hbm, wmix), (docs_hbm, docs), (bias_hbm, bias), (gain_hbm, gain))
        )
    ]
    parts_of_x = [
        pltpu.make_async_copy(x_hbm.at[pl.ds(q * 128, 128)], xraw.at[pl.ds(q * 128, 128)], x_sem.at[q])
        for q in range(4)
    ]
    small[0].start()
    for q in range(4):
        parts_of_x[q].start()
    for k in range(1, 4):
        small[k].start()

    def wcopy(i):
        return pltpu.make_async_copy(w_hbm.at[i], wbuf.at[i], w_sem.at[i])

    small[0].wait()
    parts = []
    for s in range(S):
        w = jnp.concatenate([wmix[s], jnp.zeros((8, W), F32)], axis=0)
        hi = w.astype(BF).astype(F32)
        mid = (w - hi).astype(BF).astype(F32)
        low = (w - hi) - mid
        parts.append(jnp.concatenate([hi, mid, low], axis=0).astype(BF))
    sub = lax.broadcasted_iota(jnp.int32, (8, 128), 0)
    for q in range(4):
        rows = slice(q * 128, (q + 1) * 128)
        parts_of_x[q].wait()
        if q == 3:
            for i in range(3):
                wcopy(i).start()
        xs[:, rows, :] = jnp.swapaxes(xraw[rows], 0, 1)
        acc = jnp.zeros((128, 128), F32)
        logits = jnp.zeros((32, 128), F32)
        for s in range(S):
            xv = xs[s, rows, :]
            got = lax.dot_general(parts[s], xv, NT, preferred_element_type=F32)
            logits = logits + (got[0:32] + (got[32:64] + got[64:96]))
            x32 = xv.astype(F32)
            sq = x32 * x32
            acc = acc + ((sq[:, 0:128] + sq[:, 128:256]) + (sq[:, 256:384] + sq[:, 384:512]))
        squares = jnp.sum(acc.T, axis=0, keepdims=True)
        unow[:, rows] = jnp.where(
            sub < 4, logits[0:8], jnp.where(sub == 4, jnp.broadcast_to(squares, (8, 128)), 0.0)
        )
        nall[:, rows] = logits[0:24]

    entered()
    for r, (sq_, tp_) in enumerate(tp_peers):
        remote(unow, urecv.at[r], u_ss.at[r], u_rs.at[r], sq_, tp_).start()

    for k in range(1, 4):
        small[k].wait()
    dv = docs[...]
    cv = jnp.zeros((8, 128), jnp.int32)
    for k in range(1, 4):
        n = jnp.sum(jnp.where(dv < k, 1, 0), axis=1, keepdims=True)
        n = jnp.sum(n, axis=0, keepdims=True)
        cv = jnp.where(sub == k, jnp.broadcast_to(n, (8, 128)), cv)
    csend[0] = cv
    diag = lax.broadcasted_iota(jnp.int32, (24, 24), 0) == lax.broadcasted_iota(jnp.int32, (24, 24), 1)
    bias_col = jnp.sum(jnp.where(diag, jnp.broadcast_to(bias[...], (24, 24)), 0.0), axis=1, keepdims=True)

    def count_to(level, k, to):
        return remote(csend.at[level], crecv.at[k], c_ss.at[k], c_rs.at[k], to, tp)

    total = unow[...]
    for r, (sq_, tp_) in enumerate(tp_peers):
        remote(unow, urecv.at[r], u_ss.at[r], u_rs.at[r], sq_, tp_).wait_recv()
        total = total + urecv[r]
    inv_rms = lax.rsqrt(total[4:5] / (S * D) + EPS)
    pre = 1.0 / (1.0 + jnp.exp(-(total * inv_rms + bias_col[0:8])))
    pre_cols[...] = columns(pre)

    right = ((x + 1) % 4) * 2 + y
    left = ((x + 3) % 4) * 2 + y
    other_y = x * 2 + 1 - y
    b_p = other_y
    b_l0, b_l1 = left, ((x + 3) % 4) * 2 + 1 - y
    b_r0, b_r1 = right, ((x + 1) % 4) * 2 + 1 - y
    b_f0, b_f1 = ((x + 2) % 4) * 2 + y, ((x + 2) % 4) * 2 + 1 - y

    def move(c, k, blk, role, to):
        return remote(g.at[c, blk], g.at[c, blk], g_ss.at[c, k], g_rs.at[c, role], seq, to)

    def arrived(c, role, blk):
        move(c, 0, blk, role, right).wait_recv()

    def make_chunk(c):
        rows = slice(c * R, (c + 1) * R)
        v = pre_cols[rows, 0:1] * xs[0, rows, :].astype(F32)
        for s in range(1, S):
            v = v + pre_cols[rows, s : s + 1] * xs[s, rows, :].astype(F32)
        g[c, tp] = v.astype(BF)

    def send_chunk(c):
        move(c, 2, tp, 0, other_y).start()
        move(c, 0, tp, 1, right).start()
        move(c, 1, tp, 3, left).start()

    make_chunk(0)
    for c in range(NC):
        if c + 1 < NC:
            make_chunk(c + 1)
        if c < AHEAD:
            send_chunk(c)
    for d in range(3):
        count_to(0, d, z_peers[d]).start()
    for i in range(3):
        wcopy(i).wait()

    def block_of(half, d):
        return half * 8 + ((z + 4 - d) % 4) * 2 + core

    two = pl.ds(0, 2)

    def spread(c, d):
        return remote(
            sb.at[(z + d) % 4, c, two], att.at[seq, c, two],
            a_ss.at[c, d - 1], a_rs.at[c, d - 1], z_peers[d - 1], tp,
        )

    def spread_in(c, d):
        remote(
            sb.at[z, c, two], att.at[block_of(yhi, d), c, two],
            a_ss.at[c, d - 1], a_rs.at[c, d - 1], z_peers[d - 1], tp,
        ).wait_recv()

    def spread_q(c, d):
        return remote(
            sb.at[(z + d) % 4, c, 2], att.at[seq, c, 2],
            q_ss.at[c, d - 1], q_rs.at[c, d - 1], z_peers[d - 1], tp,
        )

    def spread_q_in(c, d):
        remote(
            sb.at[z, c, 2], att.at[block_of(yhi, d), c, 2],
            q_ss.at[c, d - 1], q_rs.at[c, d - 1], z_peers[d - 1], tp,
        ).wait_recv()

    def kept(c):
        return pltpu.make_async_copy(sb.at[z, c], att.at[seq, c], o_sem.at[c])

    def kv(c, d):
        return sb.at[z, c, pl.ds(0, 2)] if d == 0 else att.at[block_of(yhi, d), c, pl.ds(0, 2)]

    def twin(c, d):
        dst = att.at[block_of(yhi, d), c, pl.ds(0, 2)]
        return remote(kv(c, d), dst, sib_ss.at[c, d], sib_rs.at[c, d], sibling, tp)

    def twin_in(c, d):
        dst = att.at[yhi * 8 + ((z + 4 - d) % 4) * 2 + 1 - core, c, pl.ds(0, 2)]
        return remote(kv(c, d), dst, sib_ss.at[c, d], sib_rs.at[c, d], sibling, tp)

    def cross(c, d):
        dst = att.at[block_of(0, d), c, pl.ds(0, 2)]
        return remote(kv(c, d), dst, x_ss.at[c, d], x_rs.at[c, d], mirror, tp)

    def twin2(c, d):
        ref = att.at[block_of(0, d), c, pl.ds(0, 2)]
        return remote(ref, ref, sib2_ss.at[c, d], sib2_rs.at[c, d], sibling, tp)

    def twin2_in(c, d):
        dst = att.at[((z + 4 - d) % 4) * 2 + 1 - core, c, pl.ds(0, 2)]
        return remote(dst, dst, sib2_ss.at[c, d], sib2_rs.at[c, d], sibling, tp)

    def hand_on(i):
        arrived(i, 0, b_p)
        move(i, 3, b_p, 2, right).start()
        move(i, 4, b_p, 4, left).start()

    hand_on(0)

    def feed(i):
        @pl.when(i + AHEAD < NC)
        def _():
            send_chunk(i + AHEAD)

        @pl.when(i + 1 < NC)
        def _():
            hand_on(i + 1)

        @pl.when(i < NC)
        def _():
            arrived(i, 1, b_l0)
            move(i, 5, b_l0, 5, right).start()
            arrived(i, 4, b_r1)
            move(i, 6, b_r1, 6, left).start()

    def projected(c0):
        for e in range(2):
            c = c0 + e
            rows = slice(e * R, (e + 1) * R)
            arrived(c, 2, b_l1)
            arrived(c, 3, b_r0)
            arrived(c, 5, b_f0)
            arrived(c, 6, b_f1)
            ss = jnp.zeros((R, 128), F32)
            for b in range(8):
                g32 = g[c, b].astype(F32)
                q = g32 * g32
                ss = ss + ((q[:, 0:128] + q[:, 128:256]) + (q[:, 256:384] + q[:, 384:512]))
                gained[rows, b * W : (b + 1) * W] = (g32 * gain[:, b * W : (b + 1) * W]).astype(BF)
            norms[rows, :] = jnp.broadcast_to(
                lax.rsqrt(jnp.sum(ss, axis=1, keepdims=True) / D + EPS), (R, 128)
            )
        norm = norms[:, 0:1]
        lhs = gained[...]

        def project(slot, third):
            out = (jnp.dot(lhs, wbuf[third], preferred_element_type=F32) * norm).astype(BF)
            for h in range(4):
                for e in range(2):
                    sb[h, c0 + e, slot] = out[e * R : (e + 1) * R, h * HD : (h + 1) * HD]

        project(0, 1)
        project(1, 2)
        for e in range(2):
            for d in (2, 1, 3):
                spread(c0 + e, d).start()
        project(2, 0)
        for e in range(2):
            for d in (2, 1, 3):
                spread_q(c0 + e, d).start()
            kept(c0 + e).start()

    def share(c):
        for d in range(4):
            if d:
                spread_in(c, d)

            @pl.when(yhi == 0)
            def _():
                cross(c, d).start()

            twin(c, d).start()

    def share_far(c):
        for d in range(4):
            cross(c, d).wait_recv()
            twin2(c, d).start()

    def step(i, carry):
        feed(2 * i)

        @pl.when(i >= 1)
        def _():
            projected(2 * i - 2)

        feed(2 * i + 1)

        @pl.when(i >= 1)
        def _():
            share(2 * i - 2)
            share(2 * i - 1)

        @pl.when((i >= 2) & (yhi == 1))
        def _():
            share_far(2 * i - 4)
            share_far(2 * i - 3)

        @pl.when(i == NC // 2)
        def _():
            for r, (sq_, tp_) in enumerate(tp_peers):
                remote(nall, nrecv.at[r], n_ss.at[r], n_rs.at[r], sq_, tp_).start()

        @pl.when(i == 1)
        def _():
            v = csend[0]
            for d in range(3):
                count_to(0, d, z_peers[d]).wait_recv()
                v = v + crecv[d]
            csend[1] = v

        @pl.when(i == 2)
        def _():
            count_to(1, 3, sibling).start()

        @pl.when(i == 3)
        def _():
            count_to(1, 3, sibling).wait_recv()
            csend[2] = csend[1] + crecv[3]

        @pl.when(i == 4)
        def _():
            count_to(2, 4, mirror).start()

        return carry

    lax.fori_loop(0, NC // 2 + 1, step, 0)

    count_to(2, 4, mirror).wait_recv()
    csend[3] = csend[2] + crecv[4]
    told = pltpu.make_async_copy(csend.at[3], counts.at[0], t_sem)
    told.start()
    ztot = nall[...]
    for r, (sq_, tp_) in enumerate(tp_peers):
        remote(nall, nrecv.at[r], n_ss.at[r], n_rs.at[r], sq_, tp_).wait_recv()
        ztot = ztot + nrecv[r]
    ztot = ztot * inv_rms + bias_col
    post = 2.0 / (1.0 + jnp.exp(-ztot[0:8]))
    e0, e1 = balanced(jnp.exp(ztot[8:16]), jnp.exp(ztot[16:24]))
    mix_cols[...] = columns(jnp.concatenate([post, e0, e1], axis=0))

    @pl.when(yhi == 1)
    def _():
        share_far(NC - 2)
        share_far(NC - 1)

    told.wait()
    for r, (sq_, tp_) in enumerate(tp_peers):
        remote(unow, urecv.at[r], u_ss.at[r], u_rs.at[r], sq_, tp_).wait_send()
        remote(nall, nrecv.at[r], n_ss.at[r], n_rs.at[r], sq_, tp_).wait_send()
    for d in range(3):
        count_to(0, d, z_peers[d]).wait_send()
    count_to(1, 3, sibling).wait_send()
    count_to(2, 4, mirror).wait_send()

    def drain(c, carry):
        for k in range(7):
            move(c, k, tp, 0, right).wait_send()
        kept(c).wait()
        for d in range(1, 4):
            spread(c, d).wait_send()
            spread_q(c, d).wait_send()
            spread_q_in(c, d)
        for d in range(4):
            twin(c, d).wait_send()
            twin_in(c, d).wait_recv()

        @pl.when(yhi == 0)
        def _():
            for d in range(4):
                cross(c, d).wait_send()

        @pl.when(yhi == 1)
        def _():
            for d in range(4):
                twin2(c, d).wait_send()
                twin2_in(c, d).wait_recv()

        return carry

    lax.fori_loop(0, NC, drain, 0)


def attention_kernel(att_hbm, cnt_hbm, ctx, att, cnt, vx, m_ref, acc_ref, c_sem, k_sem, v_sem, q_sem):
    seq = lax.axis_index("seq")
    yhi, core = seq // 8, seq % 2
    counts_in = pltpu.make_async_copy(cnt_hbm.at[0], cnt, c_sem)
    counts_in.start()

    def q_in(qi):
        qb = yhi * 8 + qi * 2 + core
        return pltpu.make_async_copy(att_hbm.at[qb, :, 2], att.at[qb, :, 2], q_sem.at[qi])

    def k_in(kb):
        return pltpu.make_async_copy(att_hbm.at[kb, :, 0], att.at[kb, :, 0], k_sem.at[kb])

    def v_in(kb):
        return pltpu.make_async_copy(att_hbm.at[kb, :, 1], vx.at[kb, :, :, pl.ds(0, HD)], v_sem.at[kb])

    q_in(0).start()
    counts_in.wait()
    starts = [cnt[k, 0] for k in range(1, 4)]
    scale = HD ** (-0.5) * 1.4426950408889634

    def start_of(p):
        v = p * 0
        for c in starts:
            v = jnp.where(c <= p, jnp.maximum(v, c), v)
        return v

    first_needed = start_of((yhi * 8 + core) * T) // T

    def fetch(kb, c):
        k_in(kb).start()
        v_in(kb).start()
        return c

    def land(kb, c):
        k_in(kb).wait()
        v_in(kb).wait()
        return c

    lax.fori_loop(first_needed, yhi * 8 + core + 1, fetch, 0)
    for qi in range(1, 4):
        q_in(qi).start()
    lax.fori_loop(yhi * 8 + core + 1, yhi * 8 + core + 7, fetch, 0)

    def ones(kb, c):
        vx[kb, :, :, HD:] = jnp.ones((NC, R, HD), BF)
        return c

    lax.fori_loop(first_needed, yhi * 8 + core + 7, ones, 0)

    def one_query_block(qi, carry):
        qb = yhi * 8 + qi * 2 + core
        lax.fori_loop(jnp.where(qi == 0, first_needed, qb - 1), qb + 1, land, 0)
        q_in(qi).wait()
        q = att[qb, :, 2].reshape(T, HD)
        first = start_of(qb * T)
        last = start_of(qb * T + T - 1)
        lo = first // T
        mid = jnp.minimum((last + T - 1) // T, qb)
        qpos = qb * T + lax.broadcasted_iota(jnp.int32, (T, 1), 0)
        qstart = start_of(qpos)
        def block(kb, mode, n=1):
            k = att[pl.ds(kb, n), :, 0].reshape(n * T, HD)
            v = vx[pl.ds(kb, n)].reshape(n * T, 2 * HD)

            def scores(t):
                rows = slice(t * HALF, (t + 1) * HALF)
                s = lax.dot_general(q[rows], k, NT, preferred_element_type=F32)
                if mode != "all":
                    kpos = kb * T + lax.broadcasted_iota(jnp.int32, (1, T), 1)
                    ok = kpos >= qstart[rows]
                    if mode == "diagonal":
                        ok = ok & (kpos <= qpos[rows])
                    s = jnp.where(ok, s, NEG)
                return s

            later = scores(0)
            for t in range(T // HALF):
                rows = slice(t * HALF, (t + 1) * HALF)
                s = later
                if (t + 1) * HALF < T:
                    later = scores(t + 1)
                top = s[:, 0:128]
                for e in range(1, n * 4):
                    top = jnp.maximum(top, s[:, e * 128 : (e + 1) * 128])
                m_new = jnp.max(top, axis=1, keepdims=True)
                if mode != "diagonal":
                    m_old = m_ref[rows, 0:1]
                    m_new = jnp.maximum(m_old, m_new)
                    alpha = jnp.exp2((m_old - m_new) * scale)
                p = jnp.exp2((s - m_new) * scale).astype(BF)
                more = jnp.dot(p, v, preferred_element_type=F32)
                acc_ref[rows] = more if mode == "diagonal" else acc_ref[rows] * alpha + more
                m_ref[rows] = jnp.broadcast_to(m_new, (HALF, 128))

        def some(kb, c):
            block(kb, "start")
            return c

        def two(k, c):
            block(mid + 2 * k, "all", 2)
            return c

        def one(kb, c):
            block(kb, "all")
            return c

        block(qb, "diagonal")
        lax.fori_loop(lo, mid, some, 0)
        pairs = (qb - mid) // 2
        lax.fori_loop(0, pairs, two, 0)
        lax.fori_loop(mid + 2 * pairs, qb, one, 0)
        out = acc_ref[:, 0:HD] / acc_ref[:, HD : HD + 1]
        ctx[qi] = out.astype(BF).reshape(NO, RO, HD)
        return carry

    lax.fori_loop(0, 4, one_query_block, 0)


def last_kernel(
    ctx, wbuf, xraw, cols,
    out,
    cbuf, snd, snh, own, rcv, rch, kept,
    z_ss, z_rs, s_ss, s_rs, h_ss, h_rs,
):
    seq, tp = where_am_i()
    yhi, z, core = seq // 8, (seq // 2) % 4, seq % 2
    x, y = tp // 2, tp % 2
    right = ((x + 1) % 4) * 2 + y
    left = ((x + 3) % 4) * 2 + y
    other_y = x * 2 + 1 - y
    z_peers = [yhi * 8 + ((z + d) % 4) * 2 + core for d in range(1, 4)]
    entered = greet([(p, tp) for p in z_peers] + [(seq, right), (seq, left), (seq, other_y)])
    entered()

    def back(c, d):
        return remote(
            ctx.at[(z + d) % 4, c], cbuf.at[z, c], z_ss.at[c, d - 1], z_rs.at[c, d - 1], z_peers[d - 1], tp
        )

    def back_in(c, d):
        remote(
            ctx.at[z, c], cbuf.at[(z + 4 - d) % 4, c], z_ss.at[c, d - 1], z_rs.at[c, d - 1], z_peers[d - 1], tp
        ).wait_recv()

    for c in range(NO):
        for d in (2, 1, 3):
            back(c, d).start()
    cbuf[z] = ctx[z]

    def pass_on(c, k, to):
        return remote(snd.at[c, k], rcv.at[c, k], s_ss.at[c, k], s_rs.at[c, k], seq, to)

    def half(c, k, to):
        return remote(snh.at[c, k], rch.at[c, k], h_ss.at[c, k], h_rs.at[c, k], seq, to)

    to_right, to_left, far = ((x + 1) % 4) * 2, ((x + 3) % 4) * 2, ((x + 2) % 4) * 2

    def project(c, carry):
        for d in range(1, 4):
            back_in(c, d)
        lhs = jnp.concatenate([cbuf[h, c] for h in range(4)], axis=1)

        def term(b):
            cols = pl.ds(pl.multiple_of(b * W, W), W)
            return jnp.dot(lhs, wbuf[:, cols], preferred_element_type=F32)

        snd[c, 0] = term(far + 1 - y).astype(BF)
        snd[c, 1] = term(to_right + 1 - y).astype(BF)
        pass_on(c, 0, other_y).start()
        snd[c, 2] = term(to_left + 1 - y).astype(BF)
        pass_on(c, 1, right).start()
        own[c, 0] = term(far + y)
        pass_on(c, 2, left).start()
        own[c, 1] = term(to_right + y)
        own[c, 2] = term(to_left + y)
        own[c, 3] = term(other_y)
        own[c, 4] = term(tp)
        return carry

    lax.fori_loop(0, NO, project, 0)

    def second(c, carry):
        pass_on(c, 0, other_y).wait_recv()
        far_sum = (own[c, 0] + rcv[c, 0].astype(F32)).astype(BF)
        snh[c, 0] = far_sum[0 : RO // 2]
        snh[c, 1] = far_sum[RO // 2 :]
        half(c, 0, right).start()
        half(c, 1, left).start()
        return carry

    lax.fori_loop(0, NO, second, 0)

    def third(c, carry):
        pass_on(c, 1, right).wait_recv()
        pass_on(c, 2, left).wait_recv()
        snd[c, 5] = (own[c, 3] + (rcv[c, 1].astype(F32) + rcv[c, 2].astype(F32))).astype(BF)
        pass_on(c, 5, other_y).start()
        half(c, 0, right).wait_recv()
        snd[c, 3, 0 : RO // 2] = (own[c, 1, 0 : RO // 2] + rch[c, 0].astype(F32)).astype(BF)
        snd[c, 3, RO // 2 :] = own[c, 1, RO // 2 :].astype(BF)
        pass_on(c, 3, right).start()
        half(c, 1, left).wait_recv()
        snd[c, 4, 0 : RO // 2] = own[c, 2, 0 : RO // 2].astype(BF)
        snd[c, 4, RO // 2 :] = (own[c, 2, RO // 2 :] + rch[c, 1].astype(F32)).astype(BF)
        pass_on(c, 4, left).start()
        return carry

    lax.fori_loop(0, NO, third, 0)

    def fourth(c, carry):
        rows = pl.ds(pl.multiple_of(c * RO, RO), RO)
        xv = jnp.swapaxes(xraw[rows], 0, 1)
        wide = [xv[j].astype(F32) for j in range(S)]
        for i in range(S):
            k = 8 + 4 * i
            v = cols[rows, k : k + 1] * wide[0]
            for j in range(1, S):
                v = v + cols[rows, k + j : k + j + 1] * wide[j]
            kept[i] = v
        pass_on(c, 5, other_y).wait_recv()
        mine = own[c, 4] + rcv[c, 5].astype(F32)
        pass_on(c, 3, right).wait_recv()
        pass_on(c, 4, left).wait_recv()
        branch = mine + (rcv[c, 3].astype(F32) + rcv[c, 4].astype(F32))
        new = [(kept[i] + cols[rows, 4 + i : 5 + i] * branch).astype(BF) for i in range(S)]
        out[rows] = jnp.swapaxes(jnp.stack(new, axis=0), 0, 1)
        return carry

    lax.fori_loop(0, NO, fourth, 0)

    def drain(c, carry):
        for d in range(1, 4):
            back(c, d).wait_send()
        for k in range(6):
            pass_on(c, k, right).wait_send()
        half(c, 0, right).wait_send()
        half(c, 1, left).wait_send()
        return carry

    lax.fori_loop(0, NO, drain, 0)


def store_kernel(x, out, sem):
    copies = [
        pltpu.make_async_copy(x.at[pl.ds(q * 128, 128)], out.at[pl.ds(q * 128, 128)], sem.at[q])
        for q in range(4)
    ]
    for copy in copies:
        copy.start()
    for copy in copies:
        copy.wait()


def local(streams, doc_ids, mix_weight, mix_bias, attn_gain, w_qkv, w_out):
    wmix = jnp.transpose(mix_weight, (0, 2, 1))
    wq = jnp.transpose(w_qkv, (1, 0, 2))
    vm = pl.BlockSpec(memory_space=VMEM)
    hbm = pl.BlockSpec(memory_space=pl.ANY)
    sds = jax.ShapeDtypeStruct
    att, mix_cols, counts = pl.pallas_call(
        first_kernel,
        name="gather_project",
        out_shape=(
            sds((BLOCKS, NC, 3, R, HD), BF),
            sds((T, 128), F32),
            sds((TILES, 8, 128), jnp.int32),
        ),
        in_specs=[hbm] * 6,
        out_specs=(hbm, vm, hbm),
        scratch_shapes=[
            VMEM((T, S, W), BF),
            VMEM((S, T, W), BF),
            VMEM((4, 128), jnp.int32),
            VMEM((S, 24, W), F32),
            VMEM((1, 24), F32),
            VMEM((1, D), F32),
            VMEM((3, D, W), BF),
            VMEM((NC, 8, R, W), BF),
            VMEM((4, NC, 3, R, HD), BF),
            VMEM((2 * R, D), BF),
            VMEM((2 * R, 128), F32),
            VMEM((8, T), F32),
            VMEM((7, 8, T), F32),
            VMEM((24, T), F32),
            VMEM((7, 24, T), F32),
            VMEM((4, 8, 128), jnp.int32),
            VMEM((5, 8, 128), jnp.int32),
            VMEM((T, 128), F32),
            DMA((4,)),
            DMA((4,)),
            DMA((3,)),
            DMA((7,)), DMA((7,)),
            DMA((7,)), DMA((7,)),
            DMA((5,)), DMA((5,)),
            DMA((NC, 7)), DMA((NC, 7)),
            DMA((NC, 3)), DMA((NC, 3)),
            DMA((NC, 3)), DMA((NC, 3)),
            DMA((NC,)),
            DMA(()),
            DMA((NC, 4)), DMA((NC, 4)),
            DMA((NC, 4)), DMA((NC, 4)),
            DMA((NC, 4)), DMA((NC, 4)),
        ],
        compiler_params=pltpu.CompilerParams(
            collective_id=0, has_side_effects=True, vmem_limit_bytes=60 * 1024 * 1024
        ),
    )(
        streams, doc_ids.reshape(4, 128), wmix, mix_bias.reshape(1, 24), attn_gain.reshape(1, D), wq,
    )
    ctx = pl.pallas_call(
        attention_kernel,
        name="attention",
        out_shape=sds((4, NO, RO, HD), BF),
        in_specs=[hbm, hbm],
        out_specs=vm,
        scratch_shapes=[
            VMEM((16, NC, 3, R, HD), BF),
            pltpu.SMEM((8, 128), jnp.int32),
            VMEM((16, NC, R, 2 * HD), BF),
            VMEM((T, 128), F32), VMEM((T, 2 * HD), F32),
            DMA(()), DMA((16,)), DMA((16,)), DMA((4,)),
        ],
        compiler_params=pltpu.CompilerParams(vmem_limit_bytes=30 * 1024 * 1024),
    )(att, counts)
    new = pl.pallas_call(
        last_kernel,
        name="project_out",
        out_shape=sds((T, S, W), BF),
        in_specs=[vm] * 4,
        out_specs=vm,
        scratch_shapes=[
            VMEM((4, NO, RO, HD), BF),
            VMEM((NO, 6, RO, W), BF),
            VMEM((NO, 2, RO // 2, W), BF),
            VMEM((NO, 5, RO, W), F32),
            VMEM((NO, 6, RO, W), BF),
            VMEM((NO, 2, RO // 2, W), BF),
            VMEM((S, RO, W), F32),
            DMA((NO, 3)), DMA((NO, 3)),
            DMA((NO, 6)), DMA((NO, 6)),
            DMA((NO, 2)), DMA((NO, 2)),
        ],
        compiler_params=pltpu.CompilerParams(
            collective_id=1, has_side_effects=True, vmem_limit_bytes=30 * 1024 * 1024
        ),
    )(ctx, w_out, streams, mix_cols)
    return pl.pallas_call(
        store_kernel,
        name="store",
        out_shape=sds((T, S, W), BF),
        in_specs=[vm],
        out_specs=hbm,
        scratch_shapes=[DMA((4,))],
        compiler_params=pltpu.CompilerParams(vmem_limit_bytes=8 * 1024 * 1024),
    )(new)


def solution(mesh):
    in_specs = (
        P("seq", None, "tp"),
        P("seq"),
        P(None, "tp", None),
        P(),
        P(),
        P(None, None, "tp"),
        P("tp", None),
    )
    return jax.shard_map(
        local, mesh=mesh, in_specs=in_specs, out_specs=P("seq", None, "tp"), check_vma=False
    )
```

```python
import jax
import jax.numpy as jnp
from jax import lax
from jax.experimental import pallas as pl
from jax.experimental.pallas import tpu as pltpu
from jax.sharding import PartitionSpec as P

D = 4096
HD = 128
S = 4
ROUNDS = 20
EPS = 1e-6
T = 512
W = 512
NC = 8
NO = 4
RO = T // NO
BLOCKS = 160
TILES = 9216
HALF = 256
AHEAD = 3
R = T // NC
F32 = jnp.float32
BF = jnp.bfloat16
MESH = pl.DeviceIdType.MESH
NT = (((1,), (1,)), ((), ()))
NEG = -1e30
VMEM = pltpu.VMEM
DMA = pltpu.SemaphoreType.DMA


def where_am_i():
    seq = lax.axis_index("seq")
    tp = lax.axis_index("tp")
    return seq, tp


def remote(src, dst, ssem, rsem, seq, tp):
    return pltpu.make_async_remote_copy(
        src_ref=src, dst_ref=dst, send_sem=ssem, recv_sem=rsem,
        device_id={"seq": seq, "tp": tp}, device_id_type=MESH,
    )


def greet(peers):
    barrier = pltpu.get_barrier_semaphore()
    for seq, tp in peers:
        pl.semaphore_signal(barrier, inc=1, device_id={"seq": seq, "tp": tp}, device_id_type=MESH)
    return lambda: pl.semaphore_wait(barrier, len(peers))


def columns(rows8):
    k = rows8.shape[0]
    if k < 128:
        rows8 = jnp.concatenate([rows8, jnp.zeros((128 - k, rows8.shape[1]), F32)], axis=0)
    return rows8.T


def balanced(e0, e1):
    sub = lax.broadcasted_iota(jnp.int32, e0.shape, 0)
    even, low = sub % 2 == 0, sub % 4 < 2

    def row_total(e):
        u = e + jnp.where(even, pltpu.roll(e, 7, 0), pltpu.roll(e, 1, 0))
        return u + jnp.where(low, pltpu.roll(u, 6, 0), pltpu.roll(u, 2, 0))

    def one_round(_, pair):
        e0, e1 = pair
        e0 = e0 / row_total(e0)
        e1 = e1 / row_total(e1)
        t = e0 + e1
        t = t + pltpu.roll(t, 4, 0)
        return e0 / t, e1 / t

    return lax.fori_loop(0, ROUNDS, one_round, (e0, e1))


def first_kernel(
    x_hbm, docs_hbm, wmix_hbm, bias_hbm, gain_hbm, w_hbm,
    att, mix_cols, counts,
    xraw, xs, docs, wmix, bias, gain,
    wbuf, g, sb, gained, norms, unow, urecv, nall, nrecv, csend, crecv, pre_cols,
    x_sem, i_sem, w_sem, u_ss, u_rs, n_ss, n_rs, c_ss, c_rs, g_ss, g_rs, a_ss, a_rs, q_rs, o_sem, t_sem,
    sib_ss, sib_rs, x_ss, x_rs, sib2_ss, sib2_rs,
):
    seq, tp = where_am_i()
    yhi, z, core = seq // 8, (seq // 2) % 4, seq % 2
    x, y = tp // 2, tp % 2
    sibling, mirror = seq + 1 - 2 * core, (seq + 8) % 16
    tp_peers = [(seq, (tp + r) % 8) for r in range(1, 8)]
    z_peers = [yhi * 8 + ((z + d) % 4) * 2 + core for d in range(1, 4)]
    entered = greet(tp_peers + [(p, tp) for p in z_peers] + [(sibling, tp), (mirror, tp)])

    small = [
        pltpu.make_async_copy(a, b, i_sem.at[i])
        for i, (a, b) in enumerate(
            ((wmix_hbm, wmix), (docs_hbm, docs), (bias_hbm, bias), (gain_hbm, gain))
        )
    ]
    parts_of_x = [
        pltpu.make_async_copy(x_hbm.at[pl.ds(q * 128, 128)], xraw.at[pl.ds(q * 128, 128)], x_sem.at[q])
        for q in range(4)
    ]
    small[0].start()
    for q in range(4):
        parts_of_x[q].start()
    for k in range(1, 4):
        small[k].start()

    def wcopy(i):
        return pltpu.make_async_copy(w_hbm.at[i], wbuf.at[i], w_sem)

    small[0].wait()
    parts = []
    for s in range(S):
        w = jnp.concatenate([wmix[s], jnp.zeros((8, W), F32)], axis=0)
        hi = w.astype(BF).astype(F32)
        mid = (w - hi).astype(BF).astype(F32)
        low = (w - hi) - mid
        parts.append(jnp.concatenate([hi, mid, low], axis=0).astype(BF))
    sub = lax.broadcasted_iota(jnp.int32, (8, 128), 0)
    for q in range(4):
        rows = slice(q * 128, (q + 1) * 128)
        parts_of_x[q].wait()
        if q == 3:
            for i in range(3):
                wcopy(i).start()
        xs[:, rows, :] = jnp.swapaxes(xraw[rows], 0, 1)
        acc = jnp.zeros((128, 128), F32)
        logits = jnp.zeros((32, 128), F32)
        for s in range(S):
            xv = xs[s, rows, :]
            got = lax.dot_general(parts[s], xv, NT, preferred_element_type=F32)
            logits = logits + (got[0:32] + (got[32:64] + got[64:96]))
            x32 = xv.astype(F32)
            sq = x32 * x32
            acc = acc + ((sq[:, 0:128] + sq[:, 128:256]) + (sq[:, 256:384] + sq[:, 384:512]))
        squares = jnp.sum(acc.T, axis=0, keepdims=True)
        unow[:, rows] = jnp.where(
            sub < 4, logits[0:8], jnp.where(sub == 4, jnp.broadcast_to(squares, (8, 128)), 0.0)
        )
        nall[0, :, rows] = logits[0:24]

    entered()
    for r, (sq_, tp_) in enumerate(tp_peers):
        remote(unow, urecv.at[r], u_ss, u_rs, sq_, tp_).start()

    def to_y():
        return remote(nall.at[0], nrecv.at[0], n_ss.at[0], n_rs.at[0], seq, x * 2 + 1 - y)

    def to_x(k):
        return remote(nall.at[1], nrecv.at[k], n_ss.at[1], n_rs.at[1], seq, ((x + k) % 4) * 2 + y)

    to_y().start()
    for k in range(1, 4):
        small[k].wait()
    dv = docs[...]
    cv = jnp.zeros((8, 128), jnp.int32)
    for k in range(1, 4):
        n = jnp.sum(jnp.where(dv < k, 1, 0), axis=1, keepdims=True)
        n = jnp.sum(n, axis=0, keepdims=True)
        cv = jnp.where(sub == k, jnp.broadcast_to(n, (8, 128)), cv)
    csend[0] = cv
    diag = lax.broadcasted_iota(jnp.int32, (24, 24), 0) == lax.broadcasted_iota(jnp.int32, (24, 24), 1)
    bias_col = jnp.sum(jnp.where(diag, jnp.broadcast_to(bias[...], (24, 24)), 0.0), axis=1, keepdims=True)

    def count_to(level, k, to):
        return remote(csend.at[level], crecv.at[k], c_ss, c_rs.at[level], to, tp)

    total = unow[...]
    remote(urecv, urecv, u_ss, u_rs, seq, tp_peers[0][1]).wait_recv()
    for r in range(7):
        total = total + urecv[r]
    inv_rms = lax.rsqrt(total[4:5] / (S * D) + EPS)
    pre = 1.0 / (1.0 + jnp.exp(-(total * inv_rms + bias_col[0:8])))
    pre_cols[...] = columns(pre)

    right = ((x + 1) % 4) * 2 + y
    left = ((x + 3) % 4) * 2 + y
    other_y = x * 2 + 1 - y
    b_p = other_y
    b_l0 = left
    b_r1 = ((x + 1) % 4) * 2 + 1 - y

    def move(c, blk, role, to):
        return remote(g.at[c, blk], g.at[c, blk], g_ss, g_rs.at[c, role], seq, to)

    def arrived(c, role, n):
        some = g.at[c, pl.ds(0, n)]
        remote(some, some, g_ss, g_rs.at[c, role], seq, right).wait_recv()

    def make_chunk(c):
        rows = slice(c * R, (c + 1) * R)
        v = pre_cols[rows, 0:1] * xs[0, rows, :].astype(F32)
        for s in range(1, S):
            v = v + pre_cols[rows, s : s + 1] * xs[s, rows, :].astype(F32)
        g[c, tp] = v.astype(BF)

    def send_chunk(c):
        move(c, tp, 0, other_y).start()
        move(c, tp, 1, right).start()
        move(c, tp, 3, left).start()

    make_chunk(0)
    for c in range(NC):
        if c + 1 < NC:
            make_chunk(c + 1)
        if c < AHEAD:
            send_chunk(c)
    for d in range(3):
        count_to(0, d, z_peers[d]).start()
    pltpu.make_async_copy(w_hbm, wbuf, w_sem).wait()

    def block_of(half, d):
        return half * 8 + ((z + 4 - d) % 4) * 2 + core

    two = pl.ds(0, 2)

    def spread(c, d):
        return remote(
            sb.at[(z + d) % 4, c, two], att.at[seq, c, two],
            a_ss, a_rs.at[c], z_peers[d - 1], tp,
        )

    def spread_in(c):
        ref = sb.at[pl.ds(0, 3), c, two]
        remote(ref, ref, a_ss, a_rs.at[c], z_peers[0], tp).wait_recv()

    def spread_q(c, d):
        return remote(
            sb.at[(z + d) % 4, c, 2], att.at[seq, c, 2],
            a_ss, q_rs, z_peers[d - 1], tp,
        )

    def kept():
        return pltpu.make_async_copy(sb.at[z], att.at[seq], o_sem)

    def kv(c, d):
        return sb.at[z, c, pl.ds(0, 2)] if d == 0 else att.at[block_of(yhi, d), c, pl.ds(0, 2)]

    def twin(c, d):
        dst = att.at[block_of(yhi, d), c, pl.ds(0, 2)]
        return remote(kv(c, d), dst, sib_ss, sib_rs, sibling, tp)

    def cross(c, d):
        dst = att.at[block_of(0, d), c, pl.ds(0, 2)]
        return remote(kv(c, d), dst, x_ss, x_rs.at[c], mirror, tp)

    def twin2(c, d):
        ref = att.at[block_of(0, d), c, pl.ds(0, 2)]
        return remote(ref, ref, sib2_ss, sib2_rs, sibling, tp)

    def hand_on(i):
        arrived(i, 0, 1)
        move(i, b_p, 3, right).start()
        move(i, b_p, 2, left).start()

    hand_on(0)

    def feed(i):
        @pl.when(i + AHEAD < NC)
        def _():
            send_chunk(i + AHEAD)

        @pl.when(i + 1 < NC)
        def _():
            hand_on(i + 1)

        @pl.when(i < NC)
        def _():
            arrived(i, 1, 1)
            move(i, b_l0, 3, right).start()
            arrived(i, 2, 1)
            move(i, b_r1, 3, left).start()

    def projected(c0):
        for e in range(2):
            c = c0 + e
            rows = slice(e * R, (e + 1) * R)
            arrived(c, 3, 4)
            ss = jnp.zeros((R, 128), F32)
            for b in range(8):
                g32 = g[c, b].astype(F32)
                q = g32 * g32
                ss = ss + ((q[:, 0:128] + q[:, 128:256]) + (q[:, 256:384] + q[:, 384:512]))
                gained[rows, b * W : (b + 1) * W] = (g32 * gain[:, b * W : (b + 1) * W]).astype(BF)
            norms[rows, :] = jnp.broadcast_to(
                lax.rsqrt(jnp.sum(ss, axis=1, keepdims=True) / D + EPS), (R, 128)
            )
        norm = norms[:, 0:1]
        lhs = gained[...]

        def project(slot, third):
            out = (jnp.dot(lhs, wbuf[third], preferred_element_type=F32) * norm).astype(BF)
            for h in range(4):
                for e in range(2):
                    sb[h, c0 + e, slot] = out[e * R : (e + 1) * R, h * HD : (h + 1) * HD]

        project(0, 1)
        project(1, 2)
        for e in range(2):
            for d in (2, 1, 3):
                spread(c0 + e, d).start()
        project(2, 0)
        for e in range(2):
            for d in (2, 1, 3):
                spread_q(c0 + e, d).start()

    def share(c):
        spread_in(c)
        for d in range(4):

            @pl.when(yhi == 0)
            def _():
                cross(c, d).start()

            twin(c, d).start()

    def share_far(c):
        ref = sb.at[:, c, two]
        remote(ref, ref, x_ss, x_rs.at[c], mirror, tp).wait_recv()
        for d in range(4):
            twin2(c, d).start()

    def step(i, carry):
        feed(2 * i)

        @pl.when(i >= 1)
        def _():
            projected(2 * i - 2)

        feed(2 * i + 1)

        @pl.when(i >= 1)
        def _():
            share(2 * i - 2)
            share(2 * i - 1)

        @pl.when((i >= 2) & (yhi == 1))
        def _():
            share_far(2 * i - 4)
            share_far(2 * i - 3)

        @pl.when(i == NC // 2 - 1)
        def _():
            for k in (2, 1, 3):
                to_x(k).start()

        @pl.when(i == 1)
        def _():
            to_y().wait_recv()
            nall[1] = nall[0] + nrecv[0]
            v = csend[0]
            remote(crecv.at[pl.ds(0, 3)], crecv.at[pl.ds(0, 3)], c_ss, c_rs.at[0], sibling, tp).wait_recv()
            for d in range(3):
                v = v + crecv[d]
            csend[1] = v

        @pl.when(i == 2)
        def _():
            count_to(1, 3, sibling).start()

        @pl.when(i == 3)
        def _():
            count_to(1, 3, sibling).wait_recv()
            csend[2] = csend[1] + crecv[3]

        @pl.when(i == 4)
        def _():
            count_to(2, 4, mirror).start()

        return carry

    lax.fori_loop(0, NC // 2 + 1, step, 0)
    kept().start()

    count_to(2, 4, mirror).wait_recv()
    csend[3] = csend[2] + crecv[4]
    told = pltpu.make_async_copy(csend.at[3], counts.at[0], t_sem)
    told.start()
    three = nrecv.at[pl.ds(1, 3)]
    remote(three, three, n_ss.at[1], n_rs.at[1], seq, right).wait_recv()
    ztot = (nall[1] + nrecv[1]) + (nrecv[2] + nrecv[3])
    ztot = ztot * inv_rms + bias_col
    post = 2.0 / (1.0 + jnp.exp(-ztot[0:8]))
    e0, e1 = balanced(jnp.exp(ztot[8:16]), jnp.exp(ztot[16:24]))
    mix_cols[...] = columns(jnp.concatenate([post, e0, e1], axis=0))

    @pl.when(yhi == 1)
    def _():
        share_far(NC - 2)
        share_far(NC - 1)

    told.wait()
    kept().wait()

    def all_of(ref, ssem, rsem):
        return remote(ref, ref, ssem, rsem, sibling, tp)

    all_of(urecv, u_ss, u_rs).wait_send()
    all_of(nall.at[0], n_ss.at[0], n_rs.at[0]).wait_send()
    all_of(three, n_ss.at[1], n_rs.at[1]).wait_send()
    all_of(crecv, c_ss, c_rs.at[0]).wait_send()
    all_of(g.at[pl.ds(0, 7)], g_ss, g_rs.at[0, 0]).wait_send()
    all_of(sb.at[pl.ds(0, 3)], a_ss, a_rs.at[0]).wait_send()
    all_of(sb.at[pl.ds(0, 3), :, 2], a_ss, q_rs).wait_recv()
    twins = all_of(sb.at[:, :, two], sib_ss, sib_rs)
    twins.wait_send()
    twins.wait_recv()

    @pl.when(yhi == 0)
    def _():
        all_of(sb.at[:, :, two], x_ss, x_rs.at[0]).wait_send()

    @pl.when(yhi == 1)
    def _():
        far = all_of(sb.at[:, :, two], sib2_ss, sib2_rs)
        far.wait_send()
        far.wait_recv()


def attention_kernel(att_hbm, cnt_hbm, ctx, att, cnt, vx, m_ref, acc_ref, c_sem, k_sem, v_sem, q_sem):
    seq = lax.axis_index("seq")
    yhi, core = seq // 8, seq % 2
    counts_in = pltpu.make_async_copy(cnt_hbm.at[0], cnt, c_sem)
    counts_in.start()

    def q_in(qi):
        qb = yhi * 8 + qi * 2 + core
        return pltpu.make_async_copy(att_hbm.at[qb, :, 2], att.at[qb, :, 2], q_sem.at[qi])

    def k_in(kb):
        return pltpu.make_async_copy(att_hbm.at[kb, :, 0], att.at[kb, :, 0], k_sem.at[kb])

    def v_in(kb):
        return pltpu.make_async_copy(att_hbm.at[kb, :, 1], vx.at[kb, :, :, pl.ds(0, HD)], v_sem.at[kb])

    q_in(0).start()
    k_in(yhi * 8 + core).start()
    v_in(yhi * 8 + core).start()
    counts_in.wait()
    starts = [cnt[k, 0] for k in range(1, 4)]
    scale = HD ** (-0.5) * 1.4426950408889634

    def start_of(p):
        v = p * 0
        for c in starts:
            v = jnp.where(c <= p, jnp.maximum(v, c), v)
        return v

    first_needed = start_of((yhi * 8 + core) * T) // T

    def fetch(kb, c):
        k_in(kb).start()
        v_in(kb).start()
        return c

    def land(kb, c):
        k_in(kb).wait()
        v_in(kb).wait()
        return c

    lax.fori_loop(first_needed, yhi * 8 + core, fetch, 0)
    for qi in range(1, 4):
        q_in(qi).start()
    lax.fori_loop(yhi * 8 + core + 1, yhi * 8 + core + 7, fetch, 0)

    def ones(kb, c):
        vx[kb, :, :, HD:] = jnp.ones((NC, R, HD), BF)
        return c

    lax.fori_loop(first_needed, yhi * 8 + core + 7, ones, 0)

    def one_query_block(qi, carry):
        qb = yhi * 8 + qi * 2 + core
        q_in(qi).wait()
        land(qb, 0)
        q = att[qb, :, 2].reshape(T, HD)
        first = start_of(qb * T)
        last = start_of(qb * T + T - 1)
        lo = first // T
        mid = jnp.minimum((last + T - 1) // T, qb)
        qpos = qb * T + lax.broadcasted_iota(jnp.int32, (T, 1), 0)
        qstart = start_of(qpos)
        def block(kb, mode, n=1):
            k = att[pl.ds(kb, n), :, 0].reshape(n * T, HD)
            v = vx[pl.ds(kb, n)].reshape(n * T, 2 * HD)

            def scores(t):
                rows = slice(t * HALF, (t + 1) * HALF)
                s = lax.dot_general(q[rows], k, NT, preferred_element_type=F32)
                if mode != "all":
                    kpos = kb * T + lax.broadcasted_iota(jnp.int32, (1, T), 1)
                    ok = kpos >= qstart[rows]
                    if mode == "diagonal":
                        ok = ok & (kpos <= qpos[rows])
                    s = jnp.where(ok, s, NEG)
                return s

            later = scores(0)
            for t in range(T // HALF):
                rows = slice(t * HALF, (t + 1) * HALF)
                s = later
                if (t + 1) * HALF < T:
                    later = scores(t + 1)
                top = s[:, 0:128]
                for e in range(1, n * 4):
                    top = jnp.maximum(top, s[:, e * 128 : (e + 1) * 128])
                m_new = jnp.max(top, axis=1, keepdims=True)
                if mode != "diagonal":
                    m_old = m_ref[rows, 0:1]
                    m_new = jnp.maximum(m_old, m_new)
                    alpha = jnp.exp2((m_old - m_new) * scale)
                p = jnp.exp2((s - m_new) * scale).astype(BF)
                more = jnp.dot(p, v, preferred_element_type=F32)
                acc_ref[rows] = more if mode == "diagonal" else acc_ref[rows] * alpha + more
                m_ref[rows] = jnp.broadcast_to(m_new, (HALF, 128))

        def some(kb, c):
            block(kb, "start")
            return c

        def two(k, c):
            block(mid + 2 * k, "all", 2)
            return c

        def one(kb, c):
            block(kb, "all")
            return c

        block(qb, "diagonal")
        lax.fori_loop(jnp.where(qi == 0, first_needed, qb - 1), qb, land, 0)
        lax.fori_loop(lo, mid, some, 0)
        pairs = (qb - mid) // 2
        lax.fori_loop(0, pairs, two, 0)
        lax.fori_loop(mid + 2 * pairs, qb, one, 0)
        out = acc_ref[:, 0:HD] / acc_ref[:, HD : HD + 1]
        ctx[qi] = out.astype(BF).reshape(NO, RO, HD)
        return carry

    lax.fori_loop(0, 4, one_query_block, 0)


def last_kernel(
    ctx, wbuf, xraw, cols,
    out,
    cbuf, snd, snh, own, rcv, rch, kept,
    z_ss, z_rs, s_ss, s_rs, h_ss, h_rs,
):
    seq, tp = where_am_i()
    yhi, z, core = seq // 8, (seq // 2) % 4, seq % 2
    x, y = tp // 2, tp % 2
    right = ((x + 1) % 4) * 2 + y
    left = ((x + 3) % 4) * 2 + y
    other_y = x * 2 + 1 - y
    z_peers = [yhi * 8 + ((z + d) % 4) * 2 + core for d in range(1, 4)]
    entered = greet([(p, tp) for p in z_peers] + [(seq, right), (seq, left), (seq, other_y)])
    entered()

    def back(c, d):
        return remote(
            ctx.at[(z + d) % 4, c], cbuf.at[z, c], z_ss, z_rs.at[c], z_peers[d - 1], tp
        )

    def back_in(c):
        ref = ctx.at[pl.ds(0, 3), c]
        remote(ref, ref, z_ss, z_rs.at[c], z_peers[0], tp).wait_recv()

    for c in range(NO):
        for d in (2, 1, 3):
            back(c, d).start()
    cbuf[z] = ctx[z]

    def pass_on(c, k, to):
        return remote(snd.at[c, k], rcv.at[c, k], s_ss, s_rs.at[c, k], seq, to)

    def half(c, k, to):
        return remote(snh.at[c, k], rch.at[c, k], h_ss, h_rs.at[c, k], seq, to)

    to_right, to_left, far = ((x + 1) % 4) * 2, ((x + 3) % 4) * 2, ((x + 2) % 4) * 2

    def project(c, carry):
        back_in(c)
        lhs = jnp.concatenate([cbuf[h, c] for h in range(4)], axis=1)

        def term(b):
            cols = pl.ds(pl.multiple_of(b * W, W), W)
            return jnp.dot(lhs, wbuf[:, cols], preferred_element_type=F32)

        snd[c, 0] = term(far + 1 - y).astype(BF)
        snd[c, 1] = term(to_right + 1 - y).astype(BF)
        pass_on(c, 0, other_y).start()
        snd[c, 2] = term(to_left + 1 - y).astype(BF)
        pass_on(c, 1, right).start()
        own[c, 0] = term(far + y)
        pass_on(c, 2, left).start()
        own[c, 1] = term(to_right + y)
        own[c, 2] = term(to_left + y)
        own[c, 3] = term(other_y)
        own[c, 4] = term(tp)
        return carry

    lax.fori_loop(0, NO, project, 0)

    def second(c, carry):
        pass_on(c, 0, other_y).wait_recv()
        far_sum = (own[c, 0] + rcv[c, 0].astype(F32)).astype(BF)
        snh[c, 0] = far_sum[0 : RO // 2]
        snh[c, 1] = far_sum[RO // 2 :]
        half(c, 0, right).start()
        half(c, 1, left).start()
        return carry

    lax.fori_loop(0, NO, second, 0)

    def third(c, carry):
        pass_on(c, 1, right).wait_recv()
        pass_on(c, 2, left).wait_recv()
        snd[c, 5] = (own[c, 3] + (rcv[c, 1].astype(F32) + rcv[c, 2].astype(F32))).astype(BF)
        pass_on(c, 5, other_y).start()
        half(c, 0, right).wait_recv()
        snd[c, 3, 0 : RO // 2] = (own[c, 1, 0 : RO // 2] + rch[c, 0].astype(F32)).astype(BF)
        snd[c, 3, RO // 2 :] = own[c, 1, RO // 2 :].astype(BF)
        pass_on(c, 3, right).start()
        half(c, 1, left).wait_recv()
        snd[c, 4, 0 : RO // 2] = own[c, 2, 0 : RO // 2].astype(BF)
        snd[c, 4, RO // 2 :] = (own[c, 2, RO // 2 :] + rch[c, 1].astype(F32)).astype(BF)
        pass_on(c, 4, left).start()
        return carry

    lax.fori_loop(0, NO, third, 0)

    def fourth(c, carry):
        rows = pl.ds(pl.multiple_of(c * RO, RO), RO)
        xv = jnp.swapaxes(xraw[rows], 0, 1)
        wide = [xv[j].astype(F32) for j in range(S)]
        for i in range(S):
            k = 8 + 4 * i
            v = cols[rows, k : k + 1] * wide[0]
            for j in range(1, S):
                v = v + cols[rows, k + j : k + j + 1] * wide[j]
            kept[i] = v
        pass_on(c, 5, other_y).wait_recv()
        mine = own[c, 4] + rcv[c, 5].astype(F32)
        pass_on(c, 3, right).wait_recv()
        pass_on(c, 4, left).wait_recv()
        branch = mine + (rcv[c, 3].astype(F32) + rcv[c, 4].astype(F32))
        new = [(kept[i] + cols[rows, 4 + i : 5 + i] * branch).astype(BF) for i in range(S)]
        out[rows] = jnp.swapaxes(jnp.stack(new, axis=0), 0, 1)
        return carry

    lax.fori_loop(0, NO, fourth, 0)

    everything = ctx.at[pl.ds(0, 3)]
    remote(everything, everything, z_ss, z_rs.at[0], seq, right).wait_send()
    remote(snd, snd, s_ss, s_rs.at[0, 0], seq, right).wait_send()
    remote(snh, snh, h_ss, h_rs.at[0, 0], seq, right).wait_send()


def store_kernel(x, out, sem):
    copies = [
        pltpu.make_async_copy(x.at[pl.ds(q * 128, 128)], out.at[pl.ds(q * 128, 128)], sem.at[q])
        for q in range(4)
    ]
    for copy in copies:
        copy.start()
    for copy in copies:
        copy.wait()


def local(streams, doc_ids, mix_weight, mix_bias, attn_gain, w_qkv, w_out):
    wmix = jnp.transpose(mix_weight, (0, 2, 1))
    wq = jnp.transpose(w_qkv, (1, 0, 2))
    vm = pl.BlockSpec(memory_space=VMEM)
    hbm = pl.BlockSpec(memory_space=pl.ANY)
    sds = jax.ShapeDtypeStruct
    att, mix_cols, counts = pl.pallas_call(
        first_kernel,
        name="gather_project",
        out_shape=(
            sds((BLOCKS, NC, 3, R, HD), BF),
            sds((T, 128), F32),
            sds((TILES, 8, 128), jnp.int32),
        ),
        in_specs=[hbm] * 6,
        out_specs=(hbm, vm, hbm),
        scratch_shapes=[
            VMEM((T, S, W), BF),
            VMEM((S, T, W), BF),
            VMEM((4, 128), jnp.int32),
            VMEM((S, 24, W), F32),
            VMEM((1, 24), F32),
            VMEM((1, D), F32),
            VMEM((3, D, W), BF),
            VMEM((NC, 8, R, W), BF),
            VMEM((4, NC, 3, R, HD), BF),
            VMEM((2 * R, D), BF),
            VMEM((2 * R, 128), F32),
            VMEM((8, T), F32),
            VMEM((7, 8, T), F32),
            VMEM((2, 24, T), F32),
            VMEM((4, 24, T), F32),
            VMEM((4, 8, 128), jnp.int32),
            VMEM((5, 8, 128), jnp.int32),
            VMEM((T, 128), F32),
            DMA((4,)),
            DMA((4,)),
            DMA(()),
            DMA(()), DMA(()),
            DMA((2,)), DMA((2,)),
            DMA(()), DMA((3,)),
            DMA(()), DMA((NC, 4)),
            DMA(()), DMA((NC,)),
            DMA(()),
            DMA(()),
            DMA(()),
            DMA(()), DMA(()),
            DMA(()), DMA((NC,)),
            DMA(()), DMA(()),
        ],
        compiler_params=pltpu.CompilerParams(
            collective_id=0, has_side_effects=True, vmem_limit_bytes=60 * 1024 * 1024
        ),
    )(
        streams, doc_ids.reshape(4, 128), wmix, mix_bias.reshape(1, 24), attn_gain.reshape(1, D), wq,
    )
    ctx = pl.pallas_call(
        attention_kernel,
        name="attention",
        out_shape=sds((4, NO, RO, HD), BF),
        in_specs=[hbm, hbm],
        out_specs=vm,
        scratch_shapes=[
            VMEM((16, NC, 3, R, HD), BF),
            pltpu.SMEM((8, 128), jnp.int32),
            VMEM((16, NC, R, 2 * HD), BF),
            VMEM((T, 128), F32), VMEM((T, 2 * HD), F32),
            DMA(()), DMA((16,)), DMA((16,)), DMA((4,)),
        ],
        compiler_params=pltpu.CompilerParams(vmem_limit_bytes=30 * 1024 * 1024),
    )(att, counts)
    new = pl.pallas_call(
        last_kernel,
        name="project_out",
        out_shape=sds((T, S, W), BF),
        in_specs=[vm] * 4,
        out_specs=vm,
        scratch_shapes=[
            VMEM((4, NO, RO, HD), BF),
            VMEM((NO, 6, RO, W), BF),
            VMEM((NO, 2, RO // 2, W), BF),
            VMEM((NO, 5, RO, W), F32),
            VMEM((NO, 6, RO, W), BF),
            VMEM((NO, 2, RO // 2, W), BF),
            VMEM((S, RO, W), F32),
            DMA(()), DMA((NO,)),
            DMA(()), DMA((NO, 6)),
            DMA(()), DMA((NO, 2)),
        ],
        compiler_params=pltpu.CompilerParams(
            collective_id=1, has_side_effects=True, vmem_limit_bytes=30 * 1024 * 1024
        ),
    )(ctx, w_out, streams, mix_cols)
    return pl.pallas_call(
        store_kernel,
        name="store",
        out_shape=sds((T, S, W), BF),
        in_specs=[vm],
        out_specs=hbm,
        scratch_shapes=[DMA((4,))],
        compiler_params=pltpu.CompilerParams(vmem_limit_bytes=8 * 1024 * 1024),
    )(new)


def solution(mesh):
    in_specs = (
        P("seq", None, "tp"),
        P("seq"),
        P(None, "tp", None),
        P(),
        P(),
        P(None, None, "tp"),
        P("tp", None),
    )
    return jax.shard_map(
        local, mesh=mesh, in_specs=in_specs, out_specs=P("seq", None, "tp"), check_vma=False
    )
```

```python
import jax
import jax.numpy as jnp
from jax import lax
from jax.experimental import pallas as pl
from jax.experimental.pallas import tpu as pltpu
from jax.sharding import PartitionSpec as P

D = 4096
HD = 128
S = 4
ROUNDS = 20
EPS = 1e-6
T = 512
W = 512
NC = 8
NO = 4
RO = T // NO
BLOCKS = 160
TILES = 9216
HALF = 256
AHEAD = 4
HANDED = 2
R = T // NC
F32 = jnp.float32
BF = jnp.bfloat16
MESH = pl.DeviceIdType.MESH
NT = (((1,), (1,)), ((), ()))
NEG = -1e30
VMEM = pltpu.VMEM
DMA = pltpu.SemaphoreType.DMA


def where_am_i():
    seq = lax.axis_index("seq")
    tp = lax.axis_index("tp")
    return seq, tp


def remote(src, dst, ssem, rsem, seq, tp):
    return pltpu.make_async_remote_copy(
        src_ref=src, dst_ref=dst, send_sem=ssem, recv_sem=rsem,
        device_id={"seq": seq, "tp": tp}, device_id_type=MESH,
    )


def greet(peers):
    barrier = pltpu.get_barrier_semaphore()
    for seq, tp in peers:
        pl.semaphore_signal(barrier, inc=1, device_id={"seq": seq, "tp": tp}, device_id_type=MESH)
    return lambda: pl.semaphore_wait(barrier, len(peers))


def columns(rows8):
    k = rows8.shape[0]
    if k < 128:
        rows8 = jnp.concatenate([rows8, jnp.zeros((128 - k, rows8.shape[1]), F32)], axis=0)
    return rows8.T


def balanced(e0, e1):
    sub = lax.broadcasted_iota(jnp.int32, e0.shape, 0)
    even, low = sub % 2 == 0, sub % 4 < 2

    def row_total(e):
        u = e + jnp.where(even, pltpu.roll(e, 7, 0), pltpu.roll(e, 1, 0))
        return u + jnp.where(low, pltpu.roll(u, 6, 0), pltpu.roll(u, 2, 0))

    def one_round(_, pair):
        e0, e1 = pair
        e0 = e0 / row_total(e0)
        e1 = e1 / row_total(e1)
        t = e0 + e1
        t = t + pltpu.roll(t, 4, 0)
        return e0 / t, e1 / t

    return lax.fori_loop(0, ROUNDS, one_round, (e0, e1))


def first_kernel(
    x_hbm, docs_hbm, wmix_hbm, bias_hbm, gain_hbm, w_hbm,
    att, mix_cols, counts,
    xraw, xs, docs, wmix, bias, gain,
    wbuf, g, sb, gained, norms, unow, urecv, nall, nrecv, csend, crecv, pre_cols,
    x_sem, i_sem, w_sem, u_ss, u_rs, n_ss, n_rs, c_ss, c_rs, g_ss, g_rs, a_ss, a_rs, q_rs, o_sem, t_sem,
    sib_ss, sib_rs, x_ss, x_rs, sib2_ss, sib2_rs,
):
    seq, tp = where_am_i()
    yhi, z, core = seq // 8, (seq // 2) % 4, seq % 2
    x, y = tp // 2, tp % 2
    sibling, mirror = seq + 1 - 2 * core, (seq + 8) % 16
    far_first = ((2, 1), (2, 0), (1, 1), (3, 1), (1, 0), (3, 0), (0, 1))
    tp_peers = [(seq, ((x + dx) % 4) * 2 + (y + dy) % 2) for dx, dy in far_first]
    z_peers = [yhi * 8 + ((z + d) % 4) * 2 + core for d in range(1, 4)]
    entered = greet(tp_peers + [(p, tp) for p in z_peers] + [(sibling, tp), (mirror, tp)])

    small = [
        pltpu.make_async_copy(a, b, i_sem.at[i])
        for i, (a, b) in enumerate(
            ((wmix_hbm, wmix), (docs_hbm, docs), (bias_hbm, bias), (gain_hbm, gain))
        )
    ]
    parts_of_x = [
        pltpu.make_async_copy(x_hbm.at[pl.ds(q * 128, 128)], xraw.at[pl.ds(q * 128, 128)], x_sem.at[q])
        for q in range(4)
    ]
    small[0].start()
    for q in range(4):
        parts_of_x[q].start()
    for k in range(1, 4):
        small[k].start()

    def wcopy(i):
        return pltpu.make_async_copy(w_hbm.at[i], wbuf.at[i], w_sem)

    small[0].wait()
    parts = []
    for s in range(S):
        w = jnp.concatenate([wmix[s], jnp.zeros((8, W), F32)], axis=0)
        hi = w.astype(BF).astype(F32)
        mid = (w - hi).astype(BF).astype(F32)
        low = (w - hi) - mid
        parts.append(jnp.concatenate([hi, mid, low], axis=0).astype(BF))
    sub = lax.broadcasted_iota(jnp.int32, (8, 128), 0)
    for q in range(4):
        rows = slice(q * 128, (q + 1) * 128)
        parts_of_x[q].wait()
        if q == 3:
            for i in range(3):
                wcopy(i).start()
        xs[:, rows, :] = jnp.swapaxes(xraw[rows], 0, 1)
        acc = jnp.zeros((128, 128), F32)
        logits = jnp.zeros((32, 128), F32)
        for s in range(S):
            xv = xs[s, rows, :]
            got = lax.dot_general(parts[s], xv, NT, preferred_element_type=F32)
            logits = logits + (got[0:32] + (got[32:64] + got[64:96]))
            x32 = xv.astype(F32)
            sq = x32 * x32
            acc = acc + ((sq[:, 0:128] + sq[:, 128:256]) + (sq[:, 256:384] + sq[:, 384:512]))
        squares = jnp.sum(acc.T, axis=0, keepdims=True)
        unow[:, rows] = jnp.where(
            sub < 4, logits[0:8], jnp.where(sub == 4, jnp.broadcast_to(squares, (8, 128)), 0.0)
        )
        nall[0, :, rows] = logits[0:24]

    entered()
    for r, (sq_, tp_) in enumerate(tp_peers):
        remote(unow, urecv.at[r], u_ss, u_rs, sq_, tp_).start()

    def to_y():
        return remote(nall.at[0], nrecv.at[0], n_ss.at[0], n_rs.at[0], seq, x * 2 + 1 - y)

    def to_x(k):
        return remote(nall.at[1], nrecv.at[k], n_ss.at[1], n_rs.at[1], seq, ((x + k) % 4) * 2 + y)

    to_y().start()
    for k in range(1, 4):
        small[k].wait()
    dv = docs[...]
    cv = jnp.zeros((8, 128), jnp.int32)
    for k in range(1, 4):
        n = jnp.sum(jnp.where(dv < k, 1, 0), axis=1, keepdims=True)
        n = jnp.sum(n, axis=0, keepdims=True)
        cv = jnp.where(sub == k, jnp.broadcast_to(n, (8, 128)), cv)
    csend[0] = cv
    diag = lax.broadcasted_iota(jnp.int32, (24, 24), 0) == lax.broadcasted_iota(jnp.int32, (24, 24), 1)
    bias_col = jnp.sum(jnp.where(diag, jnp.broadcast_to(bias[...], (24, 24)), 0.0), axis=1, keepdims=True)

    def count_to(level, k, to):
        return remote(csend.at[level], crecv.at[k], c_ss, c_rs.at[level], to, tp)

    total = unow[...]
    remote(urecv, urecv, u_ss, u_rs, seq, tp_peers[0][1]).wait_recv()
    for r in range(7):
        total = total + urecv[r]
    inv_rms = lax.rsqrt(total[4:5] / (S * D) + EPS)
    pre = 1.0 / (1.0 + jnp.exp(-(total * inv_rms + bias_col[0:8])))
    pre_cols[...] = columns(pre)

    right = ((x + 1) % 4) * 2 + y
    left = ((x + 3) % 4) * 2 + y
    other_y = x * 2 + 1 - y
    b_p = other_y
    b_far = ((x + 2) % 4) * 2 + y

    def half_on(c, h, to):
        rows = g.at[c, right if h else left, pl.ds(h * (R // 2), R // 2)]
        return remote(rows, rows, g_ss, g_rs.at[c, 2], seq, to)

    def move(c, blk, role, to):
        return remote(g.at[c, blk], g.at[c, blk], g_ss, g_rs.at[c, role], seq, to)

    def arrived(c, role, n):
        some = g.at[c, pl.ds(0, n)]
        remote(some, some, g_ss, g_rs.at[c, role], seq, right).wait_recv()

    def make_chunk(c):
        rows = slice(c * R, (c + 1) * R)
        v = pre_cols[rows, 0:1] * xs[0, rows, :].astype(F32)
        for s in range(1, S):
            v = v + pre_cols[rows, s : s + 1] * xs[s, rows, :].astype(F32)
        g[c, tp] = v.astype(BF)

    def send_chunk(c):
        move(c, tp, 0, other_y).start()
        move(c, tp, 1, right).start()
        move(c, tp, 1, left).start()

    make_chunk(0)
    for c in range(NC):
        if c + 1 < NC:
            make_chunk(c + 1)
        if c < AHEAD:
            send_chunk(c)
    for d in range(3):
        count_to(0, d, z_peers[d]).start()
    pltpu.make_async_copy(w_hbm, wbuf, w_sem).wait()

    def block_of(half, d):
        return half * 8 + ((z + 4 - d) % 4) * 2 + core

    two = pl.ds(0, 2)

    def spread(c, d):
        return remote(
            sb.at[(z + d) % 4, c, two], att.at[seq, c, two],
            a_ss, a_rs.at[c], z_peers[d - 1], tp,
        )

    def spread_in(c):
        ref = sb.at[pl.ds(0, 3), c, two]
        remote(ref, ref, a_ss, a_rs.at[c], z_peers[0], tp).wait_recv()

    def spread_q(c, d):
        return remote(
            sb.at[(z + d) % 4, c, 2], att.at[seq, c, 2],
            a_ss, q_rs, z_peers[d - 1], tp,
        )

    def kept():
        return pltpu.make_async_copy(sb.at[z], att.at[seq], o_sem)

    def kv(c, d):
        return sb.at[z, c, pl.ds(0, 2)] if d == 0 else att.at[block_of(yhi, d), c, pl.ds(0, 2)]

    def twin(c, d):
        dst = att.at[block_of(yhi, d), c, pl.ds(0, 2)]
        return remote(kv(c, d), dst, sib_ss, sib_rs, sibling, tp)

    def cross(c, d):
        dst = att.at[block_of(0, d), c, pl.ds(0, 2)]
        return remote(kv(c, d), dst, x_ss, x_rs.at[c], mirror, tp)

    def twin2(c, d):
        ref = att.at[block_of(0, d), c, pl.ds(0, 2)]
        return remote(ref, ref, sib2_ss, sib2_rs, sibling, tp)

    def hand_on(i):
        arrived(i, 0, 1)
        move(i, b_p, 3, right).start()
        move(i, b_p, 3, left).start()

    for c in range(HANDED):
        hand_on(c)

    def feed(i):
        @pl.when(i + AHEAD < NC)
        def _():
            send_chunk(i + AHEAD)

        @pl.when(i + HANDED < NC)
        def _():
            hand_on(i + HANDED)

        @pl.when(i < NC)
        def _():
            arrived(i, 1, 2)
            half_on(i, 0, right).start()
            half_on(i, 1, left).start()

        @pl.when((i >= 1) & (i <= NC))
        def _():
            arrived(i - 1, 2, 1)
            move(i - 1, b_far, 3, other_y).start()

    def projected(c0):
        for e in range(2):
            c = c0 + e
            rows = slice(e * R, (e + 1) * R)
            arrived(c, 3, 3)
            ss = jnp.zeros((R, 128), F32)
            for b in range(8):
                g32 = g[c, b].astype(F32)
                q = g32 * g32
                ss = ss + ((q[:, 0:128] + q[:, 128:256]) + (q[:, 256:384] + q[:, 384:512]))
                gained[rows, b * W : (b + 1) * W] = (g32 * gain[:, b * W : (b + 1) * W]).astype(BF)
            norms[rows, :] = jnp.broadcast_to(
                lax.rsqrt(jnp.sum(ss, axis=1, keepdims=True) / D + EPS), (R, 128)
            )
        norm = norms[:, 0:1]
        lhs = gained[...]

        def project(slot, third):
            out = (jnp.dot(lhs, wbuf[third], preferred_element_type=F32) * norm).astype(BF)
            for h in range(4):
                for e in range(2):
                    sb[h, c0 + e, slot] = out[e * R : (e + 1) * R, h * HD : (h + 1) * HD]

        project(0, 1)
        project(1, 2)
        for e in range(2):
            for d in (2, 1, 3):
                spread(c0 + e, d).start()
        project(2, 0)
        for e in range(2):
            for d in (2, 1, 3):
                spread_q(c0 + e, d).start()

    def share(c):
        spread_in(c)
        for d in range(4):

            @pl.when(yhi == 0)
            def _():
                cross(c, d).start()

            twin(c, d).start()

    def share_far(c):
        ref = sb.at[:, c, two]
        remote(ref, ref, x_ss, x_rs.at[c], mirror, tp).wait_recv()
        for d in range(4):
            twin2(c, d).start()

    def step(i, carry):
        @pl.when(i == 1)
        def _():
            count_to(1, 3, sibling).start()

        @pl.when(i == 2)
        def _():
            count_to(2, 4, mirror).start()

        feed(2 * i)

        @pl.when(i >= 1)
        def _():
            projected(2 * i - 2)

        feed(2 * i + 1)

        @pl.when(i == 0)
        def _():
            to_y().wait_recv()
            nall[1] = nall[0] + nrecv[0]
            v = csend[0]
            remote(crecv.at[pl.ds(0, 3)], crecv.at[pl.ds(0, 3)], c_ss, c_rs.at[0], sibling, tp).wait_recv()
            for d in range(3):
                v = v + crecv[d]
            csend[1] = v

        @pl.when(i == 1)
        def _():
            count_to(1, 3, sibling).wait_recv()
            csend[2] = csend[1] + crecv[3]

        @pl.when(i >= 1)
        def _():
            share(2 * i - 2)
            share(2 * i - 1)

        @pl.when((i >= 2) & (yhi == 1))
        def _():
            share_far(2 * i - 4)
            share_far(2 * i - 3)

        @pl.when(i == NC // 2 - 1)
        def _():
            for k in (2, 1, 3):
                to_x(k).start()

        return carry

    lax.fori_loop(0, NC // 2 + 1, step, 0)
    kept().start()

    count_to(2, 4, mirror).wait_recv()
    csend[3] = csend[2] + crecv[4]
    told = pltpu.make_async_copy(csend.at[3], counts.at[0], t_sem)
    told.start()
    three = nrecv.at[pl.ds(1, 3)]
    remote(three, three, n_ss.at[1], n_rs.at[1], seq, right).wait_recv()
    ztot = (nall[1] + nrecv[1]) + (nrecv[2] + nrecv[3])
    ztot = ztot * inv_rms + bias_col
    post = 2.0 / (1.0 + jnp.exp(-ztot[0:8]))
    e0, e1 = balanced(jnp.exp(ztot[8:16]), jnp.exp(ztot[16:24]))
    mix_cols[...] = columns(jnp.concatenate([post, e0, e1], axis=0))

    @pl.when(yhi == 1)
    def _():
        share_far(NC - 2)
        share_far(NC - 1)

    told.wait()
    kept().wait()

    def all_of(ref, ssem, rsem):
        return remote(ref, ref, ssem, rsem, sibling, tp)

    all_of(urecv, u_ss, u_rs).wait_send()
    all_of(nall.at[0], n_ss.at[0], n_rs.at[0]).wait_send()
    all_of(three, n_ss.at[1], n_rs.at[1]).wait_send()
    all_of(crecv, c_ss, c_rs.at[0]).wait_send()
    all_of(g.at[pl.ds(0, 7)], g_ss, g_rs.at[0, 0]).wait_send()
    all_of(sb.at[pl.ds(0, 3)], a_ss, a_rs.at[0]).wait_send()
    all_of(sb.at[pl.ds(0, 3), :, 2], a_ss, q_rs).wait_recv()
    twins = all_of(sb.at[:, :, two], sib_ss, sib_rs)
    twins.wait_send()
    twins.wait_recv()

    @pl.when(yhi == 0)
    def _():
        all_of(sb.at[:, :, two], x_ss, x_rs.at[0]).wait_send()

    @pl.when(yhi == 1)
    def _():
        far = all_of(sb.at[:, :, two], sib2_ss, sib2_rs)
        far.wait_send()
        far.wait_recv()


def attention_kernel(att_hbm, cnt_hbm, ctx, att, cnt, vx, m_ref, acc_ref, c_sem, k_sem, v_sem, q_sem):
    seq = lax.axis_index("seq")
    yhi, core = seq // 8, seq % 2
    counts_in = pltpu.make_async_copy(cnt_hbm.at[0], cnt, c_sem)
    counts_in.start()

    def q_in(qi):
        qb = yhi * 8 + qi * 2 + core
        return pltpu.make_async_copy(att_hbm.at[qb, :, 2], att.at[qb, :, 2], q_sem.at[qi])

    def k_in(kb):
        return pltpu.make_async_copy(att_hbm.at[kb, :, 0], att.at[kb, :, 0], k_sem.at[kb])

    def v_in(kb):
        return pltpu.make_async_copy(att_hbm.at[kb, :, 1], vx.at[kb, :, :, pl.ds(0, HD)], v_sem.at[kb])

    q_in(0).start()
    k_in(yhi * 8 + core).start()
    v_in(yhi * 8 + core).start()
    counts_in.wait()
    starts = [cnt[k, 0] for k in range(1, 4)]
    scale = HD ** (-0.5) * 1.4426950408889634

    def start_of(p):
        v = p * 0
        for c in starts:
            v = jnp.where(c <= p, jnp.maximum(v, c), v)
        return v

    first_needed = start_of((yhi * 8 + core) * T) // T

    def fetch(kb, c):
        k_in(kb).start()
        v_in(kb).start()
        return c

    def land(kb, c):
        k_in(kb).wait()
        v_in(kb).wait()
        return c

    lax.fori_loop(first_needed, yhi * 8 + core, fetch, 0)
    for qi in range(1, 4):
        q_in(qi).start()
    lax.fori_loop(yhi * 8 + core + 1, yhi * 8 + core + 7, fetch, 0)

    def ones(kb, c):
        vx[kb, :, :, HD:] = jnp.ones((NC, R, HD), BF)
        return c

    lax.fori_loop(first_needed, yhi * 8 + core + 7, ones, 0)

    def one_query_block(qi, carry):
        qb = yhi * 8 + qi * 2 + core
        q_in(qi).wait()
        land(qb, 0)
        q = att[qb, :, 2].reshape(T, HD)
        first = start_of(qb * T)
        last = start_of(qb * T + T - 1)
        lo = first // T
        mid = jnp.minimum((last + T - 1) // T, qb)
        qpos = qb * T + lax.broadcasted_iota(jnp.int32, (T, 1), 0)
        qstart = start_of(qpos)
        def block(kb, mode, n=1):
            k = att[pl.ds(kb, n), :, 0].reshape(n * T, HD)
            v = vx[pl.ds(kb, n)].reshape(n * T, 2 * HD)

            def scores(t):
                rows = slice(t * HALF, (t + 1) * HALF)
                s = lax.dot_general(q[rows], k, NT, preferred_element_type=F32)
                if mode != "all":
                    kpos = kb * T + lax.broadcasted_iota(jnp.int32, (1, T), 1)
                    ok = kpos >= qstart[rows]
                    if mode == "diagonal":
                        ok = ok & (kpos <= qpos[rows])
                    s = jnp.where(ok, s, NEG)
                return s

            later = scores(0)
            for t in range(T // HALF):
                rows = slice(t * HALF, (t + 1) * HALF)
                s = later
                if (t + 1) * HALF < T:
                    later = scores(t + 1)
                top = s[:, 0:128]
                for e in range(1, n * 4):
                    top = jnp.maximum(top, s[:, e * 128 : (e + 1) * 128])
                m_new = jnp.max(top, axis=1, keepdims=True)
                if mode != "diagonal":
                    m_old = m_ref[rows, 0:1]
                    m_new = jnp.maximum(m_old, m_new)
                    alpha = jnp.exp2((m_old - m_new) * scale)
                p = jnp.exp2((s - m_new) * scale).astype(BF)
                more = jnp.dot(p, v, preferred_element_type=F32)
                acc_ref[rows] = more if mode == "diagonal" else acc_ref[rows] * alpha + more
                m_ref[rows] = jnp.broadcast_to(m_new, (HALF, 128))

        def some(kb, c):
            block(kb, "start")
            return c

        def two(k, c):
            block(mid + 2 * k, "all", 2)
            return c

        def one(kb, c):
            block(kb, "all")
            return c

        block(qb, "diagonal")
        lax.fori_loop(jnp.where(qi == 0, first_needed, qb - 1), qb, land, 0)
        lax.fori_loop(lo, mid, some, 0)
        pairs = (qb - mid) // 2
        lax.fori_loop(0, pairs, two, 0)
        lax.fori_loop(mid + 2 * pairs, qb, one, 0)
        out = acc_ref[:, 0:HD] / acc_ref[:, HD : HD + 1]
        ctx[qi] = out.astype(BF).reshape(NO, RO, HD)
        return carry

    lax.fori_loop(0, 4, one_query_block, 0)


def last_kernel(
    ctx, wbuf, xraw, cols,
    out,
    cbuf, snd, snh, own, rcv, rch, kept,
    z_ss, z_rs, s_ss, s_rs, h_ss, h_rs,
):
    seq, tp = where_am_i()
    yhi, z, core = seq // 8, (seq // 2) % 4, seq % 2
    x, y = tp // 2, tp % 2
    right = ((x + 1) % 4) * 2 + y
    left = ((x + 3) % 4) * 2 + y
    other_y = x * 2 + 1 - y
    z_peers = [yhi * 8 + ((z + d) % 4) * 2 + core for d in range(1, 4)]
    entered = greet([(p, tp) for p in z_peers] + [(seq, right), (seq, left), (seq, other_y)])
    entered()

    def back(c, d):
        return remote(
            ctx.at[(z + d) % 4, c], cbuf.at[z, c], z_ss, z_rs.at[c], z_peers[d - 1], tp
        )

    def back_in(c):
        ref = ctx.at[pl.ds(0, 3), c]
        remote(ref, ref, z_ss, z_rs.at[c], z_peers[0], tp).wait_recv()

    for c in range(NO):
        for d in (2, 1, 3):
            back(c, d).start()
    cbuf[z] = ctx[z]

    def pass_on(c, k, to):
        return remote(snd.at[c, k], rcv.at[c, k], s_ss, s_rs.at[c, k], seq, to)

    def half(c, k, to):
        return remote(snh.at[c, k], rch.at[c, k], h_ss, h_rs.at[c, k], seq, to)

    to_right, to_left, far = ((x + 1) % 4) * 2, ((x + 3) % 4) * 2, ((x + 2) % 4) * 2

    def project(c, carry):
        back_in(c)
        lhs = jnp.concatenate([cbuf[h, c] for h in range(4)], axis=1)

        def term(b):
            cols = pl.ds(pl.multiple_of(b * W, W), W)
            return jnp.dot(lhs, wbuf[:, cols], preferred_element_type=F32)

        snd[c, 0] = term(far + 1 - y).astype(BF)
        snd[c, 1] = term(to_right + 1 - y).astype(BF)
        pass_on(c, 0, other_y).start()
        snd[c, 2] = term(to_left + 1 - y).astype(BF)
        pass_on(c, 1, right).start()
        own[c, 0] = term(far + y)
        pass_on(c, 2, left).start()
        own[c, 1] = term(to_right + y)
        own[c, 2] = term(to_left + y)
        own[c, 3] = term(other_y)
        own[c, 4] = term(tp)
        return carry

    lax.fori_loop(0, NO, project, 0)

    def second(c, carry):
        pass_on(c, 0, other_y).wait_recv()
        far_sum = (own[c, 0] + rcv[c, 0].astype(F32)).astype(BF)
        snh[c, 0] = far_sum[0 : RO // 2]
        snh[c, 1] = far_sum[RO // 2 :]
        half(c, 0, right).start()
        half(c, 1, left).start()
        return carry

    lax.fori_loop(0, NO, second, 0)

    def third(c, carry):
        pass_on(c, 1, right).wait_recv()
        pass_on(c, 2, left).wait_recv()
        snd[c, 5] = (own[c, 3] + (rcv[c, 1].astype(F32) + rcv[c, 2].astype(F32))).astype(BF)
        pass_on(c, 5, other_y).start()
        half(c, 0, right).wait_recv()
        snd[c, 3, 0 : RO // 2] = (own[c, 1, 0 : RO // 2] + rch[c, 0].astype(F32)).astype(BF)
        snd[c, 3, RO // 2 :] = own[c, 1, RO // 2 :].astype(BF)
        pass_on(c, 3, right).start()
        half(c, 1, left).wait_recv()
        snd[c, 4, 0 : RO // 2] = own[c, 2, 0 : RO // 2].astype(BF)
        snd[c, 4, RO // 2 :] = (own[c, 2, RO // 2 :] + rch[c, 1].astype(F32)).astype(BF)
        pass_on(c, 4, left).start()
        return carry

    lax.fori_loop(0, NO, third, 0)

    def fourth(c, carry):
        rows = pl.ds(pl.multiple_of(c * RO, RO), RO)
        xv = jnp.swapaxes(xraw[rows], 0, 1)
        wide = [xv[j].astype(F32) for j in range(S)]
        for i in range(S):
            k = 8 + 4 * i
            v = cols[rows, k : k + 1] * wide[0]
            for j in range(1, S):
                v = v + cols[rows, k + j : k + j + 1] * wide[j]
            kept[i] = v
        pass_on(c, 5, other_y).wait_recv()
        mine = own[c, 4] + rcv[c, 5].astype(F32)
        pass_on(c, 3, right).wait_recv()
        pass_on(c, 4, left).wait_recv()
        branch = mine + (rcv[c, 3].astype(F32) + rcv[c, 4].astype(F32))
        new = [(kept[i] + cols[rows, 4 + i : 5 + i] * branch).astype(BF) for i in range(S)]
        out[rows] = jnp.swapaxes(jnp.stack(new, axis=0), 0, 1)
        return carry

    lax.fori_loop(0, NO, fourth, 0)

    everything = ctx.at[pl.ds(0, 3)]
    remote(everything, everything, z_ss, z_rs.at[0], seq, right).wait_send()
    remote(snd, snd, s_ss, s_rs.at[0, 0], seq, right).wait_send()
    remote(snh, snh, h_ss, h_rs.at[0, 0], seq, right).wait_send()


def store_kernel(x, out, sem):
    copies = [
        pltpu.make_async_copy(x.at[pl.ds(q * 128, 128)], out.at[pl.ds(q * 128, 128)], sem.at[q])
        for q in range(4)
    ]
    for copy in copies:
        copy.start()
    for copy in copies:
        copy.wait()


def local(streams, doc_ids, mix_weight, mix_bias, attn_gain, w_qkv, w_out):
    wmix = jnp.transpose(mix_weight, (0, 2, 1))
    wq = jnp.transpose(w_qkv, (1, 0, 2))
    vm = pl.BlockSpec(memory_space=VMEM)
    hbm = pl.BlockSpec(memory_space=pl.ANY)
    sds = jax.ShapeDtypeStruct
    att, mix_cols, counts = pl.pallas_call(
        first_kernel,
        name="gather_project",
        out_shape=(
            sds((BLOCKS, NC, 3, R, HD), BF),
            sds((T, 128), F32),
            sds((TILES, 8, 128), jnp.int32),
        ),
        in_specs=[hbm] * 6,
        out_specs=(hbm, vm, hbm),
        scratch_shapes=[
            VMEM((T, S, W), BF),
            VMEM((S, T, W), BF),
            VMEM((4, 128), jnp.int32),
            VMEM((S, 24, W), F32),
            VMEM((1, 24), F32),
            VMEM((1, D), F32),
            VMEM((3, D, W), BF),
            VMEM((NC, 8, R, W), BF),
            VMEM((4, NC, 3, R, HD), BF),
            VMEM((2 * R, D), BF),
            VMEM((2 * R, 128), F32),
            VMEM((8, T), F32),
            VMEM((7, 8, T), F32),
            VMEM((2, 24, T), F32),
            VMEM((4, 24, T), F32),
            VMEM((4, 8, 128), jnp.int32),
            VMEM((5, 8, 128), jnp.int32),
            VMEM((T, 128), F32),
            DMA((4,)),
            DMA((4,)),
            DMA(()),
            DMA(()), DMA(()),
            DMA((2,)), DMA((2,)),
            DMA(()), DMA((3,)),
            DMA(()), DMA((NC, 4)),
            DMA(()), DMA((NC,)),
            DMA(()),
            DMA(()),
            DMA(()),
            DMA(()), DMA(()),
            DMA(()), DMA((NC,)),
            DMA(()), DMA(()),
        ],
        compiler_params=pltpu.CompilerParams(
            collective_id=0, has_side_effects=True, vmem_limit_bytes=60 * 1024 * 1024
        ),
    )(
        streams, doc_ids.reshape(4, 128), wmix, mix_bias.reshape(1, 24), attn_gain.reshape(1, D), wq,
    )
    ctx = pl.pallas_call(
        attention_kernel,
        name="attention",
        out_shape=sds((4, NO, RO, HD), BF),
        in_specs=[hbm, hbm],
        out_specs=vm,
        scratch_shapes=[
            VMEM((16, NC, 3, R, HD), BF),
            pltpu.SMEM((8, 128), jnp.int32),
            VMEM((16, NC, R, 2 * HD), BF),
            VMEM((T, 128), F32), VMEM((T, 2 * HD), F32),
            DMA(()), DMA((16,)), DMA((16,)), DMA((4,)),
        ],
        compiler_params=pltpu.CompilerParams(vmem_limit_bytes=30 * 1024 * 1024),
    )(att, counts)
    new = pl.pallas_call(
        last_kernel,
        name="project_out",
        out_shape=sds((T, S, W), BF),
        in_specs=[vm] * 4,
        out_specs=vm,
        scratch_shapes=[
            VMEM((4, NO, RO, HD), BF),
            VMEM((NO, 6, RO, W), BF),
            VMEM((NO, 2, RO // 2, W), BF),
            VMEM((NO, 5, RO, W), F32),
            VMEM((NO, 6, RO, W), BF),
            VMEM((NO, 2, RO // 2, W), BF),
            VMEM((S, RO, W), F32),
            DMA(()), DMA((NO,)),
            DMA(()), DMA((NO, 6)),
            DMA(()), DMA((NO, 2)),
        ],
        compiler_params=pltpu.CompilerParams(
            collective_id=1, has_side_effects=True, vmem_limit_bytes=30 * 1024 * 1024
        ),
    )(ctx, w_out, streams, mix_cols)
    return pl.pallas_call(
        store_kernel,
        name="store",
        out_shape=sds((T, S, W), BF),
        in_specs=[vm],
        out_specs=hbm,
        scratch_shapes=[DMA((4,))],
        compiler_params=pltpu.CompilerParams(vmem_limit_bytes=8 * 1024 * 1024),
    )(new)


def solution(mesh):
    in_specs = (
        P("seq", None, "tp"),
        P("seq"),
        P(None, "tp", None),
        P(),
        P(),
        P(None, None, "tp"),
        P("tp", None),
    )
    return jax.shard_map(
        local, mesh=mesh, in_specs=in_specs, out_specs=P("seq", None, "tp"), check_vma=False
    )
```

```python
import jax
import jax.numpy as jnp
from jax import lax
from jax.experimental import pallas as pl
from jax.experimental.pallas import tpu as pltpu
from jax.sharding import PartitionSpec as P

D = 4096
HD = 128
S = 4
ROUNDS = 20
EPS = 1e-6
T = 512
W = 512
NC = 8
NO = 4
RO = T // NO
BLOCKS = 160
TILES = 9216
HALF = 256
AHEAD = 3
HANDED = 1
R = T // NC
F32 = jnp.float32
BF = jnp.bfloat16
MESH = pl.DeviceIdType.MESH
NT = (((1,), (1,)), ((), ()))
NEG = -1e30
VMEM = pltpu.VMEM
DMA = pltpu.SemaphoreType.DMA


def where_am_i():
    seq = lax.axis_index("seq")
    tp = lax.axis_index("tp")
    return seq, tp


def remote(src, dst, ssem, rsem, seq, tp):
    return pltpu.make_async_remote_copy(
        src_ref=src, dst_ref=dst, send_sem=ssem, recv_sem=rsem,
        device_id={"seq": seq, "tp": tp}, device_id_type=MESH,
    )


def greet(peers):
    barrier = pltpu.get_barrier_semaphore()
    for seq, tp in peers:
        pl.semaphore_signal(barrier, inc=1, device_id={"seq": seq, "tp": tp}, device_id_type=MESH)
    return lambda: pl.semaphore_wait(barrier, len(peers))


def columns(rows8):
    k = rows8.shape[0]
    if k < 128:
        rows8 = jnp.concatenate([rows8, jnp.zeros((128 - k, rows8.shape[1]), F32)], axis=0)
    return rows8.T


def balanced(e0, e1):
    sub = lax.broadcasted_iota(jnp.int32, e0.shape, 0)
    even, low = sub % 2 == 0, sub % 4 < 2

    def row_total(e):
        u = e + jnp.where(even, pltpu.roll(e, 7, 0), pltpu.roll(e, 1, 0))
        return u + jnp.where(low, pltpu.roll(u, 6, 0), pltpu.roll(u, 2, 0))

    def one_round(_, pair):
        e0, e1 = pair
        e0 = e0 / row_total(e0)
        e1 = e1 / row_total(e1)
        t = e0 + e1
        t = t + pltpu.roll(t, 4, 0)
        return e0 / t, e1 / t

    return lax.fori_loop(0, ROUNDS, one_round, (e0, e1))


def first_kernel(
    x_hbm, docs_hbm, wmix_hbm, bias_hbm, gain_hbm, w_hbm,
    att, mix_cols, counts,
    xraw, xs, docs, wmix, bias, gain,
    wbuf, g, sb, gained, norms, unow, urecv, nall, nrecv, csend, crecv, pre_cols, cols,
    x_sem, i_sem, w_sem, u_ss, u_rs, n_ss, n_rs, c_ss, c_rs, g_ss, g_rs, a_ss, a_rs, q_rs, o_sem, t_sem, m_sem,
    sib_ss, sib_rs, x_ss, x_rs, sib2_ss, sib2_rs,
):
    seq, tp = where_am_i()
    yhi, z, core = seq // 8, (seq // 2) % 4, seq % 2
    x, y = tp // 2, tp % 2
    sibling, mirror = seq + 1 - 2 * core, (seq + 8) % 16
    far_first = ((2, 1), (2, 0), (1, 1), (3, 1), (1, 0), (3, 0), (0, 1))
    tp_peers = [(seq, ((x + dx) % 4) * 2 + (y + dy) % 2) for dx, dy in far_first]
    z_peers = [yhi * 8 + ((z + d) % 4) * 2 + core for d in range(1, 4)]
    entered = greet(tp_peers + [(p, tp) for p in z_peers] + [(sibling, tp), (mirror, tp)])

    small = [
        pltpu.make_async_copy(a, b, i_sem.at[i])
        for i, (a, b) in enumerate(
            ((wmix_hbm, wmix), (docs_hbm, docs), (bias_hbm, bias), (gain_hbm, gain))
        )
    ]
    parts_of_x = [
        pltpu.make_async_copy(x_hbm.at[pl.ds(q * 128, 128)], xraw.at[pl.ds(q * 128, 128)], x_sem.at[q])
        for q in range(4)
    ]
    small[0].start()
    for q in range(4):
        parts_of_x[q].start()
    for k in range(1, 4):
        small[k].start()

    def wcopy(i):
        return pltpu.make_async_copy(w_hbm.at[i], wbuf.at[i], w_sem)

    small[0].wait()
    parts = []
    for s in range(S):
        w = jnp.concatenate([wmix[s], jnp.zeros((8, W), F32)], axis=0)
        hi = w.astype(BF).astype(F32)
        mid = (w - hi).astype(BF).astype(F32)
        low = (w - hi) - mid
        parts.append(jnp.concatenate([hi, mid, low], axis=0).astype(BF))
    sub = lax.broadcasted_iota(jnp.int32, (8, 128), 0)
    for q in range(4):
        rows = slice(q * 128, (q + 1) * 128)
        parts_of_x[q].wait()
        if q == 3:
            for i in range(3):
                wcopy(i).start()
        xs[:, rows, :] = jnp.swapaxes(xraw[rows], 0, 1)
        acc = jnp.zeros((128, 128), F32)
        logits = jnp.zeros((32, 128), F32)
        for s in range(S):
            xv = xs[s, rows, :]
            got = lax.dot_general(parts[s], xv, NT, preferred_element_type=F32)
            logits = logits + (got[0:32] + (got[32:64] + got[64:96]))
            x32 = xv.astype(F32)
            sq = x32 * x32
            acc = acc + ((sq[:, 0:128] + sq[:, 128:256]) + (sq[:, 256:384] + sq[:, 384:512]))
        squares = jnp.sum(acc.T, axis=0, keepdims=True)
        unow[:, rows] = jnp.where(
            sub < 4, logits[0:8], jnp.where(sub == 4, jnp.broadcast_to(squares, (8, 128)), 0.0)
        )
        nall[0, :, rows] = logits[0:24]

    entered()
    for r, (sq_, tp_) in enumerate(tp_peers):
        remote(unow, urecv.at[r], u_ss, u_rs, sq_, tp_).start()

    def to_y():
        return remote(nall.at[0], nrecv.at[0], n_ss.at[0], n_rs.at[0], seq, x * 2 + 1 - y)

    def to_x(k):
        return remote(nall.at[1], nrecv.at[k], n_ss.at[1], n_rs.at[1], seq, ((x + k) % 4) * 2 + y)

    to_y().start()
    for k in range(1, 4):
        small[k].wait()
    dv = docs[...]
    cv = jnp.zeros((8, 128), jnp.int32)
    for k in range(1, 4):
        n = jnp.sum(jnp.where(dv < k, 1, 0), axis=1, keepdims=True)
        n = jnp.sum(n, axis=0, keepdims=True)
        cv = jnp.where(sub == k, jnp.broadcast_to(n, (8, 128)), cv)
    csend[0] = cv
    diag = lax.broadcasted_iota(jnp.int32, (24, 24), 0) == lax.broadcasted_iota(jnp.int32, (24, 24), 1)
    bias_col = jnp.sum(jnp.where(diag, jnp.broadcast_to(bias[...], (24, 24)), 0.0), axis=1, keepdims=True)

    def count_to(level, k, to):
        return remote(csend.at[level], crecv.at[k], c_ss, c_rs.at[level], to, tp)

    total = unow[...]
    remote(urecv, urecv, u_ss, u_rs, seq, tp_peers[0][1]).wait_recv()
    for r in range(7):
        total = total + urecv[r]
    inv_rms = lax.rsqrt(total[4:5] / (S * D) + EPS)
    pre = 1.0 / (1.0 + jnp.exp(-(total * inv_rms + bias_col[0:8])))
    pre_cols[...] = columns(pre)

    right = ((x + 1) % 4) * 2 + y
    left = ((x + 3) % 4) * 2 + y
    other_y = x * 2 + 1 - y
    b_p = other_y
    b_l0 = left
    b_r1 = ((x + 1) % 4) * 2 + 1 - y

    def move(c, blk, role, to):
        return remote(g.at[c, blk], g.at[c, blk], g_ss, g_rs.at[c, role], seq, to)

    def arrived(c, role, n):
        some = g.at[c, pl.ds(0, n)]
        remote(some, some, g_ss, g_rs.at[c, role], seq, right).wait_recv()

    def make_chunk(c):
        rows = slice(c * R, (c + 1) * R)
        v = pre_cols[rows, 0:1] * xs[0, rows, :].astype(F32)
        for s in range(1, S):
            v = v + pre_cols[rows, s : s + 1] * xs[s, rows, :].astype(F32)
        g[c, tp] = v.astype(BF)

    def send_chunk(c):
        move(c, tp, 0, other_y).start()
        move(c, tp, 1, right).start()
        move(c, tp, 3, left).start()

    make_chunk(0)
    for c in range(NC):
        if c + 1 < NC:
            make_chunk(c + 1)
        if c < AHEAD:
            send_chunk(c)
    for d in range(3):
        count_to(0, d, z_peers[d]).start()
    pltpu.make_async_copy(w_hbm, wbuf, w_sem).wait()

    def block_of(half, d):
        return half * 8 + ((z + 4 - d) % 4) * 2 + core

    two = pl.ds(0, 2)

    def spread(c, d):
        return remote(
            sb.at[(z + d) % 4, c, two], att.at[seq, c, two],
            a_ss, a_rs.at[c], z_peers[d - 1], tp,
        )

    def spread_in(c):
        ref = sb.at[pl.ds(0, 3), c, two]
        remote(ref, ref, a_ss, a_rs.at[c], z_peers[0], tp).wait_recv()

    def spread_q(c, d):
        return remote(
            sb.at[(z + d) % 4, c, 2], att.at[seq, c, 2],
            a_ss, q_rs, z_peers[d - 1], tp,
        )

    def kept():
        return pltpu.make_async_copy(sb.at[z], att.at[seq], o_sem)

    def kv(c, d):
        return sb.at[z, c, pl.ds(0, 2)] if d == 0 else att.at[block_of(yhi, d), c, pl.ds(0, 2)]

    def twin(c, d):
        dst = att.at[block_of(yhi, d), c, pl.ds(0, 2)]
        return remote(kv(c, d), dst, sib_ss, sib_rs, sibling, tp)

    def cross(c, d):
        dst = att.at[block_of(0, d), c, pl.ds(0, 2)]
        return remote(kv(c, d), dst, x_ss, x_rs.at[c], mirror, tp)

    def twin2(c, d):
        ref = att.at[block_of(0, d), c, pl.ds(0, 2)]
        return remote(ref, ref, sib2_ss, sib2_rs, sibling, tp)

    def hand_on(i):
        arrived(i, 0, 1)
        move(i, b_p, 3, right).start()
        move(i, b_p, 2, left).start()

    for c in range(HANDED):
        hand_on(c)

    def feed(i):
        @pl.when(i + AHEAD < NC)
        def _():
            send_chunk(i + AHEAD)

        @pl.when(i + HANDED < NC)
        def _():
            hand_on(i + HANDED)

        @pl.when(i < NC)
        def _():
            arrived(i, 1, 1)
            move(i, b_l0, 3, right).start()
            arrived(i, 2, 1)
            move(i, b_r1, 3, left).start()

    def projected(c0):
        for e in range(2):
            c = c0 + e
            rows = slice(e * R, (e + 1) * R)
            arrived(c, 3, 4)
            ss = jnp.zeros((R, 128), F32)
            for b in range(8):
                g32 = g[c, b].astype(F32)
                q = g32 * g32
                ss = ss + ((q[:, 0:128] + q[:, 128:256]) + (q[:, 256:384] + q[:, 384:512]))
                gained[rows, b * W : (b + 1) * W] = (g32 * gain[:, b * W : (b + 1) * W]).astype(BF)
            norms[rows, :] = jnp.broadcast_to(
                lax.rsqrt(jnp.sum(ss, axis=1, keepdims=True) / D + EPS), (R, 128)
            )
        norm = norms[:, 0:1]
        lhs = gained[...]

        def project(slot, third):
            out = (jnp.dot(lhs, wbuf[third], preferred_element_type=F32) * norm).astype(BF)
            for h in range(4):
                for e in range(2):
                    sb[h, c0 + e, slot] = out[e * R : (e + 1) * R, h * HD : (h + 1) * HD]

        project(0, 1)
        project(1, 2)
        for e in range(2):
            for d in (2, 1, 3):
                spread(c0 + e, d).start()

        @pl.when(yhi == 0)
        def _():
            for e in range(2):
                cross(c0 + e, 0).start()

        for e in range(2):
            twin(c0 + e, 0).start()
        project(2, 0)
        for e in range(2):
            for d in (2, 1, 3):
                spread_q(c0 + e, d).start()

    def share(c):
        spread_in(c)
        for d in range(1, 4):

            @pl.when(yhi == 0)
            def _():
                cross(c, d).start()

            twin(c, d).start()

    def share_far(c):
        ref = sb.at[:, c, two]
        remote(ref, ref, x_ss, x_rs.at[c], mirror, tp).wait_recv()
        for d in range(4):
            twin2(c, d).start()

    def step(i, carry):
        @pl.when(i == 1)
        def _():
            count_to(1, 3, sibling).start()

        @pl.when(i == 2)
        def _():
            count_to(2, 4, mirror).start()

        feed(2 * i)

        @pl.when(i >= 1)
        def _():
            projected(2 * i - 2)

        feed(2 * i + 1)

        @pl.when(i == 0)
        def _():
            to_y().wait_recv()
            nall[1] = nall[0] + nrecv[0]
            v = csend[0]
            remote(crecv.at[pl.ds(0, 3)], crecv.at[pl.ds(0, 3)], c_ss, c_rs.at[0], sibling, tp).wait_recv()
            for d in range(3):
                v = v + crecv[d]
            csend[1] = v

        @pl.when(i == 1)
        def _():
            count_to(1, 3, sibling).wait_recv()
            csend[2] = csend[1] + crecv[3]

        @pl.when(i >= 1)
        def _():
            share(2 * i - 2)
            share(2 * i - 1)

        @pl.when((i >= 2) & (yhi == 1))
        def _():
            share_far(2 * i - 4)
            share_far(2 * i - 3)

        @pl.when(i == NC // 2 - 1)
        def _():
            for k in (2, 1, 3):
                to_x(k).start()

        return carry

    lax.fori_loop(0, NC // 2 + 1, step, 0)
    kept().start()

    count_to(2, 4, mirror).wait_recv()
    csend[3] = csend[2] + crecv[4]
    told = pltpu.make_async_copy(csend.at[3], counts.at[0], t_sem)
    told.start()
    three = nrecv.at[pl.ds(1, 3)]
    remote(three, three, n_ss.at[1], n_rs.at[1], seq, right).wait_recv()
    ztot = (nall[1] + nrecv[1]) + (nrecv[2] + nrecv[3])
    ztot = ztot * inv_rms + bias_col
    post = 2.0 / (1.0 + jnp.exp(-ztot[0:8]))
    e0, e1 = balanced(jnp.exp(ztot[8:16]), jnp.exp(ztot[16:24]))
    cols[...] = columns(jnp.concatenate([post, e0, e1], axis=0))
    noted = pltpu.make_async_copy(cols, mix_cols, m_sem)
    noted.start()

    @pl.when(yhi == 1)
    def _():
        share_far(NC - 2)
        share_far(NC - 1)

    told.wait()
    noted.wait()
    kept().wait()

    def all_of(ref, ssem, rsem):
        return remote(ref, ref, ssem, rsem, sibling, tp)

    all_of(urecv, u_ss, u_rs).wait_send()
    all_of(nall.at[0], n_ss.at[0], n_rs.at[0]).wait_send()
    all_of(three, n_ss.at[1], n_rs.at[1]).wait_send()
    all_of(crecv, c_ss, c_rs.at[0]).wait_send()
    all_of(g.at[pl.ds(0, 7)], g_ss, g_rs.at[0, 0]).wait_send()
    all_of(sb.at[pl.ds(0, 3)], a_ss, a_rs.at[0]).wait_send()
    all_of(sb.at[pl.ds(0, 3), :, 2], a_ss, q_rs).wait_recv()
    twins = all_of(sb.at[:, :, two], sib_ss, sib_rs)
    twins.wait_send()
    twins.wait_recv()

    @pl.when(yhi == 0)
    def _():
        all_of(sb.at[:, :, two], x_ss, x_rs.at[0]).wait_send()

    @pl.when(yhi == 1)
    def _():
        far = all_of(sb.at[:, :, two], sib2_ss, sib2_rs)
        far.wait_send()
        far.wait_recv()


def attention_kernel(att_hbm, cnt_hbm, ctx, att, cnt, vx, m_ref, acc_ref, c_sem, k_sem, v_sem, q_sem):
    seq = lax.axis_index("seq")
    yhi, core = seq // 8, seq % 2
    counts_in = pltpu.make_async_copy(cnt_hbm.at[0], cnt, c_sem)
    counts_in.start()

    def q_in(qi):
        qb = yhi * 8 + qi * 2 + core
        return pltpu.make_async_copy(att_hbm.at[qb, :, 2], att.at[qb, :, 2], q_sem.at[qi])

    def k_in(kb):
        return pltpu.make_async_copy(att_hbm.at[kb, :, 0], att.at[kb, :, 0], k_sem.at[kb])

    def v_in(kb):
        return pltpu.make_async_copy(att_hbm.at[kb, :, 1], vx.at[kb, :, :, pl.ds(0, HD)], v_sem.at[kb])

    q_in(0).start()
    k_in(yhi * 8 + core).start()
    v_in(yhi * 8 + core).start()
    counts_in.wait()
    starts = [cnt[k, 0] for k in range(1, 4)]
    scale = HD ** (-0.5) * 1.4426950408889634

    def start_of(p):
        v = p * 0
        for c in starts:
            v = jnp.where(c <= p, jnp.maximum(v, c), v)
        return v

    first_needed = start_of((yhi * 8 + core) * T) // T

    def fetch(kb, c):
        k_in(kb).start()
        v_in(kb).start()
        return c

    def land(kb, c):
        k_in(kb).wait()
        v_in(kb).wait()
        return c

    lax.fori_loop(first_needed, yhi * 8 + core, fetch, 0)
    for qi in range(1, 4):
        q_in(qi).start()
    lax.fori_loop(yhi * 8 + core + 1, yhi * 8 + core + 7, fetch, 0)

    def ones(kb, c):
        vx[kb, :, :, HD:] = jnp.ones((NC, R, HD), BF)
        return c

    lax.fori_loop(first_needed, yhi * 8 + core + 7, ones, 0)

    def one_query_block(qi, carry):
        qb = yhi * 8 + qi * 2 + core
        q_in(qi).wait()
        land(qb, 0)
        q = att[qb, :, 2].reshape(T, HD)
        first = start_of(qb * T)
        last = start_of(qb * T + T - 1)
        lo = first // T
        mid = jnp.minimum((last + T - 1) // T, qb)
        qpos = qb * T + lax.broadcasted_iota(jnp.int32, (T, 1), 0)
        qstart = start_of(qpos)
        def block(kb, mode, n=1):
            k = att[pl.ds(kb, n), :, 0].reshape(n * T, HD)
            v = vx[pl.ds(kb, n)].reshape(n * T, 2 * HD)

            def scores(t):
                rows = slice(t * HALF, (t + 1) * HALF)
                s = lax.dot_general(q[rows], k, NT, preferred_element_type=F32)
                if mode != "all":
                    kpos = kb * T + lax.broadcasted_iota(jnp.int32, (1, T), 1)
                    ok = kpos >= qstart[rows]
                    if mode == "diagonal":
                        ok = ok & (kpos <= qpos[rows])
                    s = jnp.where(ok, s, NEG)
                return s

            later = scores(0)
            for t in range(T // HALF):
                rows = slice(t * HALF, (t + 1) * HALF)
                s = later
                if (t + 1) * HALF < T:
                    later = scores(t + 1)
                top = s[:, 0:128]
                for e in range(1, n * 4):
                    top = jnp.maximum(top, s[:, e * 128 : (e + 1) * 128])
                m_new = jnp.max(top, axis=1, keepdims=True)
                if mode != "diagonal":
                    m_old = m_ref[rows, 0:1]
                    m_new = jnp.maximum(m_old, m_new)
                    alpha = jnp.exp2((m_old - m_new) * scale)
                p = jnp.exp2((s - m_new) * scale).astype(BF)
                more = jnp.dot(p, v, preferred_element_type=F32)
                acc_ref[rows] = more if mode == "diagonal" else acc_ref[rows] * alpha + more
                m_ref[rows] = jnp.broadcast_to(m_new, (HALF, 128))

        def some(kb, c):
            block(kb, "start")
            return c

        def two(k, c):
            block(mid + 4 * k, "all", 4)
            return c

        def one(kb, c):
            block(kb, "all")
            return c

        block(qb, "diagonal")
        lax.fori_loop(jnp.where(qi == 0, first_needed, qb - 1), qb, land, 0)
        lax.fori_loop(lo, mid, some, 0)
        pairs = (qb - mid) // 4
        lax.fori_loop(0, pairs, two, 0)
        lax.fori_loop(mid + 4 * pairs, qb, one, 0)
        out = acc_ref[:, 0:HD] / acc_ref[:, HD : HD + 1]
        ctx[qi] = out.astype(BF).reshape(NO, RO, HD)
        return carry

    lax.fori_loop(0, 4, one_query_block, 0)


def last_kernel(
    ctx, wbuf, xraw, cols,
    out,
    cbuf, snd, snh, own, rcv, rch, kept,
    z_ss, z_rs, s_ss, s_rs, h_ss, h_rs,
):
    seq, tp = where_am_i()
    yhi, z, core = seq // 8, (seq // 2) % 4, seq % 2
    x, y = tp // 2, tp % 2
    right = ((x + 1) % 4) * 2 + y
    left = ((x + 3) % 4) * 2 + y
    other_y = x * 2 + 1 - y
    z_peers = [yhi * 8 + ((z + d) % 4) * 2 + core for d in range(1, 4)]
    entered = greet([(p, tp) for p in z_peers] + [(seq, right), (seq, left), (seq, other_y)])
    entered()

    def back(c, d):
        return remote(
            ctx.at[(z + d) % 4, c], cbuf.at[z, c], z_ss, z_rs.at[c], z_peers[d - 1], tp
        )

    def back_in(c):
        ref = ctx.at[pl.ds(0, 3), c]
        remote(ref, ref, z_ss, z_rs.at[c], z_peers[0], tp).wait_recv()

    for c in range(NO):
        for d in (2, 1, 3):
            back(c, d).start()
    cbuf[z] = ctx[z]

    def pass_on(c, k, to):
        return remote(snd.at[c, k], rcv.at[c, k], s_ss, s_rs.at[c, k], seq, to)

    def half(c, k, to):
        return remote(snh.at[c, k], rch.at[c, k], h_ss, h_rs.at[c, k], seq, to)

    to_right, to_left, far = ((x + 1) % 4) * 2, ((x + 3) % 4) * 2, ((x + 2) % 4) * 2

    def project(c, carry):
        back_in(c)
        lhs = jnp.concatenate([cbuf[h, c] for h in range(4)], axis=1)

        def term(b):
            cols = pl.ds(pl.multiple_of(b * W, W), W)
            return jnp.dot(lhs, wbuf[:, cols], preferred_element_type=F32)

        snd[c, 0] = term(far + 1 - y).astype(BF)
        snd[c, 1] = term(to_right + 1 - y).astype(BF)
        pass_on(c, 0, other_y).start()
        snd[c, 2] = term(to_left + 1 - y).astype(BF)
        pass_on(c, 1, right).start()
        own[c, 0] = term(far + y)
        pass_on(c, 2, left).start()
        own[c, 1] = term(to_right + y)
        own[c, 2] = term(to_left + y)
        own[c, 3] = term(other_y)
        own[c, 4] = term(tp)
        return carry

    lax.fori_loop(0, NO, project, 0)

    def second(c, carry):
        pass_on(c, 0, other_y).wait_recv()
        far_sum = (own[c, 0] + rcv[c, 0].astype(F32)).astype(BF)
        snh[c, 0] = far_sum[0 : RO // 2]
        snh[c, 1] = far_sum[RO // 2 :]
        half(c, 0, right).start()
        half(c, 1, left).start()
        return carry

    lax.fori_loop(0, NO, second, 0)

    def third(c, carry):
        pass_on(c, 1, right).wait_recv()
        pass_on(c, 2, left).wait_recv()
        snd[c, 5] = (own[c, 3] + (rcv[c, 1].astype(F32) + rcv[c, 2].astype(F32))).astype(BF)
        pass_on(c, 5, other_y).start()
        half(c, 0, right).wait_recv()
        snd[c, 3, 0 : RO // 2] = (own[c, 1, 0 : RO // 2] + rch[c, 0].astype(F32)).astype(BF)
        snd[c, 3, RO // 2 :] = own[c, 1, RO // 2 :].astype(BF)
        pass_on(c, 3, right).start()
        half(c, 1, left).wait_recv()
        snd[c, 4, 0 : RO // 2] = own[c, 2, 0 : RO // 2].astype(BF)
        snd[c, 4, RO // 2 :] = (own[c, 2, RO // 2 :] + rch[c, 1].astype(F32)).astype(BF)
        pass_on(c, 4, left).start()
        return carry

    lax.fori_loop(0, NO, third, 0)

    def fourth(c, carry):
        rows = pl.ds(pl.multiple_of(c * RO, RO), RO)
        xv = jnp.swapaxes(xraw[rows], 0, 1)
        wide = [xv[j].astype(F32) for j in range(S)]
        for i in range(S):
            k = 8 + 4 * i
            v = cols[rows, k : k + 1] * wide[0]
            for j in range(1, S):
                v = v + cols[rows, k + j : k + j + 1] * wide[j]
            kept[i] = v
        pass_on(c, 5, other_y).wait_recv()
        mine = own[c, 4] + rcv[c, 5].astype(F32)
        pass_on(c, 3, right).wait_recv()
        pass_on(c, 4, left).wait_recv()
        branch = mine + (rcv[c, 3].astype(F32) + rcv[c, 4].astype(F32))
        new = [(kept[i] + cols[rows, 4 + i : 5 + i] * branch).astype(BF) for i in range(S)]
        out[rows] = jnp.swapaxes(jnp.stack(new, axis=0), 0, 1)
        return carry

    lax.fori_loop(0, NO, fourth, 0)

    everything = ctx.at[pl.ds(0, 3)]
    remote(everything, everything, z_ss, z_rs.at[0], seq, right).wait_send()
    remote(snd, snd, s_ss, s_rs.at[0, 0], seq, right).wait_send()
    remote(snh, snh, h_ss, h_rs.at[0, 0], seq, right).wait_send()


def store_kernel(x, out, sem):
    copies = [
        pltpu.make_async_copy(x.at[pl.ds(q * 128, 128)], out.at[pl.ds(q * 128, 128)], sem.at[q])
        for q in range(4)
    ]
    for copy in copies:
        copy.start()
    for copy in copies:
        copy.wait()


def local(streams, doc_ids, mix_weight, mix_bias, attn_gain, w_qkv, w_out):
    wmix = jnp.transpose(mix_weight, (0, 2, 1))
    wq = jnp.transpose(w_qkv, (1, 0, 2))
    vm = pl.BlockSpec(memory_space=VMEM)
    hbm = pl.BlockSpec(memory_space=pl.ANY)
    sds = jax.ShapeDtypeStruct
    att, mix_cols, counts = pl.pallas_call(
        first_kernel,
        name="gather_project",
        out_shape=(
            sds((BLOCKS, NC, 3, R, HD), BF),
            sds((T, 128), F32),
            sds((TILES, 8, 128), jnp.int32),
        ),
        in_specs=[hbm] * 6,
        out_specs=(hbm, hbm, hbm),
        scratch_shapes=[
            VMEM((T, S, W), BF),
            VMEM((S, T, W), BF),
            VMEM((4, 128), jnp.int32),
            VMEM((S, 24, W), F32),
            VMEM((1, 24), F32),
            VMEM((1, D), F32),
            VMEM((3, D, W), BF),
            VMEM((NC, 8, R, W), BF),
            VMEM((4, NC, 3, R, HD), BF),
            VMEM((2 * R, D), BF),
            VMEM((2 * R, 128), F32),
            VMEM((8, T), F32),
            VMEM((7, 8, T), F32),
            VMEM((2, 24, T), F32),
            VMEM((4, 24, T), F32),
            VMEM((4, 8, 128), jnp.int32),
            VMEM((5, 8, 128), jnp.int32),
            VMEM((T, 128), F32),
            VMEM((T, 128), F32),
            DMA((4,)),
            DMA((4,)),
            DMA(()),
            DMA(()), DMA(()),
            DMA((2,)), DMA((2,)),
            DMA(()), DMA((3,)),
            DMA(()), DMA((NC, 4)),
            DMA(()), DMA((NC,)),
            DMA(()),
            DMA(()),
            DMA(()),
            DMA(()),
            DMA(()), DMA(()),
            DMA(()), DMA((NC,)),
            DMA(()), DMA(()),
        ],
        compiler_params=pltpu.CompilerParams(
            collective_id=0, has_side_effects=True, vmem_limit_bytes=60 * 1024 * 1024
        ),
    )(
        streams, doc_ids.reshape(4, 128), wmix, mix_bias.reshape(1, 24), attn_gain.reshape(1, D), wq,
    )
    ctx = pl.pallas_call(
        attention_kernel,
        name="attention",
        out_shape=sds((4, NO, RO, HD), BF),
        in_specs=[hbm, hbm],
        out_specs=vm,
        scratch_shapes=[
            VMEM((16, NC, 3, R, HD), BF),
            pltpu.SMEM((8, 128), jnp.int32),
            VMEM((16, NC, R, 2 * HD), BF),
            VMEM((T, 128), F32), VMEM((T, 2 * HD), F32),
            DMA(()), DMA((16,)), DMA((16,)), DMA((4,)),
        ],
        compiler_params=pltpu.CompilerParams(vmem_limit_bytes=30 * 1024 * 1024),
    )(att, counts)
    new = pl.pallas_call(
        last_kernel,
        name="project_out",
        out_shape=sds((T, S, W), BF),
        in_specs=[vm] * 4,
        out_specs=vm,
        scratch_shapes=[
            VMEM((4, NO, RO, HD), BF),
            VMEM((NO, 6, RO, W), BF),
            VMEM((NO, 2, RO // 2, W), BF),
            VMEM((NO, 5, RO, W), F32),
            VMEM((NO, 6, RO, W), BF),
            VMEM((NO, 2, RO // 2, W), BF),
            VMEM((S, RO, W), F32),
            DMA(()), DMA((NO,)),
            DMA(()), DMA((NO, 6)),
            DMA(()), DMA((NO, 2)),
        ],
        compiler_params=pltpu.CompilerParams(
            collective_id=1, has_side_effects=True, vmem_limit_bytes=30 * 1024 * 1024
        ),
    )(ctx, w_out, streams, mix_cols)
    return pl.pallas_call(
        store_kernel,
        name="store",
        out_shape=sds((T, S, W), BF),
        in_specs=[vm],
        out_specs=hbm,
        scratch_shapes=[DMA((4,))],
        compiler_params=pltpu.CompilerParams(vmem_limit_bytes=8 * 1024 * 1024),
    )(new)


def solution(mesh):
    in_specs = (
        P("seq", None, "tp"),
        P("seq"),
        P(None, "tp", None),
        P(),
        P(),
        P(None, None, "tp"),
        P("tp", None),
    )
    return jax.shard_map(
        local, mesh=mesh, in_specs=in_specs, out_specs=P("seq", None, "tp"), check_vma=False
    )
```

```python
import jax
import jax.numpy as jnp
from jax import lax
from jax.experimental import pallas as pl
from jax.experimental.pallas import tpu as pltpu
from jax.sharding import PartitionSpec as P

D = 4096
HD = 128
S = 4
ROUNDS = 20
EPS = 1e-6
T = 512
W = 512
NC = 8
NO = 4
RO = T // NO
BLOCKS = 160
TILES = 9216
HALF = 256
AHEAD = 3
HANDED = 1
R = T // NC
F32 = jnp.float32
BF = jnp.bfloat16
MESH = pl.DeviceIdType.MESH
NT = (((1,), (1,)), ((), ()))
NEG = -1e30
VMEM = pltpu.VMEM
DMA = pltpu.SemaphoreType.DMA


def where_am_i():
    seq = lax.axis_index("seq")
    tp = lax.axis_index("tp")
    return seq, tp


def remote(src, dst, ssem, rsem, seq, tp):
    return pltpu.make_async_remote_copy(
        src_ref=src, dst_ref=dst, send_sem=ssem, recv_sem=rsem,
        device_id={"seq": seq, "tp": tp}, device_id_type=MESH,
    )


def greet(peers):
    barrier = pltpu.get_barrier_semaphore()
    for seq, tp in peers:
        pl.semaphore_signal(barrier, inc=1, device_id={"seq": seq, "tp": tp}, device_id_type=MESH)
    return lambda: pl.semaphore_wait(barrier, len(peers))


def columns(rows8):
    k = rows8.shape[0]
    if k < 128:
        rows8 = jnp.concatenate([rows8, jnp.zeros((128 - k, rows8.shape[1]), F32)], axis=0)
    return rows8.T


def balanced(e0, e1):
    sub = lax.broadcasted_iota(jnp.int32, e0.shape, 0)
    even, low = sub % 2 == 0, sub % 4 < 2

    def row_total(e):
        u = e + jnp.where(even, pltpu.roll(e, 7, 0), pltpu.roll(e, 1, 0))
        return u + jnp.where(low, pltpu.roll(u, 6, 0), pltpu.roll(u, 2, 0))

    def one_round(_, pair):
        e0, e1 = pair
        e0 = e0 / row_total(e0)
        e1 = e1 / row_total(e1)
        t = e0 + e1
        t = t + pltpu.roll(t, 4, 0)
        return e0 / t, e1 / t

    return lax.fori_loop(0, ROUNDS, one_round, (e0, e1))


def first_kernel(
    x_hbm, docs_hbm, wmix_hbm, bias_hbm, gain_hbm, w_hbm,
    att, mix_cols, counts,
    xraw, xs, docs, wmix, bias, gain,
    wbuf, g, sb, gained, norms, unow, urecv, nall, nrecv, csend, crecv, pre_cols, cols,
    x_sem, i_sem, w_sem, u_ss, u_rs, n_ss, n_rs, c_ss, c_rs, g_ss, g_rs, a_ss, a_rs, q_rs, o_sem, t_sem, m_sem,
    sib_ss, sib_rs, x_ss, x_rs, sib2_ss, sib2_rs,
):
    seq, tp = where_am_i()
    yhi, z, core = seq // 8, (seq // 2) % 4, seq % 2
    x, y = tp // 2, tp % 2
    sibling, mirror = seq + 1 - 2 * core, (seq + 8) % 16
    far_first = ((2, 1), (2, 0), (1, 1), (3, 1), (1, 0), (3, 0), (0, 1))
    tp_peers = [(seq, ((x + dx) % 4) * 2 + (y + dy) % 2) for dx, dy in far_first]
    z_peers = [yhi * 8 + ((z + d) % 4) * 2 + core for d in range(1, 4)]
    entered = greet(tp_peers + [(p, tp) for p in z_peers] + [(sibling, tp), (mirror, tp)])

    small = [
        pltpu.make_async_copy(a, b, i_sem.at[i])
        for i, (a, b) in enumerate(
            ((wmix_hbm, wmix), (docs_hbm, docs), (bias_hbm, bias), (gain_hbm, gain))
        )
    ]
    parts_of_x = [
        pltpu.make_async_copy(x_hbm.at[pl.ds(q * 128, 128)], xraw.at[pl.ds(q * 128, 128)], x_sem.at[q])
        for q in range(4)
    ]
    small[0].start()
    for q in range(4):
        parts_of_x[q].start()
    for k in range(1, 4):
        small[k].start()

    def wcopy(i):
        return pltpu.make_async_copy(w_hbm.at[i], wbuf.at[i], w_sem)

    small[0].wait()
    parts = []
    for s in range(S):
        w = jnp.concatenate([wmix[s], jnp.zeros((8, W), F32)], axis=0)
        hi = w.astype(BF).astype(F32)
        mid = (w - hi).astype(BF).astype(F32)
        low = (w - hi) - mid
        parts.append(jnp.concatenate([hi, mid, low], axis=0).astype(BF))
    sub = lax.broadcasted_iota(jnp.int32, (8, 128), 0)
    for q in range(4):
        rows = slice(q * 128, (q + 1) * 128)
        parts_of_x[q].wait()
        if q == 3:
            for i in range(3):
                wcopy(i).start()
        xs[:, rows, :] = jnp.swapaxes(xraw[rows], 0, 1)
        acc = jnp.zeros((128, 128), F32)
        logits = jnp.zeros((32, 128), F32)
        for s in range(S):
            xv = xs[s, rows, :]
            got = lax.dot_general(parts[s], xv, NT, preferred_element_type=F32)
            logits = logits + (got[0:32] + (got[32:64] + got[64:96]))
            x32 = xv.astype(F32)
            sq = x32 * x32
            acc = acc + ((sq[:, 0:128] + sq[:, 128:256]) + (sq[:, 256:384] + sq[:, 384:512]))
        squares = jnp.sum(acc.T, axis=0, keepdims=True)
        unow[:, rows] = jnp.where(
            sub < 4, logits[0:8], jnp.where(sub == 4, jnp.broadcast_to(squares, (8, 128)), 0.0)
        )
        nall[0, :, rows] = logits[0:24]

    entered()
    for r, (sq_, tp_) in enumerate(tp_peers):
        remote(unow, urecv.at[r], u_ss, u_rs, sq_, tp_).start()

    def to_y():
        return remote(nall.at[0], nrecv.at[0], n_ss.at[0], n_rs.at[0], seq, x * 2 + 1 - y)

    def to_x(k):
        return remote(nall.at[1], nrecv.at[k], n_ss.at[1], n_rs.at[1], seq, ((x + k) % 4) * 2 + y)

    to_y().start()
    for k in range(1, 4):
        small[k].wait()
    dv = docs[...]
    cv = jnp.zeros((8, 128), jnp.int32)
    for k in range(1, 4):
        n = jnp.sum(jnp.where(dv < k, 1, 0), axis=1, keepdims=True)
        n = jnp.sum(n, axis=0, keepdims=True)
        cv = jnp.where(sub == k, jnp.broadcast_to(n, (8, 128)), cv)
    csend[0] = cv
    diag = lax.broadcasted_iota(jnp.int32, (24, 24), 0) == lax.broadcasted_iota(jnp.int32, (24, 24), 1)
    bias_col = jnp.sum(jnp.where(diag, jnp.broadcast_to(bias[...], (24, 24)), 0.0), axis=1, keepdims=True)

    def count_to(level, k, to):
        return remote(csend.at[level], crecv.at[k], c_ss, c_rs.at[level], to, tp)

    total = unow[...]
    remote(urecv, urecv, u_ss, u_rs, seq, tp_peers[0][1]).wait_recv()
    for r in range(7):
        total = total + urecv[r]
    inv_rms = lax.rsqrt(total[4:5] / (S * D) + EPS)
    pre = 1.0 / (1.0 + jnp.exp(-(total * inv_rms + bias_col[0:8])))
    pre_cols[...] = columns(pre)

    right = ((x + 1) % 4) * 2 + y
    left = ((x + 3) % 4) * 2 + y
    other_y = x * 2 + 1 - y
    b_p = other_y
    b_l0 = left
    b_r1 = ((x + 1) % 4) * 2 + 1 - y

    def move(c, blk, role, to):
        return remote(g.at[c, blk], g.at[c, blk], g_ss, g_rs.at[c, role], seq, to)

    def arrived(c, role, n):
        some = g.at[c, pl.ds(0, n)]
        remote(some, some, g_ss, g_rs.at[c, role], seq, right).wait_recv()

    def make_chunk(c):
        rows = slice(c * R, (c + 1) * R)
        v = pre_cols[rows, 0:1] * xs[0, rows, :].astype(F32)
        for s in range(1, S):
            v = v + pre_cols[rows, s : s + 1] * xs[s, rows, :].astype(F32)
        g[c, tp] = v.astype(BF)

    def send_chunk(c):
        move(c, tp, 0, other_y).start()
        move(c, tp, 1, right).start()
        move(c, tp, 3, left).start()

    make_chunk(0)
    for c in range(NC):
        if c + 1 < NC:
            make_chunk(c + 1)
        if c < AHEAD:
            send_chunk(c)
    for d in range(3):
        count_to(0, d, z_peers[d]).start()
    pltpu.make_async_copy(w_hbm, wbuf, w_sem).wait()

    def block_of(half, d):
        return half * 8 + ((z + 4 - d) % 4) * 2 + core

    two = pl.ds(0, 2)

    def spread(c, d):
        return remote(
            sb.at[(z + d) % 4, c, two], att.at[seq, c, two],
            a_ss, a_rs.at[c, d - 1], z_peers[d - 1], tp,
        )

    def spread_in(c, d):
        ref = sb.at[0, c, two]
        remote(ref, ref, a_ss, a_rs.at[c, d - 1], z_peers[0], tp).wait_recv()

    def spread_q(c, d):
        return remote(
            sb.at[(z + d) % 4, c, 2], att.at[seq, c, 2],
            a_ss, q_rs, z_peers[d - 1], tp,
        )

    def kept():
        return pltpu.make_async_copy(sb.at[z], att.at[seq], o_sem)

    def kv(c, d):
        return sb.at[z, c, pl.ds(0, 2)] if d == 0 else att.at[block_of(yhi, d), c, pl.ds(0, 2)]

    def twin(c, d):
        dst = att.at[block_of(yhi, d), c, pl.ds(0, 2)]
        return remote(kv(c, d), dst, sib_ss, sib_rs, sibling, tp)

    def cross(c, d):
        dst = att.at[block_of(0, d), c, pl.ds(0, 2)]
        return remote(kv(c, d), dst, x_ss, x_rs.at[c], mirror, tp)

    def twin2(c, d):
        ref = att.at[block_of(0, d), c, pl.ds(0, 2)]
        return remote(ref, ref, sib2_ss, sib2_rs, sibling, tp)

    def hand_on(i):
        arrived(i, 0, 1)
        move(i, b_p, 3, right).start()
        move(i, b_p, 2, left).start()

    for c in range(HANDED):
        hand_on(c)

    def feed(i):
        @pl.when(i + AHEAD < NC)
        def _():
            send_chunk(i + AHEAD)

        @pl.when(i + HANDED < NC)
        def _():
            hand_on(i + HANDED)

        @pl.when(i < NC)
        def _():
            arrived(i, 1, 1)
            move(i, b_l0, 3, right).start()
            arrived(i, 2, 1)
            move(i, b_r1, 3, left).start()

    def projected(c0):
        for e in range(2):
            c = c0 + e
            rows = slice(e * R, (e + 1) * R)
            arrived(c, 3, 4)
            ss = jnp.zeros((R, 128), F32)
            for b in range(8):
                g32 = g[c, b].astype(F32)
                q = g32 * g32
                ss = ss + ((q[:, 0:128] + q[:, 128:256]) + (q[:, 256:384] + q[:, 384:512]))
                gained[rows, b * W : (b + 1) * W] = (g32 * gain[:, b * W : (b + 1) * W]).astype(BF)
            norms[rows, :] = jnp.broadcast_to(
                lax.rsqrt(jnp.sum(ss, axis=1, keepdims=True) / D + EPS), (R, 128)
            )
        norm = norms[:, 0:1]
        lhs = gained[...]

        def project(slot, third):
            out = (jnp.dot(lhs, wbuf[third], preferred_element_type=F32) * norm).astype(BF)
            for h in range(4):
                for e in range(2):
                    sb[h, c0 + e, slot] = out[e * R : (e + 1) * R, h * HD : (h + 1) * HD]

        project(0, 1)
        project(1, 2)
        for e in range(2):
            for d in (1, 3, 2):
                spread(c0 + e, d).start()

        @pl.when(yhi == 0)
        def _():
            for e in range(2):
                cross(c0 + e, 0).start()

        for e in range(2):
            twin(c0 + e, 0).start()
        project(2, 0)
        for e in range(2):
            for d in (2, 1, 3):
                spread_q(c0 + e, d).start()

    def share(c):
        for d in (1, 3, 2):
            spread_in(c, d)

            @pl.when(yhi == 0)
            def _():
                cross(c, d).start()

            twin(c, d).start()

    def share_far(c):
        ref = sb.at[:, c, two]
        remote(ref, ref, x_ss, x_rs.at[c], mirror, tp).wait_recv()
        for d in range(4):
            twin2(c, d).start()

    def step(i, carry):
        @pl.when(i == 1)
        def _():
            count_to(1, 3, sibling).start()

        @pl.when(i == 2)
        def _():
            count_to(2, 4, mirror).start()

        feed(2 * i)

        @pl.when(i >= 1)
        def _():
            projected(2 * i - 2)

        feed(2 * i + 1)

        @pl.when(i == 0)
        def _():
            to_y().wait_recv()
            nall[1] = nall[0] + nrecv[0]
            v = csend[0]
            remote(crecv.at[pl.ds(0, 3)], crecv.at[pl.ds(0, 3)], c_ss, c_rs.at[0], sibling, tp).wait_recv()
            for d in range(3):
                v = v + crecv[d]
            csend[1] = v

        @pl.when(i == 1)
        def _():
            count_to(1, 3, sibling).wait_recv()
            csend[2] = csend[1] + crecv[3]

        @pl.when(i >= 1)
        def _():
            share(2 * i - 2)
            share(2 * i - 1)

        @pl.when((i >= 2) & (yhi == 1))
        def _():
            share_far(2 * i - 4)
            share_far(2 * i - 3)

        @pl.when(i == NC // 2 - 1)
        def _():
            for k in (2, 1, 3):
                to_x(k).start()

        return carry

    lax.fori_loop(0, NC // 2 + 1, step, 0)
    kept().start()

    count_to(2, 4, mirror).wait_recv()
    csend[3] = csend[2] + crecv[4]
    told = pltpu.make_async_copy(csend.at[3], counts.at[0], t_sem)
    told.start()
    three = nrecv.at[pl.ds(1, 3)]
    remote(three, three, n_ss.at[1], n_rs.at[1], seq, right).wait_recv()
    ztot = (nall[1] + nrecv[1]) + (nrecv[2] + nrecv[3])
    ztot = ztot * inv_rms + bias_col
    post = 2.0 / (1.0 + jnp.exp(-ztot[0:8]))
    e0, e1 = balanced(jnp.exp(ztot[8:16]), jnp.exp(ztot[16:24]))
    cols[...] = columns(jnp.concatenate([post, e0, e1], axis=0))
    noted = pltpu.make_async_copy(cols, mix_cols, m_sem)
    noted.start()

    @pl.when(yhi == 1)
    def _():
        share_far(NC - 2)
        share_far(NC - 1)

    told.wait()
    noted.wait()
    kept().wait()

    def all_of(ref, ssem, rsem):
        return remote(ref, ref, ssem, rsem, sibling, tp)

    all_of(urecv, u_ss, u_rs).wait_send()
    all_of(nall.at[0], n_ss.at[0], n_rs.at[0]).wait_send()
    all_of(three, n_ss.at[1], n_rs.at[1]).wait_send()
    all_of(crecv, c_ss, c_rs.at[0]).wait_send()
    all_of(g.at[pl.ds(0, 7)], g_ss, g_rs.at[0, 0]).wait_send()
    all_of(sb.at[pl.ds(0, 3)], a_ss, a_rs.at[0, 0]).wait_send()
    all_of(sb.at[pl.ds(0, 3), :, 2], a_ss, q_rs).wait_recv()
    twins = all_of(sb.at[:, :, two], sib_ss, sib_rs)
    twins.wait_send()
    twins.wait_recv()

    @pl.when(yhi == 0)
    def _():
        all_of(sb.at[:, :, two], x_ss, x_rs.at[0]).wait_send()

    @pl.when(yhi == 1)
    def _():
        far = all_of(sb.at[:, :, two], sib2_ss, sib2_rs)
        far.wait_send()
        far.wait_recv()


def attention_kernel(att_hbm, cnt_hbm, ctx, att, cnt, vx, m_ref, acc_ref, c_sem, k_sem, v_sem, q_sem):
    seq = lax.axis_index("seq")
    yhi, core = seq // 8, seq % 2
    counts_in = pltpu.make_async_copy(cnt_hbm.at[0], cnt, c_sem)
    counts_in.start()

    def q_in(qi):
        qb = yhi * 8 + qi * 2 + core
        return pltpu.make_async_copy(att_hbm.at[qb, :, 2], att.at[qb, :, 2], q_sem.at[qi])

    def k_in(kb):
        return pltpu.make_async_copy(att_hbm.at[kb, :, 0], att.at[kb, :, 0], k_sem.at[kb])

    def v_in(kb):
        return pltpu.make_async_copy(att_hbm.at[kb, :, 1], vx.at[kb, :, :, pl.ds(0, HD)], v_sem.at[kb])

    q_in(0).start()
    k_in(yhi * 8 + core).start()
    v_in(yhi * 8 + core).start()
    counts_in.wait()
    starts = [cnt[k, 0] for k in range(1, 4)]
    scale = HD ** (-0.5) * 1.4426950408889634

    def start_of(p):
        v = p * 0
        for c in starts:
            v = jnp.where(c <= p, jnp.maximum(v, c), v)
        return v

    first_needed = start_of((yhi * 8 + core) * T) // T

    def fetch(kb, c):
        k_in(kb).start()
        v_in(kb).start()
        return c

    def land(kb, c):
        k_in(kb).wait()
        v_in(kb).wait()
        return c

    lax.fori_loop(first_needed, yhi * 8 + core, fetch, 0)
    for qi in range(1, 4):
        q_in(qi).start()
    lax.fori_loop(yhi * 8 + core + 1, yhi * 8 + core + 7, fetch, 0)

    def ones(kb, c):
        vx[kb, :, :, HD:] = jnp.ones((NC, R, HD), BF)
        return c

    lax.fori_loop(first_needed, yhi * 8 + core + 7, ones, 0)

    def one_query_block(qi, carry):
        qb = yhi * 8 + qi * 2 + core
        q_in(qi).wait()
        land(qb, 0)
        q = att[qb, :, 2].reshape(T, HD)
        first = start_of(qb * T)
        last = start_of(qb * T + T - 1)
        lo = first // T
        mid = jnp.minimum((last + T - 1) // T, qb)
        qpos = qb * T + lax.broadcasted_iota(jnp.int32, (T, 1), 0)
        qstart = start_of(qpos)
        def block(kb, mode, n=1):
            k = att[pl.ds(kb, n), :, 0].reshape(n * T, HD)
            v = vx[pl.ds(kb, n)].reshape(n * T, 2 * HD)

            def scores(t):
                rows = slice(t * HALF, (t + 1) * HALF)
                s = lax.dot_general(q[rows], k, NT, preferred_element_type=F32)
                if mode != "all":
                    kpos = kb * T + lax.broadcasted_iota(jnp.int32, (1, T), 1)
                    ok = kpos >= qstart[rows]
                    if mode == "diagonal":
                        ok = ok & (kpos <= qpos[rows])
                    s = jnp.where(ok, s, NEG)
                return s

            later = scores(0)
            for t in range(T // HALF):
                rows = slice(t * HALF, (t + 1) * HALF)
                s = later
                if (t + 1) * HALF < T:
                    later = scores(t + 1)
                top = s[:, 0:128]
                for e in range(1, n * 4):
                    top = jnp.maximum(top, s[:, e * 128 : (e + 1) * 128])
                m_new = jnp.max(top, axis=1, keepdims=True)
                if mode != "diagonal":
                    m_old = m_ref[rows, 0:1]
                    m_new = jnp.maximum(m_old, m_new)
                    alpha = jnp.exp2((m_old - m_new) * scale)
                p = jnp.exp2((s - m_new) * scale).astype(BF)
                more = jnp.dot(p, v, preferred_element_type=F32)
                acc_ref[rows] = more if mode == "diagonal" else acc_ref[rows] * alpha + more
                m_ref[rows] = jnp.broadcast_to(m_new, (HALF, 128))

        def some(kb, c):
            block(kb, "start")
            return c

        def two(k, c):
            block(mid + 4 * k, "all", 4)
            return c

        def one(kb, c):
            block(kb, "all")
            return c

        block(qb, "diagonal")
        lax.fori_loop(jnp.where(qi == 0, first_needed, qb - 1), qb, land, 0)
        lax.fori_loop(lo, mid, some, 0)
        pairs = (qb - mid) // 4
        lax.fori_loop(0, pairs, two, 0)
        lax.fori_loop(mid + 4 * pairs, qb, one, 0)
        out = acc_ref[:, 0:HD] / acc_ref[:, HD : HD + 1]
        ctx[qi] = out.astype(BF).reshape(NO, RO, HD)
        return carry

    lax.fori_loop(0, 4, one_query_block, 0)


def last_kernel(
    ctx, wbuf, xraw, cols,
    out,
    cbuf, snd, snh, own, rcv, rch, kept,
    z_ss, z_rs, s_ss, s_rs, h_ss, h_rs,
):
    seq, tp = where_am_i()
    yhi, z, core = seq // 8, (seq // 2) % 4, seq % 2
    x, y = tp // 2, tp % 2
    right = ((x + 1) % 4) * 2 + y
    left = ((x + 3) % 4) * 2 + y
    other_y = x * 2 + 1 - y
    z_peers = [yhi * 8 + ((z + d) % 4) * 2 + core for d in range(1, 4)]
    entered = greet([(p, tp) for p in z_peers] + [(seq, right), (seq, left), (seq, other_y)])
    entered()

    def back(c, d):
        return remote(
            ctx.at[(z + d) % 4, c], cbuf.at[z, c], z_ss, z_rs.at[c], z_peers[d - 1], tp
        )

    def back_in(c):
        ref = ctx.at[pl.ds(0, 3), c]
        remote(ref, ref, z_ss, z_rs.at[c], z_peers[0], tp).wait_recv()

    for c in range(NO):
        for d in (2, 1, 3):
            back(c, d).start()
    cbuf[z] = ctx[z]

    def pass_on(c, k, to):
        return remote(snd.at[c, k], rcv.at[c, k], s_ss, s_rs.at[c, k], seq, to)

    def half(c, k, to):
        return remote(snh.at[c, k], rch.at[c, k], h_ss, h_rs.at[c, k], seq, to)

    to_right, to_left, far = ((x + 1) % 4) * 2, ((x + 3) % 4) * 2, ((x + 2) % 4) * 2

    def project(c, carry):
        back_in(c)
        lhs = jnp.concatenate([cbuf[h, c] for h in range(4)], axis=1)

        def term(b):
            cols = pl.ds(pl.multiple_of(b * W, W), W)
            return jnp.dot(lhs, wbuf[:, cols], preferred_element_type=F32)

        snd[c, 0] = term(far + 1 - y).astype(BF)
        snd[c, 1] = term(to_right + 1 - y).astype(BF)
        pass_on(c, 0, other_y).start()
        snd[c, 2] = term(to_left + 1 - y).astype(BF)
        pass_on(c, 1, right).start()
        own[c, 0] = term(far + y)
        pass_on(c, 2, left).start()
        own[c, 1] = term(to_right + y)
        own[c, 2] = term(to_left + y)
        own[c, 3] = term(other_y)
        own[c, 4] = term(tp)
        return carry

    lax.fori_loop(0, NO, project, 0)

    def second(c, carry):
        pass_on(c, 0, other_y).wait_recv()
        far_sum = (own[c, 0] + rcv[c, 0].astype(F32)).astype(BF)
        snh[c, 0] = far_sum[0 : RO // 2]
        snh[c, 1] = far_sum[RO // 2 :]
        half(c, 0, right).start()
        half(c, 1, left).start()
        return carry

    lax.fori_loop(0, NO, second, 0)

    def third(c, carry):
        pass_on(c, 1, right).wait_recv()
        pass_on(c, 2, left).wait_recv()
        snd[c, 5] = (own[c, 3] + (rcv[c, 1].astype(F32) + rcv[c, 2].astype(F32))).astype(BF)
        pass_on(c, 5, other_y).start()
        half(c, 0, right).wait_recv()
        snd[c, 3, 0 : RO // 2] = (own[c, 1, 0 : RO // 2] + rch[c, 0].astype(F32)).astype(BF)
        snd[c, 3, RO // 2 :] = own[c, 1, RO // 2 :].astype(BF)
        pass_on(c, 3, right).start()
        half(c, 1, left).wait_recv()
        snd[c, 4, 0 : RO // 2] = own[c, 2, 0 : RO // 2].astype(BF)
        snd[c, 4, RO // 2 :] = (own[c, 2, RO // 2 :] + rch[c, 1].astype(F32)).astype(BF)
        pass_on(c, 4, left).start()
        return carry

    lax.fori_loop(0, NO, third, 0)

    def fourth(c, carry):
        rows = pl.ds(pl.multiple_of(c * RO, RO), RO)
        xv = jnp.swapaxes(xraw[rows], 0, 1)
        wide = [xv[j].astype(F32) for j in range(S)]
        for i in range(S):
            k = 8 + 4 * i
            v = cols[rows, k : k + 1] * wide[0]
            for j in range(1, S):
                v = v + cols[rows, k + j : k + j + 1] * wide[j]
            kept[i] = v
        pass_on(c, 5, other_y).wait_recv()
        mine = own[c, 4] + rcv[c, 5].astype(F32)
        pass_on(c, 3, right).wait_recv()
        pass_on(c, 4, left).wait_recv()
        branch = mine + (rcv[c, 3].astype(F32) + rcv[c, 4].astype(F32))
        new = [(kept[i] + cols[rows, 4 + i : 5 + i] * branch).astype(BF) for i in range(S)]
        out[rows] = jnp.swapaxes(jnp.stack(new, axis=0), 0, 1)
        return carry

    lax.fori_loop(0, NO, fourth, 0)

    everything = ctx.at[pl.ds(0, 3)]
    remote(everything, everything, z_ss, z_rs.at[0], seq, right).wait_send()
    remote(snd, snd, s_ss, s_rs.at[0, 0], seq, right).wait_send()
    remote(snh, snh, h_ss, h_rs.at[0, 0], seq, right).wait_send()


def store_kernel(x, out, sem):
    copies = [
        pltpu.make_async_copy(x.at[pl.ds(q * 128, 128)], out.at[pl.ds(q * 128, 128)], sem.at[q])
        for q in range(4)
    ]
    for copy in copies:
        copy.start()
    for copy in copies:
        copy.wait()


def local(streams, doc_ids, mix_weight, mix_bias, attn_gain, w_qkv, w_out):
    wmix = jnp.transpose(mix_weight, (0, 2, 1))
    wq = jnp.transpose(w_qkv, (1, 0, 2))
    vm = pl.BlockSpec(memory_space=VMEM)
    hbm = pl.BlockSpec(memory_space=pl.ANY)
    sds = jax.ShapeDtypeStruct
    att, mix_cols, counts = pl.pallas_call(
        first_kernel,
        name="gather_project",
        out_shape=(
            sds((BLOCKS, NC, 3, R, HD), BF),
            sds((T, 128), F32),
            sds((TILES, 8, 128), jnp.int32),
        ),
        in_specs=[hbm] * 6,
        out_specs=(hbm, hbm, hbm),
        scratch_shapes=[
            VMEM((T, S, W), BF),
            VMEM((S, T, W), BF),
            VMEM((4, 128), jnp.int32),
            VMEM((S, 24, W), F32),
            VMEM((1, 24), F32),
            VMEM((1, D), F32),
            VMEM((3, D, W), BF),
            VMEM((NC, 8, R, W), BF),
            VMEM((4, NC, 3, R, HD), BF),
            VMEM((2 * R, D), BF),
            VMEM((2 * R, 128), F32),
            VMEM((8, T), F32),
            VMEM((7, 8, T), F32),
            VMEM((2, 24, T), F32),
            VMEM((4, 24, T), F32),
            VMEM((4, 8, 128), jnp.int32),
            VMEM((5, 8, 128), jnp.int32),
            VMEM((T, 128), F32),
            VMEM((T, 128), F32),
            DMA((4,)),
            DMA((4,)),
            DMA(()),
            DMA(()), DMA(()),
            DMA((2,)), DMA((2,)),
            DMA(()), DMA((3,)),
            DMA(()), DMA((NC, 4)),
            DMA(()), DMA((NC, 3)),
            DMA(()),
            DMA(()),
            DMA(()),
            DMA(()),
            DMA(()), DMA(()),
            DMA(()), DMA((NC,)),
            DMA(()), DMA(()),
        ],
        compiler_params=pltpu.CompilerParams(
            collective_id=0, has_side_effects=True, vmem_limit_bytes=60 * 1024 * 1024
        ),
    )(
        streams, doc_ids.reshape(4, 128), wmix, mix_bias.reshape(1, 24), attn_gain.reshape(1, D), wq,
    )
    ctx = pl.pallas_call(
        attention_kernel,
        name="attention",
        out_shape=sds((4, NO, RO, HD), BF),
        in_specs=[hbm, hbm],
        out_specs=vm,
        scratch_shapes=[
            VMEM((16, NC, 3, R, HD), BF),
            pltpu.SMEM((8, 128), jnp.int32),
            VMEM((16, NC, R, 2 * HD), BF),
            VMEM((T, 128), F32), VMEM((T, 2 * HD), F32),
            DMA(()), DMA((16,)), DMA((16,)), DMA((4,)),
        ],
        compiler_params=pltpu.CompilerParams(vmem_limit_bytes=30 * 1024 * 1024),
    )(att, counts)
    new = pl.pallas_call(
        last_kernel,
        name="project_out",
        out_shape=sds((T, S, W), BF),
        in_specs=[vm] * 4,
        out_specs=vm,
        scratch_shapes=[
            VMEM((4, NO, RO, HD), BF),
            VMEM((NO, 6, RO, W), BF),
            VMEM((NO, 2, RO // 2, W), BF),
            VMEM((NO, 5, RO, W), F32),
            VMEM((NO, 6, RO, W), BF),
            VMEM((NO, 2, RO // 2, W), BF),
            VMEM((S, RO, W), F32),
            DMA(()), DMA((NO,)),
            DMA(()), DMA((NO, 6)),
            DMA(()), DMA((NO, 2)),
        ],
        compiler_params=pltpu.CompilerParams(
            collective_id=1, has_side_effects=True, vmem_limit_bytes=30 * 1024 * 1024
        ),
    )(ctx, w_out, streams, mix_cols)
    return pl.pallas_call(
        store_kernel,
        name="store",
        out_shape=sds((T, S, W), BF),
        in_specs=[vm],
        out_specs=hbm,
        scratch_shapes=[DMA((4,))],
        compiler_params=pltpu.CompilerParams(vmem_limit_bytes=8 * 1024 * 1024),
    )(new)


def solution(mesh):
    in_specs = (
        P("seq", None, "tp"),
        P("seq"),
        P(None, "tp", None),
        P(),
        P(),
        P(None, None, "tp"),
        P("tp", None),
    )
    return jax.shard_map(
        local, mesh=mesh, in_specs=in_specs, out_specs=P("seq", None, "tp"), check_vma=False
    )
```
